32 devices in a mesh: dp: 8 (over z, x), tensor: 4 (over y, core).
Axes of the slice: x: 2, y: 2, z: 4, core: 2. Of those that a mesh axis runs over, the one named last changes fastest.
Arguments:
- tokens: bfloat16 [8192, 1536], P('dp'), may hold values from -6 to 6
- lengths: int32 [12], replicated, may hold values from 512 to 1024, as said below
- owners: int32 [12], replicated, may hold values from 0 to 7, as said below
- first_gain: float32 [1536], replicated, may hold values from 0.5 to 1.5
- query_weight: bfloat16 [1536, 1536], P(None, 'tensor')
- key_weight: bfloat16 [1536, 768], P(None, 'tensor')
- value_weight: bfloat16 [1536, 768], P(None, 'tensor'), may hold values from -0.15625 to 0.15625
- mixing_weight: bfloat16 [1536, 1536], P(None, 'tensor'), may hold values from -2.5 to 2.5
- second_gain: float32 [1536], replicated, may hold values from 0.5 to 1.5
- gate_weight: bfloat16 [1536, 4096], P(None, 'tensor'), may hold values from -0.15625 to 0.15625
- up_weight: bfloat16 [1536, 4096], P(None, 'tensor'), may hold values from -0.15625 to 0.15625
- down_weight: bfloat16 [1536, 4096], P(None, 'tensor'), may hold values from -0.09375 to 0.09375
- cotangent: bfloat16 [8192, 1536], P('dp'), may hold values from -6 to 6
Outputs:
- layer_output: bfloat16 [8192, 1536], P(('dp', 'tensor'))
- token_grad: bfloat16 [8192, 1536], P(('dp', 'tensor'))
- first_grad: float32 [1536], replicated
- query_grad: float32 [1536, 1536], P('dp', 'tensor')
- key_grad: float32 [1536, 768], P('dp', 'tensor')
- value_grad: float32 [1536, 768], P('dp', 'tensor')
- mixing_grad: float32 [1536, 1536], P('dp', 'tensor')
- second_grad: float32 [1536], replicated
- gate_grad: float32 [1536, 4096], P('dp', 'tensor')
- up_grad: float32 [1536, 4096], P('dp', 'tensor')
- down_grad: float32 [1536, 4096], P('dp', 'tensor')
The draws below stay inside these ranges and needn't reach their ends.
Inputs may be any that keep to these rules, and one draw needn't show every extreme that they name: `lengths`: the sequences of one index of dp total at most 1024 tokens; one sequence has exactly 1024 tokens and one exactly 512. `owners`: every index of dp holds one or two sequences.
All inputs are finite; a program needn't handle non-finite values.
Results may differ from the reference program's by a relative error of at most 0.023.
Values may be sent and summed in bfloat16 or wider, within the bound.
A program may use at most 192 MiB of HBM per device.

```python
import jax
import jax.numpy as jnp
from jax import lax

D = 1536
H = 16
KV = 8
HD = 96
FF = 4096
CAP = 1024
MINLEN = 512
NSEQ = 12
TOKENS = 8192
N_DP = 8
N_TENSOR = 4


def sequence_plan(key):
    half_count = N_DP // 2
    device_order = jax.random.permutation(jax.random.fold_in(key, 1), N_DP).astype(jnp.int32)
    paired = device_order[:half_count]
    single = device_order[half_count:]
    single_len = jax.random.randint(jax.random.fold_in(key, 2), (N_DP - half_count,), MINLEN, CAP + 1, dtype=jnp.int32)
    single_len = single_len.at[0].set(CAP)
    owner_list = jnp.concatenate([jnp.repeat(paired, 2), single]).astype(jnp.int32)
    length_list = jnp.concatenate([jnp.full((2 * half_count,), MINLEN, jnp.int32), single_len]).astype(jnp.int32)
    shuffle = jax.random.permutation(jax.random.fold_in(key, 3), NSEQ)
    return (owner_list[shuffle], length_list[shuffle])


def draw_lengths(key, part):
    return sequence_plan(key)[1]


def draw_owners(key, part):
    return sequence_plan(key)[0]


def projection_pair(key):
    query_part = jax.random.normal(jax.random.fold_in(key, 21), (D, H * HD), jnp.float32) * D ** (-0.5)
    key_part = jax.random.normal(jax.random.fold_in(key, 22), (D, KV * HD), jnp.float32) * D ** (-0.5)
    return (query_part, key_part)


def draw_query_weight(key, part):
    return projection_pair(key)[0].astype(jnp.bfloat16)


def draw_key_weight(key, part):
    return projection_pair(key)[1].astype(jnp.bfloat16)


def shard_levels(stream_key, dims, pieces, least, largest):
    level, own = 1.0, jax.random.fold_in(stream_key, 6)
    for dim, shards_of in pieces:
        draws = jnp.exp(jax.random.uniform(jax.random.fold_in(own, dim), (shards_of,), jnp.float32, least / len(pieces), largest / len(pieces)))
        level = level * jnp.repeat(draws, dims[dim] // shards_of).reshape([-1 if axis == dim else 1 for axis in range(len(dims))])
    return level


def centred(stream_key, extent, scale, bound, split=(), kind=jnp.bfloat16):
    values = jax.random.normal(stream_key, extent, jnp.float32) * scale
    if len(split) > 0:
        values = shard_levels(stream_key, extent, split, -0.22, 0.18) * values
    return jnp.clip(values, min=-bound, max=bound).astype(kind)


def setup_inputs(seed: int = 0) -> dict:
    splits = jax.random.split(jax.random.key(seed), 14)
    return {
        "tokens": centred(splits[0], (TOKENS, D), 1.0, 6.0, ((0, 8),)),
        "lengths": draw_lengths(jax.random.fold_in(splits[13], 71), 0),
        "owners": draw_owners(jax.random.fold_in(splits[13], 71), 0),
        "first_gain": jnp.clip(1.0 + 0.1 * jax.random.normal(splits[3], (D,), jnp.float32), 0.5, 1.5),
        "query_weight": draw_query_weight(jax.random.fold_in(splits[13], 71), 0),
        "key_weight": draw_key_weight(jax.random.fold_in(splits[13], 71), 0),
        "value_weight": centred(splits[6], (D, KV * HD), D ** -0.5, 0.15625, ((1, 4),)),
        "mixing_weight": centred(splits[7], (D, H * HD), (max(1, H * HD // 256)) ** -0.5, 2.5, ((1, 4),)),
        "second_gain": jnp.clip(1.0 + 0.1 * jax.random.normal(splits[8], (D,), jnp.float32), 0.5, 1.5),
        "gate_weight": centred(splits[9], (D, FF), D ** -0.5, 0.15625, ((1, 4),)),
        "up_weight": centred(splits[10], (D, FF), D ** -0.5, 0.15625, ((1, 4),)),
        "down_weight": centred(splits[11], (D, FF), FF ** -0.5, 0.09375, ((1, 4),)),
        "cotangent": centred(splits[12], (TOKENS, D), 1.0, 6.0, ((0, 8),)),
    }


epsilon = 1e-05
rope_base = 10000.0
highest = lax.Precision.HIGHEST

@jax.custom_vjp
def low(v):
    return lax.optimization_barrier(v.astype(jnp.bfloat16)).astype(jnp.float32)

@jax.custom_vjp
def low_back(v):
    return v

def low_keep(v):
    return (low(v), None)

def low_pass(kept, grad):
    return (grad,)

def back_keep(v):
    return (v, None)

def back_low(kept, grad):
    return (low(grad),)
low.defvjp(low_keep, low_pass)
low_back.defvjp(back_keep, back_low)

def slot_layout(lengths, owners, device, slot_count):
    seq_count = lengths.shape[0]
    chosen = owners == device
    taken_len = jnp.where(chosen, lengths, 0).astype(jnp.int32)
    finish = jnp.cumsum(taken_len).astype(jnp.int32)
    begins = finish - taken_len
    slot_ids = jnp.arange(slot_count, dtype=jnp.int32)[:, None]
    inside = (chosen[None, :] & (slot_ids >= begins[None, :]) & (slot_ids < finish[None, :])).astype(jnp.int32)
    seq_ids = jnp.arange(seq_count, dtype=jnp.int32)[None, :]
    filled = lax.optimization_barrier(jnp.sum(inside, axis=1)).astype(jnp.int32)
    segment = lax.optimization_barrier(jnp.sum(inside * seq_ids, axis=1)).astype(jnp.int32) + (1 - filled) * seq_count
    offset = lax.optimization_barrier(jnp.sum(inside * (slot_ids - begins[None, :]), axis=1)).astype(jnp.int32) + (1 - filled) * slot_ids[:, 0]
    return (segment, offset, filled.astype(jnp.float32))

def rotary_tables(offset, head_size):
    half_size = head_size // 2
    frequency = rope_base ** (-(2.0 * jnp.arange(half_size, dtype=jnp.float32)) / head_size)
    angles = offset.astype(jnp.float32)[:, None] * frequency[None, :]
    return (jnp.cos(angles)[:, None, :], jnp.sin(angles)[:, None, :])

def rotate(values, cos_table, sin_table):
    half_size = values.shape[-1] // 2
    first_half = values[..., :half_size]
    second_half = values[..., half_size:]
    return jnp.concatenate([first_half * cos_table - second_half * sin_table, second_half * cos_table + first_half * sin_table], axis=-1)

def inverse_rms(values):
    return lax.rsqrt(lax.optimization_barrier(jnp.mean(values * values, axis=-1, keepdims=True)) + epsilon)

def matmul(left_side, right_side):
    return jnp.dot(left_side, right_side, precision=highest, preferred_element_type=jnp.float32)

def attend(queries, key_rows, values, segment):
    slot_count, heads_here, head_size = queries.shape
    sharing = heads_here // key_rows.shape[1]
    wide_keys = jnp.repeat(key_rows, sharing, axis=1)
    wide_values = jnp.repeat(values, sharing, axis=1)
    block_rows = min(512, slot_count)
    blocks = slot_count // block_rows
    slot_ids = jnp.arange(slot_count, dtype=jnp.int32)
    scaling = head_size ** (-0.5)

    def one_block(packed):
        block_queries, block_segment, block_slots = packed
        scores = low_back(jnp.einsum('qhd,khd->hqk', block_queries, wide_keys, precision=highest) * scaling)
        allowed = (block_segment[:, None] == segment[None, :]) & (slot_ids[None, :] <= block_slots[:, None])
        scores = jnp.where(allowed[None], scores, -jnp.inf)
        weights = low(jax.nn.softmax(scores, axis=-1))
        return jnp.einsum('hqk,khd->qhd', weights, wide_values, precision=highest)
    result = lax.map(jax.checkpoint(one_block), (queries.reshape(blocks, block_rows, heads_here, head_size), segment.reshape(blocks, block_rows), slot_ids.reshape(blocks, block_rows)))
    return result.reshape(slot_count, heads_here, head_size)

def device_layer(block_tokens, segment, offset, filled, params):
    first_gain, query_weight, key_weight, value_weight, mixing_weight, second_gain, gate_weight, up_weight, down_weight = params
    slot_count = block_tokens.shape[0]
    cos_table, sin_table = rotary_tables(offset, HD)
    normed = low(block_tokens * inverse_rms(block_tokens) * first_gain)
    query_cols = H * HD // N_TENSOR
    kv_cols = KV * HD // N_TENSOR
    hidden_cols = FF // N_TENSOR
    mixed_total = jnp.zeros((slot_count, D), jnp.float32)
    for group_index in range(N_TENSOR):
        group_in = low_back(normed)
        query_start = group_index * query_cols
        kv_start = group_index * kv_cols
        query_raw = low_back(matmul(group_in, query_weight[:, query_start:query_start + query_cols]))
        queries = low(rotate(query_raw.reshape(slot_count, query_cols // HD, HD), cos_table, sin_table))
        key_raw = low_back(matmul(group_in, key_weight[:, kv_start:kv_start + kv_cols]))
        key_rows = low(rotate(key_raw.reshape(slot_count, kv_cols // HD, HD), cos_table, sin_table))
        values = low(low_back(matmul(group_in, value_weight[:, kv_start:kv_start + kv_cols]))).reshape(slot_count, kv_cols // HD, HD)
        attended = low(low_back(attend(queries, key_rows, values, segment).reshape(slot_count, query_cols)))
        mixed_total = mixed_total + low(matmul(attended, mixing_weight[:, query_start:query_start + query_cols].T))
    middle = block_tokens + low_back(mixed_total)
    second_in = low(middle * inverse_rms(middle) * second_gain)
    feed_total = jnp.zeros((slot_count, D), jnp.float32)
    for group_index in range(N_TENSOR):
        group_in = low_back(second_in)
        hidden_start = group_index * hidden_cols
        gate_value = low_back(matmul(group_in, gate_weight[:, hidden_start:hidden_start + hidden_cols]))
        upward = low_back(matmul(group_in, up_weight[:, hidden_start:hidden_start + hidden_cols]))
        hidden = low(jax.nn.silu(gate_value) * upward)
        feed_total = feed_total + low(matmul(hidden, down_weight[:, hidden_start:hidden_start + hidden_cols].T))
    return (middle + low_back(feed_total)) * filled[:, None]

def reference(tokens, lengths, owners, first_gain, query_weight, key_weight, value_weight, mixing_weight, second_gain, gate_weight, up_weight, down_weight, cotangent):
    floats = (first_gain.astype(jnp.float32), query_weight.astype(jnp.float32), key_weight.astype(jnp.float32), value_weight.astype(jnp.float32), mixing_weight.astype(jnp.float32), second_gain.astype(jnp.float32), gate_weight.astype(jnp.float32), up_weight.astype(jnp.float32), down_weight.astype(jnp.float32))
    token_blocks = tokens.astype(jnp.float32).reshape(N_DP, CAP, D)
    device_ids = jnp.arange(N_DP, dtype=jnp.int32)

    def forward(block_stack, params):

        def per_device(packed):
            block_tokens, device = packed
            segment, offset, filled = slot_layout(lengths, owners, device, CAP)
            return device_layer(block_tokens, segment, offset, filled, params)
        return lax.map(jax.checkpoint(per_device), (block_stack, device_ids))
    outputs, pullback = jax.vjp(forward, token_blocks, floats)
    token_back, gradients = pullback(cotangent.astype(jnp.float32).reshape(N_DP, CAP, D))
    return (outputs.reshape(N_DP * CAP, D).astype(jnp.bfloat16), token_back.reshape(N_DP * CAP, D).astype(jnp.bfloat16), gradients[0], gradients[1], gradients[2], gradients[3], gradients[4], gradients[5], gradients[6], gradients[7], gradients[8])
```

```python
import jax
import jax.numpy as jnp
from jax import lax
from jax.sharding import PartitionSpec as P

HD = 96


epsilon = 1e-05
rope_base = 10000.0


def slot_layout(lengths, owners, device, slot_count):
    seq_count = lengths.shape[0]
    chosen = owners == device
    taken_len = jnp.where(chosen, lengths, 0)
    finish = jnp.cumsum(taken_len)
    begins = finish - taken_len
    slot_ids = jnp.arange(slot_count, dtype=jnp.int32)[:, None]
    inside = (
        chosen[None, :] & (slot_ids >= begins[None, :]) & (slot_ids < finish[None, :])
    ).astype(jnp.int32)
    seq_ids = jnp.arange(seq_count, dtype=jnp.int32)[None, :]
    filled = jnp.sum(inside, axis=1)
    segment = jnp.sum(inside * seq_ids, axis=1) + (1 - filled) * seq_count
    offset = jnp.sum(inside * (slot_ids - begins[None, :]), axis=1) + (1 - filled) * slot_ids[:, 0]
    return (segment, offset, filled.astype(jnp.float32))


def rotary_tables(offset, head_size):
    half_size = head_size // 2
    frequency = rope_base ** (-(2.0 * jnp.arange(half_size, dtype=jnp.float32)) / head_size)
    angles = offset.astype(jnp.float32)[:, None] * frequency[None, :]
    return (jnp.cos(angles)[:, None, :], jnp.sin(angles)[:, None, :])


def rotate(values, cos_table, sin_table):
    half_size = values.shape[-1] // 2
    first_half = values[..., :half_size]
    second_half = values[..., half_size:]
    return jnp.concatenate(
        [
            first_half * cos_table - second_half * sin_table,
            second_half * cos_table + first_half * sin_table,
        ],
        axis=-1,
    )


def rotate_back(values, cos_table, sin_table):
    half_size = values.shape[-1] // 2
    first_half = values[..., :half_size]
    second_half = values[..., half_size:]
    return jnp.concatenate(
        [
            first_half * cos_table + second_half * sin_table,
            second_half * cos_table - first_half * sin_table,
        ],
        axis=-1,
    )


def inverse_rms(values):
    return lax.rsqrt(jnp.mean(values * values, axis=-1, keepdims=True) + epsilon)


def norm_back(grad_in, values, inverse, gain_vector):
    scaled = grad_in * gain_vector
    return inverse * scaled - values * inverse**3 * jnp.mean(
        scaled * values, axis=-1, keepdims=True
    )


def matmul(left_side, right_side):
    return jnp.dot(left_side, right_side, preferred_element_type=jnp.float32)


def matmul_across(left_side, right_side):
    return lax.dot_general(
        left_side, right_side, (((1,), (1,)), ((), ())), preferred_element_type=jnp.float32
    )


def matmul_rows(left_side, right_side):
    return lax.dot_general(
        left_side, right_side, (((0,), (0,)), ((), ())), preferred_element_type=jnp.float32
    )


def block_scores(block_queries, key_rows, segment, slot_ids, row_start, row_stop, scaling):
    scores = (
        jnp.einsum(
            "qkgd,skd->kgqs", block_queries, key_rows[:row_stop], preferred_element_type=jnp.float32
        )
        * scaling
    )
    allowed = (segment[row_start:row_stop, None] == segment[None, :row_stop]) & (
        slot_ids[None, :row_stop] <= slot_ids[row_start:row_stop, None]
    )
    return jnp.where(allowed, scores, -jnp.inf)


def attend_forward(queries, key_rows, values, segment):
    slot_count, heads_here, head_size = queries.shape
    kv_heads = key_rows.shape[1]
    sharing = heads_here // kv_heads
    block_rows = min(512, slot_count)
    scaling = head_size ** (-0.5)
    slot_ids = jnp.arange(slot_count, dtype=jnp.int32)
    pieces = []
    totals = []
    for block_index in range(slot_count // block_rows):
        row_start = block_index * block_rows
        row_stop = row_start + block_rows
        block_queries = queries[row_start:row_stop].reshape(
            block_rows, kv_heads, sharing, head_size
        )
        scores = block_scores(
            block_queries, key_rows, segment, slot_ids, row_start, row_stop, scaling
        )
        highest_score = jnp.max(scores, axis=-1, keepdims=True)
        exponent = jnp.exp(scores - highest_score)
        denominator = jnp.sum(exponent, axis=-1, keepdims=True)
        weights = (exponent / denominator).astype(jnp.bfloat16)
        block_out = jnp.einsum(
            "kgqs,skd->qkgd", weights, values[:row_stop], preferred_element_type=jnp.float32
        )
        pieces.append(block_out.astype(jnp.bfloat16).reshape(block_rows, heads_here * head_size))
        totals.append(highest_score + jnp.log(denominator))
    return (jnp.concatenate(pieces, axis=0), jnp.concatenate(totals, axis=2))


def attend_backward(queries, key_rows, values, out_grad, totals, segment):
    slot_count, heads_here, head_size = queries.shape
    kv_heads = key_rows.shape[1]
    sharing = heads_here // kv_heads
    block_rows = min(512, slot_count)
    scaling = head_size ** (-0.5)
    slot_ids = jnp.arange(slot_count, dtype=jnp.int32)
    query_parts = []
    key_back = jnp.zeros(key_rows.shape, jnp.float32)
    value_back = jnp.zeros(values.shape, jnp.float32)
    for block_index in range(slot_count // block_rows):
        row_start = block_index * block_rows
        row_stop = row_start + block_rows
        block_queries = queries[row_start:row_stop].reshape(
            block_rows, kv_heads, sharing, head_size
        )
        block_grad = out_grad[row_start:row_stop].reshape(block_rows, kv_heads, sharing, head_size)
        scores = block_scores(
            block_queries, key_rows, segment, slot_ids, row_start, row_stop, scaling
        )
        probability = jnp.exp(scores - totals[:, :, row_start:row_stop])
        prob_low = probability.astype(jnp.bfloat16)
        prob_grad = jnp.einsum(
            "qkgd,skd->kgqs", block_grad, values[:row_stop], preferred_element_type=jnp.float32
        )
        score_low = (
            probability * (prob_grad - jnp.sum(probability * prob_grad, axis=-1, keepdims=True))
        ).astype(jnp.bfloat16)
        query_block = (
            jnp.einsum(
                "kgqs,skd->qkgd", score_low, key_rows[:row_stop], preferred_element_type=jnp.float32
            )
            * scaling
        )
        query_parts.append(query_block.reshape(block_rows, heads_here, head_size))
        key_back = key_back.at[:row_stop].add(
            jnp.einsum(
                "kgqs,qkgd->skd", score_low, block_queries, preferred_element_type=jnp.float32
            )
            * scaling
        )
        value_back = value_back.at[:row_stop].add(
            jnp.einsum("kgqs,qkgd->skd", prob_low, block_grad, preferred_element_type=jnp.float32)
        )
    return (jnp.concatenate(query_parts, axis=0), key_back, value_back)


def bits_of(count):
    return tuple(range(count.bit_length() - 1))


def positions(count, order):
    places = [0]
    for bit in reversed(order):
        places = places + [place | (1 << bit) for place in places]
    return places


def exchange(array, axis, bit):
    count = lax.axis_size(axis)
    return lax.ppermute(array, axis, [(i, i ^ (1 << bit)) for i in range(count)])


def relative(array, axis, order):
    count = lax.axis_size(axis)
    rows = array.shape[0] // count
    index = lax.axis_index(axis)
    return jnp.concatenate(
        [
            lax.dynamic_slice_in_dim(array, (index ^ place) * rows, rows, 0)
            for place in positions(count, order)
        ],
        axis=0,
    )


def absolute(array, axis, order):
    count = lax.axis_size(axis)
    rows = array.shape[0] // count
    index = lax.axis_index(axis)
    place_of = [0] * count
    for i, place in enumerate(positions(count, order)):
        place_of[place] = i
    where = jnp.asarray(place_of, jnp.int32)
    return jnp.concatenate(
        [
            lax.dynamic_slice_in_dim(array, where[index ^ block] * rows, rows, 0)
            for block in range(count)
        ],
        axis=0,
    )


def scatter_sum(keep, send, axis, order):
    for step, bit in enumerate(order):
        total = keep.astype(jnp.float32) + exchange(send, axis, bit).astype(jnp.float32)
        half = total.shape[0] // 2
        if step + 1 < len(order):
            keep = total[:half]
            send = total[half:].astype(jnp.bfloat16)
    return total


def gather(array, axis, order):
    for bit in reversed(order):
        array = jnp.concatenate([array, exchange(array, axis, bit)], axis=0)
    return array


def sum_all(array):
    for axis in ("tensor", "dp"):
        for bit in bits_of(lax.axis_size(axis)):
            array = array + exchange(array, axis, bit)
    return array


def on_device(
    tokens,
    lengths,
    owners,
    first_gain,
    query_weight,
    key_weight,
    value_weight,
    mixing_weight,
    second_gain,
    gate_weight,
    up_weight,
    down_weight,
    cotangent,
):
    slot_count = tokens.shape[0]
    tensor_count = lax.axis_size("tensor")
    share_rows = slot_count // tensor_count
    share_start = lax.axis_index("tensor") * share_rows
    t_order = bits_of(tensor_count)
    d_order = bits_of(lax.axis_size("dp"))
    z_order = (d_order[1], d_order[0]) + d_order[2:]

    def share_of(array):
        return lax.dynamic_slice_in_dim(array, share_start, share_rows, 0)

    def rows_relative(array):
        return relative(array, "tensor", t_order)

    def columns_first(array, order):
        return relative(array.T, "dp", order)

    def row_sum(make, array):
        half = array.shape[0] // 2
        send = make(array[half:]).astype(jnp.bfloat16)
        keep = make(array[:half]).astype(jnp.bfloat16)
        return scatter_sum(keep, send, "tensor", t_order)

    def weight_sum(left, right, order):
        half = left.shape[0] // 2
        send = matmul(left[half:], right).astype(jnp.bfloat16)
        keep = matmul(left[:half], right).astype(jnp.bfloat16)
        return scatter_sum(keep, send, "dp", order)

    segment, offset, filled = slot_layout(lengths, owners, lax.axis_index("dp"), slot_count)
    head_size = HD
    cos_table, sin_table = rotary_tables(offset, head_size)
    inputs = tokens.astype(jnp.float32)
    first_inv = inverse_rms(inputs)
    first_in = (inputs * first_inv * first_gain).astype(jnp.bfloat16)
    queries = rotate(
        matmul(first_in, query_weight).reshape(slot_count, -1, head_size), cos_table, sin_table
    ).astype(jnp.bfloat16)
    key_rows = rotate(
        matmul(first_in, key_weight).reshape(slot_count, -1, head_size), cos_table, sin_table
    ).astype(jnp.bfloat16)
    values = matmul(first_in, value_weight).astype(jnp.bfloat16).reshape(slot_count, -1, head_size)
    attended, log_totals = attend_forward(queries, key_rows, values, segment)
    attended = rows_relative(attended)
    mixed = row_sum(lambda rows: matmul_across(rows, mixing_weight), attended)
    inputs_share = share_of(inputs)
    first_inv_share = share_of(first_inv)
    middle = inputs_share + mixed
    second_inv = inverse_rms(middle)
    second_in = gather(
        (middle * second_inv * second_gain).astype(jnp.bfloat16), "tensor", t_order
    )
    gate_value = matmul(second_in, gate_weight)
    upward = matmul(second_in, up_weight)
    sigmoid = jax.nn.sigmoid(gate_value)
    activated = gate_value * sigmoid
    hidden = (activated * upward).astype(jnp.bfloat16)
    live_share = share_of(filled)[:, None]
    feed_sum = row_sum(lambda rows: matmul_across(rows, down_weight), hidden)
    layer_output = ((middle + feed_sum) * live_share).astype(jnp.bfloat16)
    outer_grad = share_of(cotangent).astype(jnp.float32) * live_share
    outer_low = rows_relative(cotangent * filled[:, None].astype(jnp.bfloat16))
    hidden_grad = matmul(outer_low, down_weight)
    gate_low = (hidden_grad * upward * sigmoid * (1.0 + gate_value * (1.0 - sigmoid))).astype(
        jnp.bfloat16
    )
    upward_low = (hidden_grad * activated).astype(jnp.bfloat16)
    both_low = jnp.concatenate([gate_low, upward_low], axis=1)
    both_weight = jnp.concatenate([gate_weight, up_weight], axis=1)
    second_back = row_sum(lambda rows: matmul_across(rows, both_weight), both_low)
    down_grad = weight_sum(columns_first(outer_low, z_order), hidden, z_order)
    second_columns = columns_first(second_in, d_order)
    gate_grad = weight_sum(second_columns, gate_low, d_order)
    up_grad = weight_sum(second_columns, upward_low, d_order)
    second_term = jnp.sum(second_back * middle * second_inv, axis=0)
    middle_grad = outer_grad + norm_back(second_back, middle, second_inv, second_gain)
    branch_low = gather(middle_grad.astype(jnp.bfloat16), "tensor", t_order)
    mixing_grad = weight_sum(columns_first(branch_low, z_order), attended, z_order)
    attended_grad = absolute(
        matmul(branch_low, mixing_weight).astype(jnp.bfloat16), "tensor", t_order
    )
    query_back, key_back, value_back = attend_backward(
        queries, key_rows, values, attended_grad, log_totals, segment
    )
    query_low = (
        rotate_back(query_back, cos_table, sin_table).astype(jnp.bfloat16).reshape(slot_count, -1)
    )
    key_low = (
        rotate_back(key_back, cos_table, sin_table).astype(jnp.bfloat16).reshape(slot_count, -1)
    )
    value_low = value_back.astype(jnp.bfloat16).reshape(slot_count, -1)
    projected_low = jnp.concatenate([query_low, key_low, value_low], axis=1)
    projection = jnp.concatenate([query_weight, key_weight, value_weight], axis=1)
    first_back = row_sum(
        lambda rows: matmul_across(rows, projection), rows_relative(projected_low)
    )
    projection_grad = weight_sum(columns_first(first_in, d_order), projected_low, d_order)
    token_grad = middle_grad + norm_back(first_back, inputs_share, first_inv_share, first_gain)
    first_term = jnp.sum(first_back * inputs_share * first_inv_share, axis=0)
    first_grad, second_grad = sum_all(jnp.stack([first_term, second_term]))
    query_columns = query_weight.shape[1]
    key_columns = query_columns + key_weight.shape[1]
    return (
        layer_output,
        token_grad.astype(jnp.bfloat16),
        first_grad,
        projection_grad[:, :query_columns],
        projection_grad[:, query_columns:key_columns],
        projection_grad[:, key_columns:],
        mixing_grad,
        second_grad,
        gate_grad,
        up_grad,
        down_grad,
    )


def solution(mesh):
    in_specs = (
        P("dp", None),
        P(),
        P(),
        P(),
        P(None, "tensor"),
        P(None, "tensor"),
        P(None, "tensor"),
        P(None, "tensor"),
        P(),
        P(None, "tensor"),
        P(None, "tensor"),
        P(None, "tensor"),
        P("dp", None),
    )
    out_specs = (
        P(("dp", "tensor"), None),
        P(("dp", "tensor"), None),
        P(),
        P("dp", "tensor"),
        P("dp", "tensor"),
        P("dp", "tensor"),
        P("dp", "tensor"),
        P(),
        P("dp", "tensor"),
        P("dp", "tensor"),
        P("dp", "tensor"),
    )
    return jax.shard_map(
        on_device, mesh=mesh, in_specs=in_specs, out_specs=out_specs, check_vma=False
    )
```

```python
import jax
import jax.numpy as jnp
from jax import lax
from jax.experimental import pallas as pl
from jax.experimental.pallas import tpu as pltpu
from jax.sharding import PartitionSpec as P

HD = 96


MESH = pl.DeviceIdType.MESH

epsilon = 1e-05
rope_base = 10000.0


def slot_layout(lengths, owners, device, slot_count):
    seq_count = lengths.shape[0]
    chosen = owners == device
    taken_len = jnp.where(chosen, lengths, 0)
    finish = jnp.cumsum(taken_len)
    begins = finish - taken_len
    slot_ids = jnp.arange(slot_count, dtype=jnp.int32)[:, None]
    inside = (
        chosen[None, :] & (slot_ids >= begins[None, :]) & (slot_ids < finish[None, :])
    ).astype(jnp.int32)
    seq_ids = jnp.arange(seq_count, dtype=jnp.int32)[None, :]
    filled = jnp.sum(inside, axis=1)
    segment = jnp.sum(inside * seq_ids, axis=1) + (1 - filled) * seq_count
    offset = jnp.sum(inside * (slot_ids - begins[None, :]), axis=1) + (1 - filled) * slot_ids[:, 0]
    return (segment, offset, filled.astype(jnp.float32))


def rotary_tables(offset, head_size):
    half_size = head_size // 2
    frequency = rope_base ** (-(2.0 * jnp.arange(half_size, dtype=jnp.float32)) / head_size)
    angles = offset.astype(jnp.float32)[:, None] * frequency[None, :]
    return (jnp.cos(angles)[:, None, :], jnp.sin(angles)[:, None, :])


def rotate(values, cos_table, sin_table):
    half_size = values.shape[-1] // 2
    first_half = values[..., :half_size]
    second_half = values[..., half_size:]
    return jnp.concatenate(
        [
            first_half * cos_table - second_half * sin_table,
            second_half * cos_table + first_half * sin_table,
        ],
        axis=-1,
    )


def rotate_back(values, cos_table, sin_table):
    half_size = values.shape[-1] // 2
    first_half = values[..., :half_size]
    second_half = values[..., half_size:]
    return jnp.concatenate(
        [
            first_half * cos_table + second_half * sin_table,
            second_half * cos_table - first_half * sin_table,
        ],
        axis=-1,
    )


def inverse_rms(values):
    return lax.rsqrt(jnp.mean(values * values, axis=-1, keepdims=True) + epsilon)


def norm_back(grad_in, values, inverse, gain_vector):
    scaled = grad_in * gain_vector
    return inverse * scaled - values * inverse**3 * jnp.mean(
        scaled * values, axis=-1, keepdims=True
    )


def matmul(left_side, right_side):
    return jnp.dot(left_side, right_side, preferred_element_type=jnp.float32)


def matmul_across(left_side, right_side):
    return lax.dot_general(
        left_side, right_side, (((1,), (1,)), ((), ())), preferred_element_type=jnp.float32
    )


def matmul_rows(left_side, right_side):
    return lax.dot_general(
        left_side, right_side, (((0,), (0,)), ((), ())), preferred_element_type=jnp.float32
    )


def block_scores(block_queries, key_rows, segment, slot_ids, row_start, row_stop, scaling):
    scores = (
        jnp.einsum(
            "qkgd,skd->kgqs", block_queries, key_rows[:row_stop], preferred_element_type=jnp.float32
        )
        * scaling
    )
    allowed = (segment[row_start:row_stop, None] == segment[None, :row_stop]) & (
        slot_ids[None, :row_stop] <= slot_ids[row_start:row_stop, None]
    )
    return jnp.where(allowed, scores, -jnp.inf)


def attend_forward(queries, key_rows, values, segment):
    slot_count, heads_here, head_size = queries.shape
    kv_heads = key_rows.shape[1]
    sharing = heads_here // kv_heads
    block_rows = min(512, slot_count)
    scaling = head_size ** (-0.5)
    slot_ids = jnp.arange(slot_count, dtype=jnp.int32)
    pieces = []
    totals = []
    for block_index in range(slot_count // block_rows):
        row_start = block_index * block_rows
        row_stop = row_start + block_rows
        block_queries = queries[row_start:row_stop].reshape(
            block_rows, kv_heads, sharing, head_size
        )
        scores = block_scores(
            block_queries, key_rows, segment, slot_ids, row_start, row_stop, scaling
        )
        highest_score = jnp.max(scores, axis=-1, keepdims=True)
        exponent = jnp.exp(scores - highest_score)
        denominator = jnp.sum(exponent, axis=-1, keepdims=True)
        weights = (exponent / denominator).astype(jnp.bfloat16)
        block_out = jnp.einsum(
            "kgqs,skd->qkgd", weights, values[:row_stop], preferred_element_type=jnp.float32
        )
        pieces.append(block_out.astype(jnp.bfloat16).reshape(block_rows, heads_here * head_size))
        totals.append(highest_score + jnp.log(denominator))
    return (jnp.concatenate(pieces, axis=0), jnp.concatenate(totals, axis=2))


def attend_backward(queries, key_rows, values, out_grad, totals, segment):
    slot_count, heads_here, head_size = queries.shape
    kv_heads = key_rows.shape[1]
    sharing = heads_here // kv_heads
    block_rows = min(512, slot_count)
    scaling = head_size ** (-0.5)
    slot_ids = jnp.arange(slot_count, dtype=jnp.int32)
    query_parts = []
    key_back = jnp.zeros(key_rows.shape, jnp.float32)
    value_back = jnp.zeros(values.shape, jnp.float32)
    for block_index in range(slot_count // block_rows):
        row_start = block_index * block_rows
        row_stop = row_start + block_rows
        block_queries = queries[row_start:row_stop].reshape(
            block_rows, kv_heads, sharing, head_size
        )
        block_grad = out_grad[row_start:row_stop].reshape(block_rows, kv_heads, sharing, head_size)
        scores = block_scores(
            block_queries, key_rows, segment, slot_ids, row_start, row_stop, scaling
        )
        probability = jnp.exp(scores - totals[:, :, row_start:row_stop])
        prob_low = probability.astype(jnp.bfloat16)
        prob_grad = jnp.einsum(
            "qkgd,skd->kgqs", block_grad, values[:row_stop], preferred_element_type=jnp.float32
        )
        score_low = (
            probability * (prob_grad - jnp.sum(probability * prob_grad, axis=-1, keepdims=True))
        ).astype(jnp.bfloat16)
        query_block = (
            jnp.einsum(
                "kgqs,skd->qkgd", score_low, key_rows[:row_stop], preferred_element_type=jnp.float32
            )
            * scaling
        )
        query_parts.append(query_block.reshape(block_rows, heads_here, head_size))
        key_back = key_back.at[:row_stop].add(
            jnp.einsum(
                "kgqs,qkgd->skd", score_low, block_queries, preferred_element_type=jnp.float32
            )
            * scaling
        )
        value_back = value_back.at[:row_stop].add(
            jnp.einsum("kgqs,qkgd->skd", prob_low, block_grad, preferred_element_type=jnp.float32)
        )
    return (jnp.concatenate(query_parts, axis=0), key_back, value_back)


def bits_of(count):
    return tuple(range(count.bit_length() - 1))


def positions(count, order):
    places = [0]
    for bit in reversed(order):
        places = places + [place | (1 << bit) for place in places]
    return places


def exchange(array, axis, bit):
    count = lax.axis_size(axis)
    return lax.ppermute(array, axis, [(i, i ^ (1 << bit)) for i in range(count)])


def relative(array, axis, order):
    count = lax.axis_size(axis)
    rows = array.shape[0] // count
    index = lax.axis_index(axis)
    return jnp.concatenate(
        [
            lax.dynamic_slice_in_dim(array, (index ^ place) * rows, rows, 0)
            for place in positions(count, order)
        ],
        axis=0,
    )


def scatter_sum(keep, send, axis, order):
    for step, bit in enumerate(order):
        total = keep.astype(jnp.float32) + exchange(send, axis, bit).astype(jnp.float32)
        half = total.shape[0] // 2
        if step + 1 < len(order):
            keep = total[:half]
            send = total[half:].astype(jnp.bfloat16)
    return total


def sum_all(array):
    for axis in ("tensor", "dp"):
        for bit in bits_of(lax.axis_size(axis)):
            array = array + exchange(array, axis, bit)
    return array


def flip(index, mask):
    result = index
    bit = 0
    while mask >> bit:
        if (mask >> bit) & 1:
            result = result + (1 << bit) * (1 - 2 * lax.rem(lax.div(index, 1 << bit), 2))
        bit += 1
    return result


def span(start, size, step=16):
    return pl.ds(pl.multiple_of(start, step), size)


def greet(peers):
    barrier = pltpu.get_barrier_semaphore()
    for axis, bit in peers:
        index = lax.axis_index(axis)
        pl.semaphore_signal(
            barrier, inc=1, device_id={axis: flip(index, 1 << bit)}, device_id_type=MESH
        )
    pl.semaphore_wait(barrier, len(peers))


def chunk_rows(rows):
    for size in (64, 48, 32, 16):
        if rows % size == 0:
            return size
    return rows


class Reduce:
    def __init__(self, part, sums, landing, send_sems, recv_sems, axis, order, split=1):
        self.part, self.sums, self.landing = part, sums, landing
        self.send_sems, self.recv_sems = send_sems, recv_sems
        self.axis, self.order, self.split = axis, order, split
        self.index = lax.axis_index(axis)
        self.rows = part.shape[0] >> len(order)
        self.piece = self.rows // split
        self.copies = {}
        self.lists = []
        base = 0
        for step in range(len(order)):
            kept = [0]
            for bit in reversed(order[step + 1 :]):
                kept = [place | (1 << bit) for place in kept] + kept
            self.lists.append((kept, base))
            base += len(kept) * split

    @staticmethod
    def slots(count, split=1):
        return (count - 1) * split

    def cut(self, c):
        return pl.ds(c * self.piece, self.piece)

    def units(self, step):
        kept, _ = self.lists[step]
        return [(j, c) for j in range(len(kept)) for c in range(self.split)]

    def start(self, step, j, c=0):
        kept, base = self.lists[step]
        mask = 1 << self.order[step]
        slot = base + j * self.split + c
        if step == 0:
            first = flip(self.index, kept[j] | mask) * self.rows + c * self.piece
            source = self.part.at[span(first, self.piece)]
        else:
            source = self.sums.at[self.lists[0][0].index(kept[j] | mask), self.cut(c)]
        copy = pltpu.make_async_remote_copy(
            src_ref=source,
            dst_ref=self.landing.at[slot],
            send_sem=self.send_sems.at[slot],
            recv_sem=self.recv_sems.at[slot],
            device_id={self.axis: flip(self.index, mask)},
            device_id_type=MESH,
        )
        copy.start()
        self.copies[slot] = copy

    def arrive(self, step, j, c=0, store=None):
        kept, base = self.lists[step]
        slot = base + j * self.split + c
        self.copies[slot].wait_recv()
        start = flip(self.index, kept[j]) * self.rows + c * self.piece
        size = chunk_rows(self.piece)

        spot = self.lists[0][0].index(kept[j])

        def add(i, carry):
            here = span(c * self.piece + i * size, size)
            if step == 0:
                own = self.part[span(start + i * size, size)]
            else:
                own = self.sums[spot, here]
            other = self.landing[slot, span(i * size, size)]
            total = own.astype(jnp.float32) + other.astype(jnp.float32)
            if store is None:
                self.sums[spot, here] = total.astype(self.sums.dtype)
            else:
                store(c * self.piece + i * size, size, total)
            return carry

        lax.fori_loop(0, self.piece // size, add, 0)
        if step + 1 < len(self.order):
            later, _ = self.lists[step + 1]
            mask = 1 << self.order[step + 1]
            if kept[j] & mask:
                self.start(step + 1, later.index(kept[j] ^ mask), c)

    def start_all(self):
        for j, c in self.units(0):
            self.start(0, j, c)

    def arrive_all(self, step, store=None):
        for j, c in self.units(step):
            self.arrive(step, j, c, store)

    def close(self):
        for copy in self.copies.values():
            copy.wait_send()


class Gather:
    def __init__(self, whole, send_sems, recv_sems, split=1):
        self.whole, self.split = whole, split
        self.send_sems, self.recv_sems = send_sems, recv_sems
        self.index = lax.axis_index("tensor")
        self.rows = whole.shape[0] // 4
        self.piece = self.rows // split
        self.copies = {}

    def send(self, kind, c):
        mask = (2, 1, 1)[kind]
        block = flip(self.index, 2) if kind == 2 else self.index
        rows = span(block * self.rows + c * self.piece, self.piece)
        slot = kind * self.split + c
        copy = pltpu.make_async_remote_copy(
            src_ref=self.whole.at[rows],
            dst_ref=self.whole.at[rows],
            send_sem=self.send_sems.at[slot],
            recv_sem=self.recv_sems.at[slot],
            device_id={"tensor": flip(self.index, mask)},
            device_id_type=MESH,
        )
        copy.start()
        self.copies[kind, c] = copy

    def start(self, c):
        self.send(0, c)
        self.send(1, c)

    def forward(self, c):
        self.copies[0, c].wait_recv()
        self.send(2, c)

    def finish(self, c):
        self.copies[1, c].wait_recv()
        self.copies[2, c].wait_recv()

    def close(self):
        for copy in self.copies.values():
            copy.wait_send()


TENSOR_PEERS = (("tensor", 0), ("tensor", 1))
SPLIT = 4


def middle_kernel(
    o_ref, w_ref, x_ref, gain_ref, m_ref, h_ref, part, sums, landing, rs_send, rs_recv, ag_send, ag_recv
):
    index = lax.axis_index("tensor")
    rows = o_ref.shape[0] // 4
    greet(TENSOR_PEERS)
    reduce = Reduce(part, sums, landing, rs_send, rs_recv, "tensor", (0, 1), SPLIT)
    gather = Gather(m_ref, ag_send, ag_recv, SPLIT)

    def product(place):
        block = span(flip(index, place) * rows, rows)
        columns = 512

        def tile(i, carry):
            cols = pl.ds(pl.multiple_of(i * columns, columns), columns)
            part[block, cols] = lax.dot_general(
                o_ref[block],
                w_ref[cols],
                (((1,), (1,)), ((), ())),
                preferred_element_type=jnp.float32,
            ).astype(jnp.bfloat16)
            return carry

        lax.fori_loop(0, part.shape[1] // columns, tile, 0)

    def normed(start, size, total):
        own = span(start, size)
        hidden = x_ref[own].astype(jnp.float32) + total
        h_ref[own] = hidden
        inverse = lax.rsqrt(jnp.mean(hidden * hidden, axis=-1, keepdims=True) + epsilon)
        m_ref[span(index * rows + start, size)] = (hidden * inverse * gain_ref[...]).astype(
            jnp.bfloat16
        )

    for j, (place, _) in enumerate(((3, 0), (1, 0))):
        product(place)
        for c in range(SPLIT):
            reduce.start(0, j, c)
    product(2)
    for c in range(SPLIT):
        reduce.arrive(0, 0, c)
    product(0)
    for c in range(SPLIT):
        reduce.arrive(0, 1, c)
    for c in range(SPLIT):
        reduce.arrive(1, 0, c, normed)
        gather.start(c)
    for c in range(SPLIT):
        gather.forward(c)
    for c in range(SPLIT):
        gather.finish(c)
    reduce.close()
    gather.close()


def vmem_specs(count):
    return [pl.BlockSpec(memory_space=pltpu.VMEM)] * count


def dma_sems(count):
    return [pltpu.SemaphoreType.DMA((count,)), pltpu.SemaphoreType.DMA((count,))]


def middle_call(attended, mixing_weight, token_share, second_gain):
    slots, width = attended.shape[0], mixing_weight.shape[0]
    rows = slots // 4
    count = Reduce.slots(4, SPLIT)
    return pl.pallas_call(
        middle_kernel,
        out_shape=(
            jax.ShapeDtypeStruct((slots, width), jnp.bfloat16),
            jax.ShapeDtypeStruct((rows, width), jnp.float32),
        ),
        in_specs=vmem_specs(4),
        out_specs=tuple(vmem_specs(2)),
        scratch_shapes=[
            pltpu.VMEM((slots, width), jnp.bfloat16),
            pltpu.VMEM((2, rows, width), jnp.bfloat16),
            pltpu.VMEM((count, rows // SPLIT, width), jnp.bfloat16),
            *dma_sems(count),
            *dma_sems(3 * SPLIT),
        ],
        compiler_params=pltpu.CompilerParams(
            collective_id=0, has_side_effects=True, vmem_limit_bytes=48 << 20
        ),
        name="middle",
    )(attended, mixing_weight, token_share, second_gain.reshape(1, -1))


def back_kernel(
    dp_order,
    z_order,
    dm_part,
    feed_part,
    down_part,
    gate_part,
    up_part,
    h_ref,
    cot_ref,
    live_ref,
    gain_ref,
    out_ref,
    ga_ref,
    dh_ref,
    term_ref,
    down_ref,
    gate_ref,
    up_ref,
    *scratch,
):
    index = lax.axis_index("tensor")
    rows = h_ref.shape[0]
    (dm_sum, feed_sum, down_sum, gate_sum, up_sum, *scratch) = scratch
    (dm_land, feed_land, down_land, gate_land, up_land, *sems) = scratch
    greet(TENSOR_PEERS + tuple(("dp", bit) for bit in dp_order))
    dm = Reduce(dm_part, dm_sum, dm_land, sems[0], sems[1], "tensor", (0, 1), SPLIT)
    feed = Reduce(feed_part, feed_sum, feed_land, sems[2], sems[3], "tensor", (0, 1), SPLIT)
    gather = Gather(ga_ref, sems[4], sems[5], SPLIT)
    down = Reduce(down_part, down_sum, down_land, sems[6], sems[7], "dp", z_order)
    gate = Reduce(gate_part, gate_sum, gate_land, sems[8], sems[9], "dp", dp_order)
    up = Reduce(up_part, up_sum, up_land, sems[10], sems[11], "dp", dp_order)
    width = h_ref.shape[1]
    term_ref[...] = jnp.zeros_like(term_ref)

    def finish_out(start, size, total):
        own = span(start, size)
        out_ref[own] = ((h_ref[own] + total) * live_ref[own]).astype(jnp.bfloat16)

    def finish_dm(start, size, total):
        own = span(start, size)
        hidden = h_ref[own]
        inverse = lax.rsqrt(jnp.mean(hidden * hidden, axis=-1, keepdims=True) + epsilon)
        scaled = total * gain_ref[...]
        inner = jnp.mean(scaled * hidden, axis=-1, keepdims=True)
        grad = (
            cot_ref[own].astype(jnp.float32) * live_ref[own]
            + inverse * scaled
            - hidden * (inverse * inverse * inverse) * inner
        )
        dh_ref[own] = grad
        ga_ref[span(index * rows + start, size)] = grad.astype(jnp.bfloat16)
        term_ref[...] += jnp.sum(total * hidden * inverse, axis=0, keepdims=True)

    def place(ref):
        def store(start, size, total):
            ref[span(start, size)] = total

        return store

    dm.start_all()
    feed.start_all()
    down.start_all()
    gate.start_all()
    up.start_all()
    dm.arrive_all(0)
    feed_first = feed.units(0)
    for j, c in feed_first[len(feed_first) // 2 :]:
        feed.arrive(0, j, c)
    half = down.units(0)[: len(down.units(0)) // 2]
    rest = down.units(0)[len(down.units(0)) // 2 :]
    for j, c in half:
        gate.arrive(0, j, c)
        down.arrive(0, j, c)
    for c in range(SPLIT):
        dm.arrive(1, 0, c, finish_dm)
        gather.start(c)
    for j, c in feed_first[: len(feed_first) // 2]:
        feed.arrive(0, j, c)
    for j, c in rest:
        gate.arrive(0, j, c)
        down.arrive(0, j, c)
    for c in range(SPLIT):
        gather.forward(c)
    for c in range(SPLIT):
        gather.finish(c)
    last = len(dp_order) - 1
    for step in range(1, last):
        for j, c in gate.units(step):
            gate.arrive(step, j, c)
    up.arrive_all(0)
    feed.arrive_all(1, finish_out)
    for step in range(1, last):
        for j, c in up.units(step):
            up.arrive(step, j, c)
            down.arrive(step, j, c)
    gate.arrive_all(last, place(gate_ref))
    up.arrive_all(last, place(up_ref))
    down.arrive_all(last, place(down_ref))
    for item in (dm, feed, gather, down, gate, up):
        item.close()


def back_call(
    dm_part, feed_part, down_part, gate_part, up_part, middle, cotangent, live, second_gain
):
    slots, width = dm_part.shape
    rows = slots // 4
    columns = down_part.shape[1]
    count = lax.axis_size("dp")
    dp_order = bits_of(count)
    z_order = (dp_order[1], dp_order[0]) + dp_order[2:]
    block = width // count
    share = Reduce.slots(4, SPLIT)
    total = Reduce.slots(count)

    def kernel(*refs):
        back_kernel(dp_order, z_order, *refs)

    grad = jax.ShapeDtypeStruct((block, columns), jnp.float32)
    return pl.pallas_call(
        kernel,
        out_shape=(
            jax.ShapeDtypeStruct((rows, width), jnp.bfloat16),
            jax.ShapeDtypeStruct((slots, width), jnp.bfloat16),
            jax.ShapeDtypeStruct((rows, width), jnp.float32),
            jax.ShapeDtypeStruct((1, width), jnp.float32),
            grad,
            grad,
            grad,
        ),
        in_specs=vmem_specs(9),
        out_specs=tuple(vmem_specs(7)),
        scratch_shapes=[
            pltpu.VMEM((2, rows, width), jnp.bfloat16),
            pltpu.VMEM((2, rows, width), jnp.bfloat16),
            pltpu.VMEM((count // 2, block, columns), jnp.bfloat16),
            pltpu.VMEM((count // 2, block, columns), jnp.bfloat16),
            pltpu.VMEM((count // 2, block, columns), jnp.bfloat16),
            pltpu.VMEM((share, rows // SPLIT, width), jnp.bfloat16),
            pltpu.VMEM((share, rows // SPLIT, width), jnp.bfloat16),
            pltpu.VMEM((total, block, columns), jnp.bfloat16),
            pltpu.VMEM((total, block, columns), jnp.bfloat16),
            pltpu.VMEM((total, block, columns), jnp.bfloat16),
            *dma_sems(share),
            *dma_sems(share),
            *dma_sems(3 * SPLIT),
            *dma_sems(total),
            *dma_sems(total),
            *dma_sems(total),
        ],
        compiler_params=pltpu.CompilerParams(
            collective_id=1, has_side_effects=True, vmem_limit_bytes=60 << 20
        ),
        name="back",
    )(
        dm_part,
        feed_part,
        down_part,
        gate_part,
        up_part,
        middle,
        cotangent,
        live,
        second_gain.reshape(1, -1),
    )


def on_device(
    tokens,
    lengths,
    owners,
    first_gain,
    query_weight,
    key_weight,
    value_weight,
    mixing_weight,
    second_gain,
    gate_weight,
    up_weight,
    down_weight,
    cotangent,
):
    slot_count = tokens.shape[0]
    tensor_count = lax.axis_size("tensor")
    share_rows = slot_count // tensor_count
    share_start = lax.axis_index("tensor") * share_rows
    t_order = bits_of(tensor_count)
    d_order = bits_of(lax.axis_size("dp"))
    z_order = (d_order[1], d_order[0]) + d_order[2:]

    def share_of(array):
        return lax.dynamic_slice_in_dim(array, share_start, share_rows, 0)

    def rows_relative(array):
        return relative(array, "tensor", t_order)

    def columns_first(array, order):
        return relative(array.T, "dp", order)

    def row_sum(make, array):
        half = array.shape[0] // 2
        send = make(array[half:]).astype(jnp.bfloat16)
        keep = make(array[:half]).astype(jnp.bfloat16)
        return scatter_sum(keep, send, "tensor", t_order)

    def weight_sum(left, right, order):
        half = left.shape[0] // 2
        send = matmul(left[half:], right).astype(jnp.bfloat16)
        keep = matmul(left[:half], right).astype(jnp.bfloat16)
        return scatter_sum(keep, send, "dp", order)

    segment, offset, filled = slot_layout(lengths, owners, lax.axis_index("dp"), slot_count)
    head_size = HD
    cos_table, sin_table = rotary_tables(offset, head_size)
    inputs = tokens.astype(jnp.float32)
    first_inv = inverse_rms(inputs)
    first_in = (inputs * first_inv * first_gain).astype(jnp.bfloat16)
    queries = rotate(
        matmul(first_in, query_weight).reshape(slot_count, -1, head_size), cos_table, sin_table
    ).astype(jnp.bfloat16)
    key_rows = rotate(
        matmul(first_in, key_weight).reshape(slot_count, -1, head_size), cos_table, sin_table
    ).astype(jnp.bfloat16)
    values = matmul(first_in, value_weight).astype(jnp.bfloat16).reshape(slot_count, -1, head_size)
    attended, log_totals = attend_forward(queries, key_rows, values, segment)
    inputs_share = share_of(inputs)
    first_inv_share = share_of(first_inv)
    second_in, middle = middle_call(attended, mixing_weight, share_of(tokens), second_gain)
    gate_value = matmul(second_in, gate_weight)
    upward = matmul(second_in, up_weight)
    sigmoid = jax.nn.sigmoid(gate_value)
    activated = gate_value * sigmoid
    hidden = (activated * upward).astype(jnp.bfloat16)
    live_share = share_of(filled)[:, None]
    feed_part = matmul_across(hidden, down_weight).astype(jnp.bfloat16)
    outer_low = cotangent * filled[:, None].astype(jnp.bfloat16)
    hidden_grad = matmul(outer_low, down_weight)
    gate_low = (hidden_grad * upward * sigmoid * (1.0 + gate_value * (1.0 - sigmoid))).astype(
        jnp.bfloat16
    )
    upward_low = (hidden_grad * activated).astype(jnp.bfloat16)
    second_part = (
        matmul_across(gate_low, gate_weight) + matmul_across(upward_low, up_weight)
    ).astype(jnp.bfloat16)
    down_part = matmul_rows(outer_low, hidden).astype(jnp.bfloat16)
    gate_part = matmul_rows(second_in, gate_low).astype(jnp.bfloat16)
    up_part = matmul_rows(second_in, upward_low).astype(jnp.bfloat16)
    layer_output, branch_low, middle_grad, second_term, down_grad, gate_grad, up_grad = back_call(
        second_part,
        feed_part,
        down_part,
        gate_part,
        up_part,
        middle,
        share_of(cotangent),
        live_share,
        second_gain,
    )
    second_term = second_term[0]
    mixing_grad = weight_sum(columns_first(branch_low, z_order), attended, z_order)
    attended_grad = matmul(branch_low, mixing_weight).astype(jnp.bfloat16)
    query_back, key_back, value_back = attend_backward(
        queries, key_rows, values, attended_grad, log_totals, segment
    )
    query_low = (
        rotate_back(query_back, cos_table, sin_table).astype(jnp.bfloat16).reshape(slot_count, -1)
    )
    key_low = (
        rotate_back(key_back, cos_table, sin_table).astype(jnp.bfloat16).reshape(slot_count, -1)
    )
    value_low = value_back.astype(jnp.bfloat16).reshape(slot_count, -1)
    projected_low = jnp.concatenate([query_low, key_low, value_low], axis=1)
    projection = jnp.concatenate([query_weight, key_weight, value_weight], axis=1)
    first_back = row_sum(
        lambda rows: matmul_across(rows, projection), rows_relative(projected_low)
    )
    projection_grad = weight_sum(columns_first(first_in, d_order), projected_low, d_order)
    token_grad = middle_grad + norm_back(first_back, inputs_share, first_inv_share, first_gain)
    first_term = jnp.sum(first_back * inputs_share * first_inv_share, axis=0)
    first_grad, second_grad = sum_all(jnp.stack([first_term, second_term]))
    query_columns = query_weight.shape[1]
    key_columns = query_columns + key_weight.shape[1]
    return (
        layer_output,
        token_grad.astype(jnp.bfloat16),
        first_grad,
        projection_grad[:, :query_columns],
        projection_grad[:, query_columns:key_columns],
        projection_grad[:, key_columns:],
        mixing_grad,
        second_grad,
        gate_grad,
        up_grad,
        down_grad,
    )


def solution(mesh):
    in_specs = (
        P("dp", None),
        P(),
        P(),
        P(),
        P(None, "tensor"),
        P(None, "tensor"),
        P(None, "tensor"),
        P(None, "tensor"),
        P(),
        P(None, "tensor"),
        P(None, "tensor"),
        P(None, "tensor"),
        P("dp", None),
    )
    out_specs = (
        P(("dp", "tensor"), None),
        P(("dp", "tensor"), None),
        P(),
        P("dp", "tensor"),
        P("dp", "tensor"),
        P("dp", "tensor"),
        P("dp", "tensor"),
        P(),
        P("dp", "tensor"),
        P("dp", "tensor"),
        P("dp", "tensor"),
    )
    return jax.shard_map(
        on_device, mesh=mesh, in_specs=in_specs, out_specs=out_specs, check_vma=False
    )
```

```python
import jax
import jax.numpy as jnp
from jax import lax
from jax.experimental import pallas as pl
from jax.experimental.pallas import tpu as pltpu
from jax.sharding import PartitionSpec as P

HD = 96

MESH = pl.DeviceIdType.MESH

epsilon = 1e-05
rope_base = 10000.0


def slot_layout(lengths, owners, device, slot_count):
    seq_count = lengths.shape[0]
    chosen = owners == device
    taken_len = jnp.where(chosen, lengths, 0)
    finish = jnp.cumsum(taken_len)
    begins = finish - taken_len
    slot_ids = jnp.arange(slot_count, dtype=jnp.int32)[:, None]
    inside = (
        chosen[None, :] & (slot_ids >= begins[None, :]) & (slot_ids < finish[None, :])
    ).astype(jnp.int32)
    seq_ids = jnp.arange(seq_count, dtype=jnp.int32)[None, :]
    filled = jnp.sum(inside, axis=1)
    segment = jnp.sum(inside * seq_ids, axis=1) + (1 - filled) * seq_count
    offset = jnp.sum(inside * (slot_ids - begins[None, :]), axis=1) + (1 - filled) * slot_ids[:, 0]
    return (segment, offset, filled.astype(jnp.float32))


def rotary_tables(offset, head_size):
    half_size = head_size // 2
    frequency = rope_base ** (-(2.0 * jnp.arange(half_size, dtype=jnp.float32)) / head_size)
    angles = offset.astype(jnp.float32)[:, None] * frequency[None, :]
    return (jnp.cos(angles)[:, None, :], jnp.sin(angles)[:, None, :])


def rotate(values, cos_table, sin_table):
    half_size = values.shape[-1] // 2
    first_half = values[..., :half_size]
    second_half = values[..., half_size:]
    return jnp.concatenate(
        [
            first_half * cos_table - second_half * sin_table,
            second_half * cos_table + first_half * sin_table,
        ],
        axis=-1,
    )


def inverse_rms(values):
    return lax.rsqrt(jnp.mean(values * values, axis=-1, keepdims=True) + epsilon)


def matmul(left_side, right_side):
    return jnp.dot(left_side, right_side, preferred_element_type=jnp.float32)


def matmul_across(left_side, right_side):
    return lax.dot_general(
        left_side, right_side, (((1,), (1,)), ((), ())), preferred_element_type=jnp.float32
    )


def bits_of(count):
    return tuple(range(count.bit_length() - 1))


def flip(index, mask):
    result = index
    bit = 0
    while mask >> bit:
        if (mask >> bit) & 1:
            result = result + (1 << bit) * (1 - 2 * lax.rem(lax.div(index, 1 << bit), 2))
        bit += 1
    return result


def span(start, size, step=16):
    return pl.ds(pl.multiple_of(start, step), size)


def greet(peers):
    barrier = pltpu.get_barrier_semaphore()
    for axis, bit in peers:
        index = lax.axis_index(axis)
        pl.semaphore_signal(
            barrier, inc=1, device_id={axis: flip(index, 1 << bit)}, device_id_type=MESH
        )
    pl.semaphore_wait(barrier, len(peers))


def chunk_rows(rows):
    for size in (64, 48, 32, 16):
        if rows % size == 0:
            return size
    return rows


class Reduce:
    def __init__(self, part, landing, send_sems, recv_sems, axis, order, split=1):
        self.part, self.landing = part, landing
        self.send_sems, self.recv_sems = send_sems, recv_sems
        self.axis, self.order, self.split = axis, order, split
        self.index = lax.axis_index(axis)
        self.rows = part.shape[0] >> len(order)
        self.piece = self.rows // split
        self.copies = {}
        self.lists = []
        base = 0
        for step in range(len(order)):
            kept = [0]
            for bit in reversed(order[step + 1 :]):
                kept = [place | (1 << bit) for place in kept] + kept
            self.lists.append((kept, base))
            base += len(kept) * split

    @staticmethod
    def slots(count, split=1):
        return (count - 1) * split

    def units(self, step):
        kept, _ = self.lists[step]
        return [(j, c) for j in range(len(kept)) for c in range(self.split)]

    def start(self, step, j, c=0):
        kept, base = self.lists[step]
        mask = 1 << self.order[step]
        slot = base + j * self.split + c
        source = flip(self.index, kept[j] | mask) * self.rows + c * self.piece
        copy = pltpu.make_async_remote_copy(
            src_ref=self.part.at[span(source, self.piece)],
            dst_ref=self.landing.at[slot],
            send_sem=self.send_sems.at[slot],
            recv_sem=self.recv_sems.at[slot],
            device_id={self.axis: flip(self.index, mask)},
            device_id_type=MESH,
        )
        copy.start()
        self.copies[slot] = copy

    def arrive(self, step, j, c=0, store=None):
        kept, base = self.lists[step]
        slot = base + j * self.split + c
        self.copies[slot].wait_recv()
        start = flip(self.index, kept[j]) * self.rows + c * self.piece
        size = chunk_rows(self.piece)

        def add(i, carry):
            rows = span(start + i * size, size)
            other = self.landing[slot, span(i * size, size)]
            total = self.part[rows].astype(jnp.float32) + other.astype(jnp.float32)
            if store is None:
                self.part[rows] = total.astype(self.part.dtype)
            else:
                store(c * self.piece + i * size, size, total)
            return carry

        lax.fori_loop(0, self.piece // size, add, 0)
        if step + 1 < len(self.order):
            later, _ = self.lists[step + 1]
            mask = 1 << self.order[step + 1]
            if kept[j] & mask:
                self.start(step + 1, later.index(kept[j] ^ mask), c)

    def start_all(self):
        for j, c in self.units(0):
            self.start(0, j, c)

    def arrive_all(self, step, store=None):
        for j, c in self.units(step):
            self.arrive(step, j, c, store)

    def close(self):
        for copy in self.copies.values():
            copy.wait_send()


class Gather:
    def __init__(self, whole, send_sems, recv_sems, split=1):
        self.whole, self.split = whole, split
        self.send_sems, self.recv_sems = send_sems, recv_sems
        self.index = lax.axis_index("tensor")
        self.rows = whole.shape[0] // 4
        self.piece = self.rows // split
        self.copies = {}

    def send(self, kind, c):
        mask = (2, 1, 1)[kind]
        block = flip(self.index, 2) if kind == 2 else self.index
        rows = span(block * self.rows + c * self.piece, self.piece)
        slot = kind * self.split + c
        copy = pltpu.make_async_remote_copy(
            src_ref=self.whole.at[rows],
            dst_ref=self.whole.at[rows],
            send_sem=self.send_sems.at[slot],
            recv_sem=self.recv_sems.at[slot],
            device_id={"tensor": flip(self.index, mask)},
            device_id_type=MESH,
        )
        copy.start()
        self.copies[kind, c] = copy

    def start(self, c):
        self.send(0, c)
        self.send(1, c)

    def forward(self, c):
        self.copies[0, c].wait_recv()
        self.send(2, c)

    def finish(self, c):
        self.copies[1, c].wait_recv()
        self.copies[2, c].wait_recv()

    def close(self):
        for copy in self.copies.values():
            copy.wait_send()


TENSOR_PEERS = (("tensor", 0), ("tensor", 1))
SPLIT = 4


def middle_kernel(
    o_ref, w_ref, x_ref, gain_ref, m_ref, h_ref, part, landing, rs_send, rs_recv, ag_send, ag_recv
):
    index = lax.axis_index("tensor")
    rows = o_ref.shape[0] // 4
    greet(TENSOR_PEERS)
    reduce = Reduce(part, landing, rs_send, rs_recv, "tensor", (0, 1), SPLIT)
    gather = Gather(m_ref, ag_send, ag_recv, SPLIT)

    def product(place):
        block = span(flip(index, place) * rows, rows)
        columns = 512

        def tile(i, carry):
            cols = pl.ds(pl.multiple_of(i * columns, columns), columns)
            part[block, cols] = lax.dot_general(
                o_ref[block],
                w_ref[cols],
                (((1,), (1,)), ((), ())),
                preferred_element_type=jnp.float32,
            ).astype(jnp.bfloat16)
            return carry

        lax.fori_loop(0, part.shape[1] // columns, tile, 0)

    def normed(start, size, total):
        own = span(start, size)
        hidden = x_ref[own].astype(jnp.float32) + total
        h_ref[own] = hidden
        inverse = lax.rsqrt(jnp.mean(hidden * hidden, axis=-1, keepdims=True) + epsilon)
        m_ref[span(index * rows + start, size)] = (hidden * inverse * gain_ref[...]).astype(
            jnp.bfloat16
        )

    for j, (place, _) in enumerate(((3, 0), (1, 0))):
        product(place)
        for c in range(SPLIT):
            reduce.start(0, j, c)
    product(2)
    for c in range(SPLIT):
        reduce.arrive(0, 0, c)
    product(0)
    for c in range(SPLIT):
        reduce.arrive(0, 1, c)
    for c in range(SPLIT):
        reduce.arrive(1, 0, c, normed)
        gather.start(c)
    for c in range(SPLIT):
        gather.forward(c)
    for c in range(SPLIT):
        gather.finish(c)
    reduce.close()
    gather.close()


def vmem_specs(count):
    return [pl.BlockSpec(memory_space=pltpu.VMEM)] * count


def dma_sems(count):
    return [pltpu.SemaphoreType.DMA((count,)), pltpu.SemaphoreType.DMA((count,))]


def middle_call(attended, mixing_weight, token_share, second_gain):
    slots, width = attended.shape[0], mixing_weight.shape[0]
    rows = slots // 4
    count = Reduce.slots(4, SPLIT)
    return pl.pallas_call(
        middle_kernel,
        out_shape=(
            jax.ShapeDtypeStruct((slots, width), jnp.bfloat16),
            jax.ShapeDtypeStruct((rows, width), jnp.float32),
        ),
        in_specs=vmem_specs(4),
        out_specs=tuple(vmem_specs(2)),
        scratch_shapes=[
            pltpu.VMEM((slots, width), jnp.bfloat16),
            pltpu.VMEM((count, rows // SPLIT, width), jnp.bfloat16),
            *dma_sems(count),
            *dma_sems(3 * SPLIT),
        ],
        compiler_params=pltpu.CompilerParams(
            collective_id=0, has_side_effects=True, vmem_limit_bytes=48 << 20
        ),
        name="middle",
    )(attended, mixing_weight, token_share, second_gain.reshape(1, -1))


BLOCK = 256
TILE = 384


def nn(left, right):
    return jnp.dot(left, right, preferred_element_type=jnp.float32)


def nt(left, right):
    return lax.dot_general(left, right, (((1,), (1,)), ((), ())), preferred_element_type=jnp.float32)


def tn(left, right):
    return lax.dot_general(left, right, (((0,), (0,)), ((), ())), preferred_element_type=jnp.float32)


def head(index):
    return pl.ds(index * HD, HD)


def allowed_keys(begin_row, query_start, key_count, query_count):
    keys = lax.broadcasted_iota(jnp.int32, (key_count, query_count), 0)
    queries = query_start + lax.broadcasted_iota(jnp.int32, (key_count, query_count), 1)
    return (keys >= begin_row) & (keys <= queries)


def attention_kernel(q_ref, k_ref, v_ref, begin_ref, o_ref, lse_ref):
    slots = q_ref.shape[0]
    scaling = HD ** (-0.5)
    groups = q_ref.shape[1] // k_ref.shape[1]
    for h in range(q_ref.shape[1] // HD):
        values = v_ref[:, head(h // groups)].T
        for start in range(0, slots, BLOCK):
            stop = start + BLOCK
            rows = pl.ds(start, BLOCK)
            scores = nt(k_ref[pl.ds(0, stop), head(h // groups)], q_ref[rows, head(h)]) * scaling
            allowed = allowed_keys(begin_ref[:, rows], start, stop, BLOCK)
            scores = jnp.where(allowed, scores, -jnp.inf)
            highest = jnp.max(scores, axis=0, keepdims=True)
            exponent = jnp.exp(scores - highest)
            total = jnp.sum(exponent, axis=0, keepdims=True)
            weights = (exponent * (1.0 / total)).astype(jnp.bfloat16)
            o_ref[rows, head(h)] = nn(values[:, :stop], weights).T.astype(jnp.bfloat16)
            lse_ref[pl.ds(h, 1), rows] = highest + jnp.log(total)


def attention_call(queries, key_rows, values, begin):
    slots, width = queries.shape
    return pl.pallas_call(
        attention_kernel,
        out_shape=(
            jax.ShapeDtypeStruct((slots, width), jnp.bfloat16),
            jax.ShapeDtypeStruct((width // HD, slots), jnp.float32),
        ),
        in_specs=vmem_specs(4),
        out_specs=tuple(vmem_specs(2)),
        compiler_params=pltpu.CompilerParams(vmem_limit_bytes=40 << 20),
        name="attention",
    )(queries, key_rows, values, begin)


def attention_back(q_ref, k_ref, v_ref, do_ref, begin_ref, lse_ref, keep, key_sum, value_sum, h, group, first):
    slots = q_ref.shape[0]
    scaling = HD ** (-0.5)
    keys_turned = k_ref[:, head(group)].T
    for start in reversed(range(0, slots, BLOCK)):
        stop = start + BLOCK
        rows = pl.ds(start, BLOCK)
        seen = pl.ds(0, stop)
        query = q_ref[rows, head(h)]
        grad = do_ref[rows, head(h)]
        scores = nt(k_ref[seen, head(group)], query) * scaling
        allowed = allowed_keys(begin_ref[:, rows], start, stop, BLOCK)
        weights = jnp.where(allowed, jnp.exp(scores - lse_ref[pl.ds(h, 1), rows]), 0.0)
        weights_grad = nt(v_ref[seen, head(group)], grad)
        inner = jnp.sum(weights * weights_grad, axis=0, keepdims=True)
        scores_grad = (weights * (weights_grad - inner)).astype(jnp.bfloat16)
        values_part = nn(weights.astype(jnp.bfloat16), grad)
        keys_part = nn(scores_grad, query)
        if first and stop == slots:
            value_sum[...] = values_part
            key_sum[...] = keys_part
        else:
            value_sum[seen] += values_part
            key_sum[seen] += keys_part
        keep(start, nn(keys_turned[:, :stop], scores_grad).T * scaling)


def back_kernel(
    dp_order,
    z_order,
    dm_hbm,
    feed_hbm,
    m_hbm,
    gm_hbm,
    hid_hbm,
    dgate_hbm,
    dup_hbm,
    a_hbm,
    h_ref,
    cot_ref,
    live_ref,
    x_ref,
    gain1_ref,
    gain2_ref,
    mixing_ref,
    weight_ref,
    o_ref,
    q_ref,
    k_ref,
    v_ref,
    begin_ref,
    lse_ref,
    rope_ref,
    out_ref,
    token_ref,
    gains_ref,
    down_ref,
    gate_ref,
    up_ref,
    mix_ref,
    one_ref,
    two_ref,
    *scratch,
):
    (
        wide,
        m_buf,
        hid_buf,
        dgate_buf,
        dup_buf,
        rs_part,
        rs_land,
        ga_buf,
        dh_buf,
        key_sum,
        value_sum,
        gains_land,
        *scratch,
    ) = scratch
    parts, lands, sems = scratch[:6], scratch[6:12], scratch[12:]
    stage, stage_sem, load_sems, credit, *sems = sems
    index = lax.axis_index("tensor")
    dp_index = lax.axis_index("dp")
    count = 1 << len(dp_order)

    loads = [
        pltpu.make_async_copy(source, target, load_sems.at[i])
        for i, (source, target) in enumerate(
            (
                (dm_hbm, rs_part),
                (gm_hbm, wide),
                (hid_hbm, hid_buf),
                (m_hbm, m_buf),
                (dgate_hbm, dgate_buf),
                (dup_hbm, dup_buf),
                (feed_hbm, rs_part),
                (a_hbm, wide),
            )
        )
    ]
    for load in loads[:6]:
        load.start()
    greet(TENSOR_PEERS + tuple(("dp", bit) for bit in dp_order))

    def share_reduce(first_sem):
        return Reduce(rs_part, rs_land, sems[first_sem], sems[first_sem + 1], "tensor", (0, 1), SPLIT)

    dm, feed, da = share_reduce(0), share_reduce(2), share_reduce(4)
    gather = Gather(ga_buf, sems[6], sems[7], SPLIT)
    orders = (z_order, dp_order, dp_order, z_order, dp_order, z_order)
    down, gate, up, mix, one, two = (
        Reduce(parts[i], lands[i], sems[8 + 2 * i], sems[9 + 2 * i], "dp", orders[i])
        for i in range(6)
    )
    gains_send, gains_recv = sems[20], sems[21]
    gains_ref[...] = jnp.zeros_like(gains_ref)

    def finish_out(start, size, total):
        own = span(start, size)
        out_ref[own] = ((h_ref[own] + total) * live_ref[own]).astype(jnp.bfloat16)

    def finish_dm(start, size, total):
        own = span(start, size)
        hidden = h_ref[own]
        inverse = lax.rsqrt(jnp.mean(hidden * hidden, axis=-1, keepdims=True) + epsilon)
        scaled = total * gain2_ref[...]
        inner = jnp.mean(scaled * hidden, axis=-1, keepdims=True)
        grad = (
            cot_ref[own].astype(jnp.float32) * live_ref[own]
            + inverse * scaled
            - hidden * (inverse * inverse * inverse) * inner
        )
        dh_buf[own] = grad
        ga_buf[span(index * dh_buf.shape[0] + start, size)] = grad.astype(jnp.bfloat16)
        gains_ref[pl.ds(1, 1)] += jnp.sum(total * hidden * inverse, axis=0, keepdims=True)

    def finish_da(start, size, total):
        own = span(start, size)
        values = x_ref[own].astype(jnp.float32)
        inverse = lax.rsqrt(jnp.mean(values * values, axis=-1, keepdims=True) + epsilon)
        scaled = total * gain1_ref[...]
        inner = jnp.mean(scaled * values, axis=-1, keepdims=True)
        grad = dh_buf[own] + inverse * scaled - values * (inverse * inverse * inverse) * inner
        token_ref[own] = grad.astype(jnp.bfloat16)
        gains_ref[pl.ds(0, 1)] += jnp.sum(total * values * inverse, axis=0, keepdims=True)

    flying = []

    def settle():
        for copy in flying:
            copy.wait()
        flying.clear()

    def finish_grad(reduce, target):
        settle()
        columns = pl.ds(0, reduce.part.shape[1])

        def store(start, size, total):
            stage[span(start, size), columns] = total

        reduce.arrive_all(last, store)
        copy = pltpu.make_async_copy(stage.at[:, columns], target, stage_sem)
        copy.start()
        flying.append(copy)

    def grad_tile(left, right, columns, reduce, which):
        blocks = TILE // reduce.rows
        tile = flip(lax.div(dp_index, blocks), which) * TILE
        cols = pl.ds(pl.multiple_of(tile, 128), TILE)
        width = columns.stop - columns.start
        step = min(width, 512)

        def some(i, carry):
            there = pl.ds(pl.multiple_of(i * step, 128), step)
            here = pl.ds(pl.multiple_of(columns.start + i * step, 128), step)
            reduce.part[span(tile, TILE), there] = tn(left[:, cols], right[:, here]).astype(
                jnp.bfloat16
            )
            return carry

        lax.fori_loop(0, width // step, some, 0)
        kept, _ = reduce.lists[0]
        for j, kept_place in enumerate(kept):
            if (kept_place | (1 << reduce.order[0])) // blocks == which:
                reduce.start(0, j)

    tiles = (3, 1, 2, 0)
    wide_columns = slice(0, hid_buf.shape[1])

    loads[0].wait()
    dm.start_all()
    loads[1].wait()
    loads[2].wait()
    for which in tiles[:2]:
        grad_tile(wide, hid_buf, wide_columns, down, which)
    dm.arrive_all(0)
    for which in tiles[2:]:
        grad_tile(wide, hid_buf, wide_columns, down, which)
    loads[7].start()
    loads[3].wait()
    loads[4].wait()
    for which in tiles:
        grad_tile(m_buf, dgate_buf, wide_columns, gate, which)
    loads[5].wait()
    for i, which in enumerate(tiles):
        dm.arrive(1, 0, i, finish_dm)
        gather.start(i)
        grad_tile(m_buf, dup_buf, wide_columns, up, which)
    dm.close()
    loads[6].start()
    half = count // 4
    for i in range(half):
        down.arrive(0, i)
        gate.arrive(0, i)
    for c in range(SPLIT):
        gather.forward(c)
    for i in range(half, count // 2):
        down.arrive(0, i)
        gate.arrive(0, i)
    for c in range(SPLIT):
        gather.finish(c)
    loads[6].wait()
    feed.start_all()
    narrow = slice(0, o_ref.shape[1])
    for which in tiles:
        grad_tile(ga_buf, o_ref, narrow, mix, which)
    for start in range(0, ga_buf.shape[0], BLOCK):
        rows = pl.ds(start, BLOCK)
        hid_buf[rows, narrow] = nn(ga_buf[rows], mixing_ref[...]).astype(jnp.bfloat16)
    feed.arrive_all(0)

    queries_each = q_ref.shape[1] // k_ref.shape[1]
    scaling = HD ** (-0.5)

    def turned_back(values, rows):
        half = HD // 2
        cosine, sine = rope_ref[rows, pl.ds(0, half)], rope_ref[rows, pl.ds(half, half)]
        first, second = values[:, :half], values[:, half:]
        return jnp.concatenate(
            [first * cosine + second * sine, second * cosine - first * sine], axis=1
        )

    def group_back(group, meanwhile):
        base = group * TILE

        for each in range(queries_each):

            def keep(start, values, each=each):
                rows = pl.ds(start, BLOCK)
                dgate_buf[rows, pl.ds(base + each * HD, HD)] = turned_back(values, rows).astype(
                    jnp.bfloat16
                )

            attention_back(
                q_ref,
                k_ref,
                v_ref,
                hid_buf,
                begin_ref,
                lse_ref,
                keep,
                key_sum,
                value_sum,
                group * queries_each + each,
                group,
                each == 0,
            )
            meanwhile[each]()
        for start in range(0, q_ref.shape[0], BLOCK):
            rows = pl.ds(start, BLOCK)
            dgate_buf[rows, pl.ds(base + queries_each * HD, HD)] = turned_back(
                key_sum[rows] * scaling, rows
            ).astype(jnp.bfloat16)
            dgate_buf[rows, pl.ds(base + (queries_each + 1) * HD, HD)] = value_sum[rows].astype(
                jnp.bfloat16
            )

    last = len(dp_order) - 1

    def after_head_0():
        feed.arrive_all(1, finish_out)
        pl.semaphore_signal(
            credit, inc=1, device_id={"tensor": flip(index, 1)}, device_id_type=MESH
        )
        pl.semaphore_signal(
            credit, inc=1, device_id={"tensor": flip(index, 2)}, device_id_type=MESH
        )
        feed.close()

    def nothing():
        pass

    def after_head_1():
        for j, c in down.units(1)[: max(1, len(down.units(1)) // 2)]:
            down.arrive(1, j, c)

    def after_head_2():
        for j, c in gate.units(1):
            gate.arrive(1, j, c)

    loads[7].wait()
    group_back(0, (after_head_0, nothing))
    for which in tiles:
        grad_tile(wide, dgate_buf, slice(0, TILE), one, which)
    after_head_1()
    group_back(1, (after_head_2, nothing))
    for which in tiles:
        grad_tile(wide, dgate_buf, slice(TILE, 2 * TILE), two, which)

    pl.semaphore_wait(credit, 2)

    def product(place):
        block = span(flip(index, place) * BLOCK, BLOCK)

        def tile(i, carry):
            cols = pl.ds(pl.multiple_of(i * 512, 512), 512)
            rs_part[block, cols] = nt(
                dgate_buf[block, pl.ds(0, weight_ref.shape[1])], weight_ref[cols]
            ).astype(jnp.bfloat16)
            return carry

        lax.fori_loop(0, rs_part.shape[1] // 512, tile, 0)

    for j, spot in enumerate((3, 1)):
        product(spot)
        for c in range(SPLIT):
            da.start(0, j, c)
    product(2)
    for c in range(SPLIT):
        da.arrive(0, 0, c)
    product(0)
    for c in range(SPLIT):
        da.arrive(0, 1, c)

    for j, c in down.units(1)[max(1, len(down.units(1)) // 2) :]:
        down.arrive(1, j, c)
    for c in range(SPLIT):
        da.arrive(1, 0, c, finish_da)
    gains = []
    peers = TENSOR_PEERS + tuple(("dp", bit) for bit in dp_order)

    def share_gains(i):
        axis, bit = peers[i]
        copy = pltpu.make_async_remote_copy(
            src_ref=gains_ref,
            dst_ref=gains_land.at[i],
            send_sem=gains_send.at[i],
            recv_sem=gains_recv.at[i],
            device_id={axis: flip(lax.axis_index(axis), 1 << bit)},
            device_id_type=MESH,
        )
        copy.start()
        gains.append(copy)

    def add_gains(i):
        gains[i].wait()
        gains_ref[...] += gains_land[i]

    share_gains(0)
    up.arrive_all(0)
    add_gains(0)
    share_gains(1)
    for step in range(1, last):
        if step > 1:
            down.arrive_all(step)
            gate.arrive_all(step)
    mix.arrive_all(0)
    add_gains(1)
    two.arrive_all(0)
    for i in range(2, len(peers)):
        share_gains(i)
        if i == 2:
            for step in range(1, last):
                up.arrive_all(step)
                mix.arrive_all(step)
        if i == 3:
            finish_grad(gate, gate_ref)
            finish_grad(down, down_ref)
        add_gains(i)
    one.arrive_all(0)
    for step in range(1, last):
        one.arrive_all(step)
        two.arrive_all(step)
    finish_grad(up, up_ref)
    finish_grad(mix, mix_ref)
    finish_grad(one, one_ref)
    finish_grad(two, two_ref)
    settle()
    for item in (da, gather, down, gate, up, mix, one, two):
        item.close()


def back_call(
    dm_part,
    feed_part,
    second_in,
    outer_low,
    hidden,
    gate_low,
    upward_low,
    first_in,
    middle,
    cotangent,
    live,
    token_share,
    first_gain,
    second_gain,
    mixing_weight,
    grouped_weight,
    attended,
    queries,
    key_rows,
    values,
    begin,
    log_totals,
    rope,
):
    slots, width = dm_part.shape
    rows = slots // 4
    columns = hidden.shape[1]
    heads = attended.shape[1]
    count = lax.axis_size("dp")
    dp_order = bits_of(count)
    z_order = (dp_order[1], dp_order[0]) + dp_order[2:]
    block = width // count
    share = Reduce.slots(4, SPLIT)
    total = Reduce.slots(count)

    def kernel(*refs):
        back_kernel(dp_order, z_order, *refs)

    def grad(size):
        return jax.ShapeDtypeStruct((block, size), jnp.float32)

    def low(*shape):
        return pltpu.VMEM(shape, jnp.bfloat16)

    sizes = (columns, columns, columns, heads, TILE, TILE)
    hops = 2 + len(dp_order)
    return pl.pallas_call(
        kernel,
        out_shape=(
            jax.ShapeDtypeStruct((rows, width), jnp.bfloat16),
            jax.ShapeDtypeStruct((rows, width), jnp.bfloat16),
            jax.ShapeDtypeStruct((2, width), jnp.float32),
            *(grad(size) for size in sizes),
        ),
        in_specs=[pl.BlockSpec(memory_space=pl.ANY)] * 8 + vmem_specs(15),
        out_specs=(*vmem_specs(3), *([pl.BlockSpec(memory_space=pl.ANY)] * 6)),
        scratch_shapes=[
            low(slots, width),
            low(slots, width),
            low(slots, columns),
            low(slots, columns),
            low(slots, columns),
            low(slots, width),
            low(share, rows // SPLIT, width),
            low(slots, width),
            pltpu.VMEM((rows, width), jnp.float32),
            pltpu.VMEM((slots, HD), jnp.float32),
            pltpu.VMEM((slots, HD), jnp.float32),
            pltpu.VMEM((hops, 2, width), jnp.float32),
            *(low(width, size) for size in sizes),
            *(low(total, block, size) for size in sizes),
            pltpu.VMEM((block, columns), jnp.float32),
            pltpu.SemaphoreType.DMA,
            pltpu.SemaphoreType.DMA((8,)),
            pltpu.SemaphoreType.REGULAR,
            *dma_sems(share),
            *dma_sems(share),
            *dma_sems(share),
            *dma_sems(3 * SPLIT),
            *(sem for size in sizes for sem in dma_sems(total)),
            *dma_sems(hops),
        ],
        compiler_params=pltpu.CompilerParams(
            collective_id=1, has_side_effects=True, vmem_limit_bytes=67043328
        ),
        name="back",
    )(
        dm_part,
        feed_part,
        second_in,
        outer_low,
        hidden,
        gate_low,
        upward_low,
        first_in,
        middle,
        cotangent,
        live,
        token_share,
        first_gain.reshape(1, -1),
        second_gain.reshape(1, -1),
        mixing_weight,
        grouped_weight,
        attended,
        queries,
        key_rows,
        values,
        begin,
        log_totals,
        rope,
    )


def on_device(
    tokens,
    lengths,
    owners,
    first_gain,
    query_weight,
    key_weight,
    value_weight,
    mixing_weight,
    second_gain,
    gate_weight,
    up_weight,
    down_weight,
    cotangent,
):
    slot_count = tokens.shape[0]
    share_rows = slot_count // lax.axis_size("tensor")
    share_start = lax.axis_index("tensor") * share_rows

    def share_of(array):
        return lax.dynamic_slice_in_dim(array, share_start, share_rows, 0)

    segment, offset, filled = slot_layout(lengths, owners, lax.axis_index("dp"), slot_count)
    slot_ids = jnp.arange(slot_count, dtype=jnp.int32)
    begin = jnp.where(filled > 0, slot_ids - offset, slot_ids)[None, :]
    cos_table, sin_table = rotary_tables(offset, HD)
    inputs = tokens.astype(jnp.float32)
    first_in = (inputs * inverse_rms(inputs) * first_gain).astype(jnp.bfloat16)
    queries = (
        rotate(matmul(first_in, query_weight).reshape(slot_count, -1, HD), cos_table, sin_table)
        .astype(jnp.bfloat16)
        .reshape(slot_count, -1)
    )
    key_rows = (
        rotate(matmul(first_in, key_weight).reshape(slot_count, -1, HD), cos_table, sin_table)
        .astype(jnp.bfloat16)
        .reshape(slot_count, -1)
    )
    values = matmul(first_in, value_weight).astype(jnp.bfloat16)
    attended, log_totals = attention_call(queries, key_rows, values, begin)
    token_share = share_of(tokens)
    second_in, middle = middle_call(attended, mixing_weight, token_share, second_gain)
    gate_value = matmul(second_in, gate_weight)
    upward = matmul(second_in, up_weight)
    sigmoid = jax.nn.sigmoid(gate_value)
    activated = gate_value * sigmoid
    hidden = (activated * upward).astype(jnp.bfloat16)
    feed_part = matmul_across(hidden, down_weight).astype(jnp.bfloat16)
    outer_low = cotangent * filled[:, None].astype(jnp.bfloat16)
    hidden_grad = matmul(outer_low, down_weight)
    gate_low = (hidden_grad * upward * sigmoid * (1.0 + gate_value * (1.0 - sigmoid))).astype(
        jnp.bfloat16
    )
    upward_low = (hidden_grad * activated).astype(jnp.bfloat16)
    second_part = (
        matmul_across(gate_low, gate_weight) + matmul_across(upward_low, up_weight)
    ).astype(jnp.bfloat16)
    kv_heads = key_weight.shape[1] // HD
    queries_each = query_weight.shape[1] // key_weight.shape[1]
    grouped = []
    for group in range(kv_heads):
        wide = queries_each * HD
        grouped.append(query_weight[:, group * wide : (group + 1) * wide])
        grouped.append(key_weight[:, group * HD : (group + 1) * HD])
        grouped.append(value_weight[:, group * HD : (group + 1) * HD])
    rope = jnp.concatenate([cos_table[:, 0], sin_table[:, 0]], axis=1)
    (
        layer_output,
        token_grad,
        gains,
        down_grad,
        gate_grad,
        up_grad,
        mixing_grad,
        one_grad,
        two_grad,
    ) = back_call(
        second_part,
        feed_part,
        second_in,
        outer_low,
        hidden,
        gate_low,
        upward_low,
        first_in,
        middle,
        share_of(cotangent),
        share_of(filled)[:, None],
        token_share,
        first_gain,
        second_gain,
        mixing_weight,
        jnp.concatenate(grouped, axis=1),
        attended,
        queries,
        key_rows,
        values,
        begin,
        log_totals,
        rope,
    )
    wide = queries_each * HD
    return (
        layer_output,
        token_grad,
        gains[0],
        jnp.concatenate([one_grad[:, :wide], two_grad[:, :wide]], axis=1),
        jnp.concatenate([one_grad[:, wide : wide + HD], two_grad[:, wide : wide + HD]], axis=1),
        jnp.concatenate([one_grad[:, wide + HD :], two_grad[:, wide + HD :]], axis=1),
        mixing_grad,
        gains[1],
        gate_grad,
        up_grad,
        down_grad,
    )


def solution(mesh):
    in_specs = (
        P("dp", None),
        P(),
        P(),
        P(),
        P(None, "tensor"),
        P(None, "tensor"),
        P(None, "tensor"),
        P(None, "tensor"),
        P(),
        P(None, "tensor"),
        P(None, "tensor"),
        P(None, "tensor"),
        P("dp", None),
    )
    out_specs = (
        P(("dp", "tensor"), None),
        P(("dp", "tensor"), None),
        P(),
        P("dp", "tensor"),
        P("dp", "tensor"),
        P("dp", "tensor"),
        P("dp", "tensor"),
        P(),
        P("dp", "tensor"),
        P("dp", "tensor"),
        P("dp", "tensor"),
    )
    return jax.shard_map(
        on_device, mesh=mesh, in_specs=in_specs, out_specs=out_specs, check_vma=False
    )
```

```python
import jax
import jax.numpy as jnp
import numpy as np
from jax import lax
from jax.experimental import pallas as pl
from jax.experimental.pallas import tpu as pltpu
from jax.sharding import PartitionSpec as P

HD = 96

MESH = pl.DeviceIdType.MESH

epsilon = 1e-05
rope_base = 10000.0


def bits_of(count):
    return tuple(range(count.bit_length() - 1))


def nn(left, right):
    return jnp.dot(left, right, preferred_element_type=jnp.float32)


def nt(left, right):
    return lax.dot_general(left, right, (((1,), (1,)), ((), ())), preferred_element_type=jnp.float32)


def tn(left, right):
    return lax.dot_general(left, right, (((0,), (0,)), ((), ())), preferred_element_type=jnp.float32)


def flip(index, mask):
    result = index
    bit = 0
    while mask >> bit:
        if (mask >> bit) & 1:
            result = result + (1 << bit) * (1 - 2 * lax.rem(lax.div(index, 1 << bit), 2))
        bit += 1
    return result


def span(start, size, step=16):
    return pl.ds(pl.multiple_of(start, step), size)


def greet(peers):
    barrier = pltpu.get_barrier_semaphore()
    for axis, bit in peers:
        index = lax.axis_index(axis)
        pl.semaphore_signal(
            barrier, inc=1, device_id={axis: flip(index, 1 << bit)}, device_id_type=MESH
        )
    pl.semaphore_wait(barrier, len(peers))


def chunk_rows(rows):
    for size in (64, 48, 32, 16):
        if rows % size == 0:
            return size
    return rows


class Reduce:
    def __init__(self, part, landing, send_sems, recv_sems, axis, order, split=1):
        self.part, self.landing = part, landing
        self.send_sems, self.recv_sems = send_sems, recv_sems
        self.axis, self.order, self.split = axis, order, split
        self.index = lax.axis_index(axis)
        self.rows = part.shape[0] >> len(order)
        self.piece = self.rows // split
        self.copies = {}
        self.lists = []
        base = 0
        for step in range(len(order)):
            kept = [0]
            for bit in reversed(order[step + 1 :]):
                kept = [place | (1 << bit) for place in kept] + kept
            self.lists.append((kept, base))
            base += len(kept) * split

    @staticmethod
    def slots(count, split=1):
        return (count - 1) * split

    def units(self, step):
        kept, _ = self.lists[step]
        return [(j, c) for j in range(len(kept)) for c in range(self.split)]

    def start(self, step, j, c=0):
        kept, base = self.lists[step]
        mask = 1 << self.order[step]
        slot = base + j * self.split + c
        source = flip(self.index, kept[j] | mask) * self.rows + c * self.piece
        copy = pltpu.make_async_remote_copy(
            src_ref=self.part.at[span(source, self.piece)],
            dst_ref=self.landing.at[slot],
            send_sem=self.send_sems.at[slot],
            recv_sem=self.recv_sems.at[slot],
            device_id={self.axis: flip(self.index, mask)},
            device_id_type=MESH,
        )
        copy.start()
        self.copies[slot] = copy

    def arrive(self, step, j, c=0, store=None):
        kept, base = self.lists[step]
        slot = base + j * self.split + c
        self.copies[slot].wait_recv()
        start = flip(self.index, kept[j]) * self.rows + c * self.piece
        size = chunk_rows(self.piece)

        def add(i, carry):
            rows = span(start + i * size, size)
            other = self.landing[slot, span(i * size, size)]
            total = self.part[rows].astype(jnp.float32) + other.astype(jnp.float32)
            if store is None:
                self.part[rows] = total.astype(self.part.dtype)
            else:
                store(c * self.piece + i * size, size, total)
            return carry

        lax.fori_loop(0, self.piece // size, add, 0)
        if step + 1 < len(self.order):
            later, _ = self.lists[step + 1]
            mask = 1 << self.order[step + 1]
            if kept[j] & mask:
                self.start(step + 1, later.index(kept[j] ^ mask), c)

    def start_all(self):
        for j, c in self.units(0):
            self.start(0, j, c)

    def arrive_all(self, step, store=None):
        for j, c in self.units(step):
            self.arrive(step, j, c, store)

    def close(self):
        for copy in self.copies.values():
            copy.wait_send()


class Gather:
    def __init__(self, whole, send_sems, recv_sems, split=1):
        self.whole, self.split = whole, split
        self.send_sems, self.recv_sems = send_sems, recv_sems
        self.index = lax.axis_index("tensor")
        self.rows = whole.shape[0] // 4
        self.piece = self.rows // split
        self.copies = {}

    def send(self, kind, c):
        mask = (2, 1, 1)[kind]
        block = flip(self.index, 2) if kind == 2 else self.index
        rows = span(block * self.rows + c * self.piece, self.piece)
        slot = kind * self.split + c
        copy = pltpu.make_async_remote_copy(
            src_ref=self.whole.at[rows],
            dst_ref=self.whole.at[rows],
            send_sem=self.send_sems.at[slot],
            recv_sem=self.recv_sems.at[slot],
            device_id={"tensor": flip(self.index, mask)},
            device_id_type=MESH,
        )
        copy.start()
        self.copies[kind, c] = copy

    def start(self, c):
        self.send(0, c)
        self.send(1, c)

    def forward(self, c):
        self.copies[0, c].wait_recv()
        self.send(2, c)

    def near(self, c):
        self.copies[1, c].wait_recv()

    def finish(self, c):
        self.copies[2, c].wait_recv()

    def close(self):
        for copy in self.copies.values():
            copy.wait_send()


TENSOR_PEERS = (("tensor", 0), ("tensor", 1))
SPLIT = 4


def middle_kernel(
    o_ref,
    w_ref,
    gain_ref,
    tokens_hbm,
    gm_hbm,
    gate_hbm,
    up_hbm,
    down_hbm,
    h_ref,
    m_hbm,
    hid_hbm,
    dgate_hbm,
    dup_hbm,
    feed_hbm,
    dm_hbm,
    part,
    landing,
    m_buf,
    x_buf,
    gm_buf,
    gate_w,
    up_w,
    down_w,
    hid_buf,
    dgate_buf,
    dup_buf,
    rs_send,
    rs_recv,
    ag_send,
    ag_recv,
    load_sems,
    leave_sems,
    feed_buf,
):
    index = lax.axis_index("tensor")
    rows = o_ref.shape[0] // 4
    loads = [
        pltpu.make_async_copy(source, target, load_sems.at[i])
        for i, (source, target) in enumerate(
            (
                (tokens_hbm.at[span(index * rows, rows)], x_buf),
                (gate_hbm, gate_w),
                (up_hbm, up_w),
                (gm_hbm, gm_buf),
                (down_hbm, down_w),
            )
        )
    ]
    for load in loads:
        load.start()
    greet(TENSOR_PEERS)
    reduce = Reduce(part, landing, rs_send, rs_recv, "tensor", (0, 1), SPLIT)
    gather = Gather(m_buf, ag_send, ag_recv, SPLIT)
    leaving = []

    def leave(buffer, target, half):
        there = span(half * 2 * rows, 2 * rows)
        copy = pltpu.make_async_copy(
            buffer.at[there], target.at[there], leave_sems.at[len(leaving)]
        )
        copy.start()
        leaving.append(copy)

    def product(place):
        block = span(flip(index, place) * rows, rows)
        columns = 512

        def tile(i, carry):
            cols = pl.ds(pl.multiple_of(i * columns, columns), columns)
            part[block, cols] = nt(o_ref[block], w_ref[cols]).astype(jnp.bfloat16)
            return carry

        lax.fori_loop(0, part.shape[1] // columns, tile, 0)

    def normed(start, size, total):
        own = span(start, size)
        hidden = x_buf[own].astype(jnp.float32) + total
        h_ref[own] = hidden
        inverse = lax.rsqrt(jnp.mean(hidden * hidden, axis=-1, keepdims=True) + epsilon)
        m_buf[span(index * rows + start, size)] = (hidden * inverse * gain_ref[...]).astype(
            jnp.bfloat16
        )

    def hidden_part(half, first, last):
        there = span(half * 2 * rows, 2 * rows)
        columns = 256

        def tile(i, carry):
            cols = pl.ds(pl.multiple_of(i * columns, columns), columns)
            gate = nn(m_buf[there], gate_w[:, cols])
            upward = nn(m_buf[there], up_w[:, cols])
            grad = nn(gm_buf[there], down_w[:, cols])
            sigmoid = 1.0 / (1.0 + jnp.exp(-gate))
            activated = gate * sigmoid
            hid_buf[there, cols] = (activated * upward).astype(jnp.bfloat16)
            dgate_buf[there, cols] = (
                grad * upward * sigmoid * (1.0 + gate * (1.0 - sigmoid))
            ).astype(jnp.bfloat16)
            dup_buf[there, cols] = (grad * activated).astype(jnp.bfloat16)
            return carry

        lax.fori_loop(first, last, tile, 0)

    def feed_part(half):
        there = span(half * 2 * rows, 2 * rows)

        def tile(i, carry):
            cols = pl.ds(pl.multiple_of(i * 512, 512), 512)
            feed_buf[there, cols] = nt(hid_buf[there], down_w[cols]).astype(jnp.bfloat16)
            return carry

        lax.fori_loop(0, feed_buf.shape[1] // 512, tile, 0)

    def dm_part(half):
        there = span(half * 2 * rows, 2 * rows)

        def tile(i, carry):
            cols = pl.ds(pl.multiple_of(i * 512, 512), 512)
            total = nt(dgate_buf[there], gate_w[cols]) + nt(dup_buf[there], up_w[cols])
            part[there, cols] = total.astype(jnp.bfloat16)
            return carry

        lax.fori_loop(0, part.shape[1] // 512, tile, 0)

    product(3)
    for c in range(SPLIT):
        reduce.start(0, 0, c)
    product(2)
    for c in range(SPLIT):
        reduce.arrive(0, 0, c)
    product(1)
    for c in range(SPLIT):
        reduce.start(0, 1, c)
    product(0)
    for c in range(SPLIT):
        reduce.arrive(0, 1, c)
    loads[0].wait()
    for c in range(SPLIT):
        reduce.arrive(1, 0, c, normed)
        gather.start(c)
    near = lax.div(index, 2)
    far = 1 - near
    for load in loads[1:]:
        load.wait()
    for c in range(SPLIT):
        gather.near(c)
    reduce.close()
    tiles = hid_buf.shape[1] // 256
    hidden_part(near, 0, tiles // 2)
    gather.forward(0)
    hidden_part(near, tiles // 2, tiles)
    gather.forward(1)
    leave(hid_buf, hid_hbm, near)
    leave(dgate_buf, dgate_hbm, near)
    leave(dup_buf, dup_hbm, near)
    leave(m_buf, m_hbm, near)
    feed_part(near)
    leave(feed_buf, feed_hbm, near)
    gather.forward(2)
    dm_part(near)
    leave(part, dm_hbm, near)
    for c in range(3, SPLIT):
        gather.forward(c)
    for c in range(SPLIT):
        gather.finish(c)
    leave(m_buf, m_hbm, far)
    hidden_part(far, 0, tiles)
    leave(hid_buf, hid_hbm, far)
    leave(dgate_buf, dgate_hbm, far)
    leave(dup_buf, dup_hbm, far)
    feed_part(far)
    leave(feed_buf, feed_hbm, far)
    dm_part(far)
    leave(part, dm_hbm, far)
    for copy in leaving:
        copy.wait()
    gather.close()


def vmem_specs(count):
    return [pl.BlockSpec(memory_space=pltpu.VMEM)] * count


def dma_sems(count):
    return [pltpu.SemaphoreType.DMA((count,)), pltpu.SemaphoreType.DMA((count,))]


def middle_call(
    attended, mixing_weight, second_gain, tokens, outer_low, gate_weight, up_weight, down_weight
):
    slots, width = tokens.shape
    rows = slots // 4
    columns = gate_weight.shape[1]
    count = Reduce.slots(4, SPLIT)

    def low(*shape):
        return pltpu.VMEM(shape, jnp.bfloat16)

    def result(size):
        return jax.ShapeDtypeStruct((slots, size), jnp.bfloat16)

    return pl.pallas_call(
        middle_kernel,
        out_shape=(
            jax.ShapeDtypeStruct((rows, width), jnp.float32),
            result(width),
            result(columns),
            result(columns),
            result(columns),
            result(width),
            result(width),
        ),
        in_specs=vmem_specs(3) + [pl.BlockSpec(memory_space=pl.ANY)] * 5,
        out_specs=tuple(vmem_specs(1) + [pl.BlockSpec(memory_space=pl.ANY)] * 6),
        scratch_shapes=[
            low(slots, width),
            low(count, rows // SPLIT, width),
            low(slots, width),
            low(rows, width),
            low(slots, width),
            low(width, columns),
            low(width, columns),
            low(width, columns),
            low(slots, columns),
            low(slots, columns),
            low(slots, columns),
            *dma_sems(count),
            *dma_sems(3 * SPLIT),
            pltpu.SemaphoreType.DMA((5,)),
            pltpu.SemaphoreType.DMA((12,)),
            low(slots, width),
        ],
        compiler_params=pltpu.CompilerParams(
            collective_id=0, has_side_effects=True, vmem_limit_bytes=67043328
        ),
        name="middle",
    )(
        attended,
        mixing_weight,
        second_gain.reshape(1, -1),
        tokens,
        outer_low,
        gate_weight,
        up_weight,
        down_weight,
    )


BLOCK = 256
TILE = 384


def head(index):
    return pl.ds(index * HD, HD)


def allowed_keys(begin_row, query_start, key_count, query_count):
    keys = lax.broadcasted_iota(jnp.int32, (key_count, query_count), 0)
    queries = query_start + lax.broadcasted_iota(jnp.int32, (key_count, query_count), 1)
    return (keys >= begin_row) & (keys <= queries)


def rope_tables(slots):
    half = HD // 2
    frequency = rope_base ** (-2.0 * np.arange(half) / HD)

    def table(places):
        angles = places[:, None] * frequency[None, :]
        return np.concatenate([np.cos(angles), np.sin(angles)], axis=1).astype(np.float32)

    return (
        jnp.asarray(table(np.arange(BLOCK))),
        jnp.asarray(table(np.arange(max(8, slots // BLOCK)) * BLOCK)),
    )


def block_angles(base_ref, step_ref, block):
    half = HD // 2
    low_cos, low_sin = base_ref[:, pl.ds(0, half)], base_ref[:, pl.ds(half, half)]
    high = step_ref[pl.ds(block, 1)]
    high_cos, high_sin = high[:, :half], high[:, half:]
    return (low_cos * high_cos - low_sin * high_sin, low_sin * high_cos + low_cos * high_sin)


def turn(values, cosine, sine):
    half = HD // 2
    first, second = values[:, :half], values[:, half:]
    return jnp.concatenate([first * cosine - second * sine, second * cosine + first * sine], axis=1)


def first_kernel(
    blocks,
    lengths_ref,
    owners_ref,
    x_ref,
    cot_ref,
    gain_ref,
    wq_ref,
    wk_ref,
    wv_ref,
    base_ref,
    step_ref,
    a_ref,
    gm_ref,
    q_ref,
    kv_ref,
    o_ref,
    lse_ref,
    begin_ref,
    used_ref,
    kv_all,
    turned,
):
    block = pl.program_id(0)
    index = lax.axis_index("dp")
    slots = block * BLOCK + lax.broadcasted_iota(jnp.int32, (1, BLOCK), 1)

    def sequence(s, carry):
        total, begin = carry
        length = jnp.where(owners_ref[s] == index, lengths_ref[s], 0)
        begin = jnp.where((slots >= total) & (slots < total + length), total, begin)
        return total + length, begin

    used, begin = lax.fori_loop(0, lengths_ref.shape[0], sequence, (jnp.int32(0), slots))
    begin_ref[...] = begin
    used_ref[0] = used
    size = 64

    def rows_in(i, carry):
        rows = span(i * size, size)
        values = x_ref[rows].astype(jnp.float32)
        inverse = lax.rsqrt(jnp.mean(values * values, axis=-1, keepdims=True) + epsilon)
        a_ref[rows] = (values * inverse * gain_ref[...]).astype(jnp.bfloat16)
        places = block * BLOCK + i * size + lax.broadcasted_iota(jnp.int32, (size, 1), 0)
        live = (places < used).astype(jnp.float32)
        gm_ref[rows] = (cot_ref[rows].astype(jnp.float32) * live).astype(jnp.bfloat16)
        return carry

    lax.fori_loop(0, BLOCK // size, rows_in, 0)
    cosine, sine = block_angles(base_ref, step_ref, block)
    normed = a_ref[...]
    queries = nn(normed, wq_ref[...])
    query_heads, key_heads = queries.shape[1] // HD, wk_ref.shape[0] // HD
    for h in range(query_heads):
        piece = queries[:, h * HD : (h + 1) * HD]
        q_ref[:, head(h)] = turn(piece, cosine, sine).astype(jnp.bfloat16)
    keys = nt(normed, wk_ref[...])
    for h in range(key_heads):
        piece = keys[:, h * HD : (h + 1) * HD]
        kv_ref[:, head(h)] = turn(piece, cosine, sine).astype(jnp.bfloat16)
    values = nt(normed, wv_ref[...]).astype(jnp.bfloat16)
    kv_ref[:, pl.ds(key_heads * HD, key_heads * HD)] = values
    kv_all[span(block * BLOCK, BLOCK)] = kv_ref[...]
    scaling = HD ** (-0.5)
    groups = query_heads // key_heads

    def attend(now):
        stop = (now + 1) * BLOCK
        turned[:, pl.ds(now * BLOCK, BLOCK)] = values.T
        allowed = allowed_keys(begin, now * BLOCK, stop, BLOCK)
        for h in range(query_heads):
            group = h // groups
            scores = nt(kv_all[pl.ds(0, stop), head(group)], q_ref[:, head(h)]) * scaling
            scores = jnp.where(allowed, scores, -jnp.inf)
            highest = jnp.max(scores, axis=0, keepdims=True)
            exponent = jnp.exp(scores - highest)
            total = jnp.sum(exponent, axis=0, keepdims=True)
            weights = (exponent * (1.0 / total)).astype(jnp.bfloat16)
            mixed = nn(turned[pl.ds(group * HD, HD), pl.ds(0, stop)], weights)
            o_ref[:, head(h)] = mixed.T.astype(jnp.bfloat16)
            lse_ref[pl.ds(h, 1)] = highest + jnp.log(total)

    for now in range(blocks):
        pl.when(block == now)(lambda now=now: attend(now))


def first_call(
    tokens, lengths, owners, first_gain, query_weight, key_weight, value_weight, cotangent, tables
):
    slots, width = tokens.shape
    blocks = slots // BLOCK
    columns, pairs = query_weight.shape[1], 2 * key_weight.shape[0]
    heads = columns // HD

    def kernel(*refs):
        first_kernel(blocks, *refs)

    def rows_of(size):
        return pl.BlockSpec((BLOCK, size), lambda i: (i, 0))

    def whole(array):
        return pl.BlockSpec(array.shape, lambda i: (0, 0), pipeline_mode=pl.Buffered(1))

    gain = first_gain.reshape(1, -1)
    scalars = pl.BlockSpec(memory_space=pltpu.SMEM)
    return pl.pallas_call(
        kernel,
        grid=(blocks,),
        out_shape=(
            jax.ShapeDtypeStruct((slots, width), jnp.bfloat16),
            jax.ShapeDtypeStruct((slots, width), jnp.bfloat16),
            jax.ShapeDtypeStruct((slots, columns), jnp.bfloat16),
            jax.ShapeDtypeStruct((slots, pairs), jnp.bfloat16),
            jax.ShapeDtypeStruct((slots, columns), jnp.bfloat16),
            jax.ShapeDtypeStruct((heads, slots), jnp.float32),
            jax.ShapeDtypeStruct((1, slots), jnp.int32),
            jax.ShapeDtypeStruct((1,), jnp.int32),
        ),
        in_specs=[
            scalars,
            scalars,
            rows_of(width),
            rows_of(width),
            whole(gain),
            whole(query_weight),
            whole(key_weight),
            whole(value_weight),
            whole(tables[0]),
            whole(tables[1]),
        ],
        out_specs=(
            rows_of(width),
            rows_of(width),
            rows_of(columns),
            rows_of(pairs),
            rows_of(columns),
            pl.BlockSpec((heads, BLOCK), lambda i: (0, i)),
            pl.BlockSpec((1, BLOCK), lambda i: (0, i)),
            scalars,
        ),
        scratch_shapes=[
            pltpu.VMEM((slots, pairs), jnp.bfloat16),
            pltpu.VMEM((pairs // 2, slots), jnp.bfloat16),
        ],
        compiler_params=pltpu.CompilerParams(vmem_limit_bytes=67043328),
        name="first",
    )(
        lengths,
        owners,
        tokens,
        cotangent,
        gain,
        query_weight,
        key_weight,
        value_weight,
        *tables,
    )


def last_kernel(group_columns, *refs):
    sources, targets, buffers = refs[:8], refs[8:17], refs[17:28]
    in_sems, out_sems = refs[28:]
    out, token, down, gate, up, mix, one, two = buffers[:8]
    turned = buffers[8:]
    coming = [
        pltpu.make_async_copy(source, buffer, in_sems.at[i])
        for i, (source, buffer) in enumerate(zip(sources, buffers[:8]))
    ]
    for copy in coming:
        copy.start()
    leaving = []

    def leave(buffer):
        i = len(leaving)
        copy = pltpu.make_async_copy(buffer, targets[i], out_sems.at[i])
        copy.start()
        leaving.append(copy)

    for i in (0, 1, 2, 3, 4, 5):
        coming[i].wait()
        leave(buffers[i])
    start = 0
    coming[6].wait()
    coming[7].wait()
    for buffer in turned:
        each = buffer.shape[1] // 2
        buffer[:, pl.ds(0, each)] = one[:, pl.ds(start, each)]
        buffer[:, pl.ds(each, each)] = two[:, pl.ds(start, each)]
        start += each
        leave(buffer)
    for copy in leaving:
        copy.wait()


def last_call(arrays, query_columns, key_columns):
    rows = arrays[6].shape[0]
    shapes = [jax.ShapeDtypeStruct(array.shape, array.dtype) for array in arrays[:6]]
    shapes += [
        jax.ShapeDtypeStruct((rows, size), jnp.float32)
        for size in (query_columns, key_columns, key_columns)
    ]

    def kernel(*refs):
        last_kernel(TILE, *refs)

    buffers = [pltpu.VMEM(array.shape, array.dtype) for array in arrays]
    buffers += [pltpu.VMEM(shape.shape, shape.dtype) for shape in shapes[6:]]
    return pl.pallas_call(
        kernel,
        out_shape=tuple(shapes),
        in_specs=[pl.BlockSpec(memory_space=pl.ANY)] * 8,
        out_specs=tuple([pl.BlockSpec(memory_space=pl.ANY)] * 9),
        scratch_shapes=[
            *buffers,
            pltpu.SemaphoreType.DMA((8,)),
            pltpu.SemaphoreType.DMA((9,)),
        ],
        compiler_params=pltpu.CompilerParams(vmem_limit_bytes=67043328),
        name="last",
    )(*arrays)


def attention_back(q_ref, kv_ref, do_ref, begin_ref, lse_ref, turned, sums, h, group, start, first):
    scaling = HD ** (-0.5)
    key_sum, value_sum = sums
    key_heads = kv_ref.shape[1] // (2 * HD)
    stop = start + BLOCK
    rows = pl.ds(start, BLOCK)
    seen = pl.ds(0, stop)
    query = q_ref[rows, head(h)]
    grad = do_ref[rows, head(h)]
    scores = nt(kv_ref[seen, head(group)], query) * scaling
    allowed = allowed_keys(begin_ref[:, rows], start, stop, BLOCK)
    weights = jnp.where(allowed, jnp.exp(scores - lse_ref[pl.ds(h, 1), rows]), 0.0)
    weights_grad = nt(kv_ref[seen, head(key_heads + group)], grad)
    inner = jnp.sum(weights * weights_grad, axis=0, keepdims=True)
    scores_grad = (weights * (weights_grad - inner)).astype(jnp.bfloat16)
    values_part = nn(weights.astype(jnp.bfloat16), grad)
    keys_part = nn(scores_grad, query)
    if first:
        value_sum[...] = values_part
        key_sum[...] = keys_part
    else:
        value_sum[seen] += values_part
        key_sum[seen] += keys_part
    return nn(turned[:, :stop], scores_grad).T * scaling


P_START = "start"
P_TILE = "tile"
P_ARRIVE = "arrive"
P_FORWARD = "forward"
P_FINISH = "finish"
P_BACK = "back"
P_ATTENTION = "attention"
P_KEYS = "keys"
P_PRODUCT = "product"
P_SEND = "send"
P_ADD = "add"
P_DM = "dm"
P_FEED = "feed"
P_DA = "da"
P_DOWN = "down"
P_GATE = "gate"
P_UP = "up"
P_MIX = "mix"
P_ONE = "one"
P_TWO = "two"

PLAN = (
    (P_START, P_DM),
    (P_TILE, P_DOWN, 3),
    (P_TILE, P_DOWN, 1),
    (P_TILE, P_DOWN, 2),
    (P_TILE, P_DOWN, 0),
    (P_TILE, P_GATE, 3),
    (P_ARRIVE, P_DM, 0, 0, 1),
    (P_ARRIVE, P_DM, 0, 1, 3),
    (P_ARRIVE, P_DM, 0, 1, 1),
    (P_ARRIVE, P_DM, 0, 1, 2),
    (P_TILE, P_GATE, 1),
    (P_TILE, P_GATE, 2),
    (P_ARRIVE, P_DM, 0, 1, 0),
    (P_ARRIVE, P_DM, 0, 0, 0),
    (P_ARRIVE, P_DM, 0, 0, 2),
    (P_ARRIVE, P_DM, 0, 0, 3),
    (P_ARRIVE, P_DM, 1, 0, 2),
    (P_ARRIVE, P_GATE, 0, 0, 0),
    (P_ARRIVE, P_GATE, 0, 1, 0),
    (P_TILE, P_GATE, 0),
    (P_ARRIVE, P_DM, 1, 0, 0),
    (P_TILE, P_UP, 3),
    (P_TILE, P_UP, 1),
    (P_ARRIVE, P_DM, 1, 0, 1),
    (P_ARRIVE, P_DOWN, 0, 0, 0),
    (P_TILE, P_UP, 2),
    (P_ARRIVE, P_GATE, 0, 2, 0),
    (P_ARRIVE, P_DM, 1, 0, 3),
    (P_ARRIVE, P_DOWN, 0, 2, 0),
    (P_TILE, P_UP, 0),
    (P_FORWARD, 0),
    (P_FORWARD, 2),
    (P_ARRIVE, P_DOWN, 0, 3, 0),
    (P_FINISH, 2),
    (P_ARRIVE, P_GATE, 0, 3, 0),
    (P_FINISH, 0),
    (P_ARRIVE, P_DOWN, 0, 1, 0),
    (P_FORWARD, 1),
    (P_FINISH, 1),
    (P_FORWARD, 3),
    (P_FINISH, 3),
    (P_START, P_FEED),
    (P_ARRIVE, P_FEED, 0, 0, 0),
    (P_ARRIVE, P_GATE, 1, 0, 0),
    (P_ARRIVE, P_FEED, 0, 1, 1),
    (P_ARRIVE, P_FEED, 0, 0, 3),
    (P_TILE, P_MIX, 3),
    (P_ARRIVE, P_UP, 0, 0, 0),
    (P_TILE, P_MIX, 1),
    (P_TILE, P_MIX, 2),
    (P_ARRIVE, P_FEED, 0, 0, 2),
    (P_TILE, P_MIX, 0),
    (P_ARRIVE, P_FEED, 0, 1, 3),
    (P_ARRIVE, P_FEED, 0, 0, 1),
    (P_ARRIVE, P_FEED, 0, 1, 0),
    (P_BACK,),
    (P_ATTENTION, 0, 3),
    (P_ATTENTION, 0, 2),
    (P_ATTENTION, 0, 1),
    (P_ATTENTION, 0, 0),
    (P_ATTENTION, 1, 3),
    (P_ARRIVE, P_FEED, 0, 1, 2),
    (P_ARRIVE, P_FEED, 1, 0, 2),
    (P_ARRIVE, P_FEED, 1, 0, 1),
    (P_ARRIVE, P_FEED, 1, 0, 0),
    (P_ARRIVE, P_DOWN, 1, 0, 0),
    (P_ATTENTION, 1, 2),
    (P_ATTENTION, 1, 1),
    (P_ATTENTION, 1, 0),
    (P_KEYS, 0),
    (P_TILE, P_ONE, 3),
    (P_TILE, P_ONE, 1),
    (P_TILE, P_ONE, 2),
    (P_TILE, P_ONE, 0),
    (P_ARRIVE, P_GATE, 1, 1, 0),
    (P_ARRIVE, P_UP, 0, 1, 0),
    (P_ARRIVE, P_FEED, 1, 0, 3),
    (P_ARRIVE, P_GATE, 2, 0, 0),
    (P_ARRIVE, P_UP, 0, 2, 0),
    (P_ATTENTION, 2, 3),
    (P_ATTENTION, 2, 2),
    (P_ATTENTION, 2, 1),
    (P_ATTENTION, 2, 0),
    (P_ATTENTION, 3, 3),
    (P_ATTENTION, 3, 2),
    (P_ATTENTION, 3, 1),
    (P_ATTENTION, 3, 0),
    (P_KEYS, 1),
    (P_TILE, P_TWO, 3),
    (P_TILE, P_TWO, 1),
    (P_ARRIVE, P_UP, 1, 0, 0),
    (P_ARRIVE, P_MIX, 0, 0, 0),
    (P_TILE, P_TWO, 2),
    (P_TILE, P_TWO, 0),
    (P_PRODUCT, 3),
    (P_PRODUCT, 1),
    (P_ARRIVE, P_ONE, 0, 0, 0),
    (P_ARRIVE, P_DOWN, 1, 1, 0),
    (P_PRODUCT, 2),
    (P_ARRIVE, P_DA, 0, 0, 2),
    (P_PRODUCT, 0),
    (P_ARRIVE, P_ONE, 0, 1, 0),
    (P_ARRIVE, P_DA, 0, 1, 1),
    (P_ARRIVE, P_MIX, 0, 1, 0),
    (P_ARRIVE, P_MIX, 0, 2, 0),
    (P_ARRIVE, P_DA, 0, 0, 3),
    (P_ARRIVE, P_MIX, 1, 0, 0),
    (P_ARRIVE, P_DA, 0, 0, 0),
    (P_ARRIVE, P_ONE, 0, 2, 0),
    (P_ARRIVE, P_DOWN, 2, 0, 0),
    (P_ARRIVE, P_TWO, 0, 0, 0),
    (P_ARRIVE, P_ONE, 0, 3, 0),
    (P_ARRIVE, P_MIX, 0, 3, 0),
    (P_ARRIVE, P_DA, 0, 1, 2),
    (P_ARRIVE, P_DA, 0, 1, 0),
    (P_ARRIVE, P_ONE, 1, 0, 0),
    (P_ARRIVE, P_ONE, 1, 1, 0),
    (P_ARRIVE, P_DA, 0, 0, 1),
    (P_ARRIVE, P_UP, 0, 3, 0),
    (P_ARRIVE, P_UP, 1, 1, 0),
    (P_ARRIVE, P_MIX, 1, 1, 0),
    (P_ARRIVE, P_MIX, 2, 0, 0),
    (P_ARRIVE, P_TWO, 0, 1, 0),
    (P_ARRIVE, P_DA, 1, 0, 2),
    (P_ARRIVE, P_DA, 1, 0, 1),
    (P_ARRIVE, P_DA, 1, 0, 0),
    (P_ARRIVE, P_TWO, 0, 2, 0),
    (P_ARRIVE, P_TWO, 1, 0, 0),
    (P_ARRIVE, P_TWO, 0, 3, 0),
    (P_ARRIVE, P_DA, 0, 1, 3),
    (P_ARRIVE, P_DA, 1, 0, 3),
    (P_SEND, 0),
    (P_ADD, 0),
    (P_ARRIVE, P_UP, 2, 0, 0),
    (P_SEND, 1),
    (P_ADD, 1),
    (P_SEND, 2),
    (P_ADD, 2),
    (P_SEND, 3),
    (P_ADD, 3),
    (P_SEND, 4),
    (P_ARRIVE, P_TWO, 1, 1, 0),
    (P_ARRIVE, P_TWO, 2, 0, 0),
    (P_ARRIVE, P_ONE, 2, 0, 0),
    (P_ADD, 4),
)
def plan_of(count, orders, reduces):
    if count == 8:
        return PLAN
    tiles = (3, 1, 2, 0)

    def units(name, step):
        return [(P_ARRIVE, name, step, j, c) for j, c in reduces[name].units(step)]

    plan = [(P_START, P_DM)]
    plan += [(P_TILE, name, which) for name in (P_DOWN, P_GATE, P_UP) for which in tiles]
    plan += units(P_DM, 0) + units(P_DM, 1)
    plan += [(P_FORWARD, c) for c in range(SPLIT)] + [(P_FINISH, c) for c in range(SPLIT)]
    plan += [(P_START, P_FEED)] + [(P_TILE, P_MIX, which) for which in tiles] + [(P_BACK,)]
    for h in range(4):
        plan += [(P_ATTENTION, h, block) for block in (3, 2, 1, 0)]
        if h % 2:
            plan += [(P_KEYS, h // 2)]
            plan += [(P_TILE, (P_ONE, P_TWO)[h // 2], which) for which in tiles]
    plan += units(P_FEED, 0) + units(P_FEED, 1)
    plan += [(P_PRODUCT, place) for place in (3, 1, 2, 0)] + units(P_DA, 0) + units(P_DA, 1)
    names = (P_DOWN, P_GATE, P_UP, P_MIX, P_ONE, P_TWO)
    for step in range(len(orders[0])):
        for name in names:
            plan += units(name, step)
    for i in range(2 + len(orders[0])):
        plan += [(P_SEND, i), (P_ADD, i)]
    return plan


def back_kernel(
    dp_order,
    z_order,
    dm_hbm,
    feed_hbm,
    m_hbm,
    gm_hbm,
    hid_hbm,
    dgate_hbm,
    dup_hbm,
    a_hbm,
    tokens_hbm,
    used_ref,
    h_ref,
    gain1_ref,
    gain2_ref,
    mixing_ref,
    query_ref,
    key_ref,
    value_ref,
    o_ref,
    q_ref,
    kv_ref,
    begin_ref,
    lse_ref,
    base_ref,
    step_ref,
    out_ref,
    token_ref,
    gains_ref,
    down_ref,
    gate_ref,
    up_ref,
    mix_ref,
    one_ref,
    two_ref,
    *scratch,
):
    (
        wide,
        m_buf,
        hid_buf,
        dgate_buf,
        rs_part,
        rs_land,
        ga_buf,
        dh_buf,
        key_sum,
        value_sum,
        gains_land,
        cot_ref,
        result,
        *scratch,
    ) = scratch
    parts, lands, sems = scratch[:6], scratch[6:12], scratch[12:]
    stage, stage_sem, out_sem, load_sems, credit, *sems = sems
    index = lax.axis_index("tensor")
    dp_index = lax.axis_index("dp")
    count = 1 << len(dp_order)

    own_rows = span(index * h_ref.shape[0], h_ref.shape[0])
    loads = [
        pltpu.make_async_copy(source, target, load_sems.at[i])
        for i, (source, target) in enumerate(
            (
                (dm_hbm, rs_part),
                (gm_hbm, wide),
                (hid_hbm, hid_buf),
                (m_hbm, m_buf),
                (dgate_hbm, dgate_buf),
                (dup_hbm, hid_buf),
                (feed_hbm, rs_part),
                (a_hbm, wide),
                (gm_hbm.at[own_rows], cot_ref),
                (tokens_hbm.at[own_rows], cot_ref),
            )
        )
    ]
    for load in loads[:5] + loads[8:9]:
        load.start()
    greet(TENSOR_PEERS + tuple(("dp", bit) for bit in dp_order))

    def share_reduce(first_sem):
        return Reduce(rs_part, rs_land, sems[first_sem], sems[first_sem + 1], "tensor", (0, 1), SPLIT)

    dm, feed, da = share_reduce(0), share_reduce(2), share_reduce(4)
    gather = Gather(ga_buf, sems[6], sems[7], SPLIT)
    orders = (z_order, dp_order, dp_order, dp_order, dp_order, dp_order)
    down, gate, up, mix, one, two = (
        Reduce(parts[i], lands[i], sems[8 + 2 * i], sems[9 + 2 * i], "dp", orders[i])
        for i in range(6)
    )
    gains_send, gains_recv = sems[20], sems[21]
    gains_ref[...] = jnp.zeros_like(gains_ref)

    def finish_out(start, size, total):
        own = span(start, size)
        places = index * h_ref.shape[0] + start + lax.broadcasted_iota(jnp.int32, (size, 1), 0)
        live = (places < used_ref[0]).astype(jnp.float32)
        result[own] = ((h_ref[own] + total) * live).astype(jnp.bfloat16)

    def finish_dm(start, size, total):
        own = span(start, size)
        hidden = h_ref[own]
        inverse = lax.rsqrt(jnp.mean(hidden * hidden, axis=-1, keepdims=True) + epsilon)
        scaled = total * gain2_ref[...]
        inner = jnp.mean(scaled * hidden, axis=-1, keepdims=True)
        grad = (
            cot_ref[own].astype(jnp.float32)
            + inverse * scaled
            - hidden * (inverse * inverse * inverse) * inner
        )
        dh_buf[own] = grad
        ga_buf[span(index * dh_buf.shape[0] + start, size)] = grad.astype(jnp.bfloat16)
        gains_ref[pl.ds(1, 1)] += jnp.sum(total * hidden * inverse, axis=0, keepdims=True)

    def finish_da(start, size, total):
        own = span(start, size)
        values = cot_ref[own].astype(jnp.float32)
        inverse = lax.rsqrt(jnp.mean(values * values, axis=-1, keepdims=True) + epsilon)
        scaled = total * gain1_ref[...]
        inner = jnp.mean(scaled * values, axis=-1, keepdims=True)
        grad = dh_buf[own] + inverse * scaled - values * (inverse * inverse * inverse) * inner
        result[own] = grad.astype(jnp.bfloat16)
        gains_ref[pl.ds(0, 1)] += jnp.sum(total * values * inverse, axis=0, keepdims=True)

    out_copy = pltpu.make_async_copy(result, out_ref, out_sem.at[0])
    token_copy = pltpu.make_async_copy(result, token_ref, out_sem.at[1])
    flying = []

    def settle():
        for copy in flying:
            copy.wait()
        flying.clear()

    def finish_grad(reduce, target):
        settle()
        columns = pl.ds(0, reduce.part.shape[1])

        def store(start, size, total):
            stage[span(start, size), columns] = total

        reduce.arrive_all(last, store)
        copy = pltpu.make_async_copy(stage.at[:, columns], target, stage_sem)
        copy.start()
        flying.append(copy)

    def grad_tile(left, right, columns, reduce, which):
        blocks = TILE // reduce.rows
        tile = flip(lax.div(dp_index, blocks), which) * TILE
        cols = pl.ds(pl.multiple_of(tile, 128), TILE)
        width = columns.stop - columns.start
        step = min(width, 512)

        def some(i, carry):
            there = pl.ds(pl.multiple_of(i * step, 128), step)
            here = pl.ds(pl.multiple_of(columns.start + i * step, 128), step)
            reduce.part[span(tile, TILE), there] = tn(left[:, cols], right[:, here]).astype(
                jnp.bfloat16
            )
            return carry

        lax.fori_loop(0, width // step, some, 0)
        kept, _ = reduce.lists[0]
        for j, kept_place in enumerate(kept):
            if (kept_place | (1 << reduce.order[0])) // blocks == which:
                reduce.start(0, j)

    slots, hidden_columns = hid_buf.shape
    query_columns, key_columns = q_ref.shape[1], kv_ref.shape[1] // 2
    queries_each = query_columns // key_columns
    group_size = query_columns // (queries_each * HD)
    scaling = HD ** (-0.5)
    last = len(dp_order) - 1
    reduces = {
        "dm": dm,
        "feed": feed,
        "da": da,
        "down": down,
        "gate": gate,
        "up": up,
        "mix": mix,
        "one": one,
        "two": two,
    }
    targets = {
        "down": down_ref,
        "gate": gate_ref,
        "up": up_ref,
        "mix": mix_ref,
        "one": one_ref,
        "two": two_ref,
    }
    sources = {
        "down": (wide, hid_buf, slice(0, hidden_columns)),
        "gate": (m_buf, dgate_buf, slice(0, hidden_columns)),
        "up": (m_buf, hid_buf, slice(0, hidden_columns)),
        "mix": (ga_buf, o_ref, slice(0, query_columns)),
        "one": (wide, dgate_buf, slice(0, TILE)),
        "two": (wide, dgate_buf, slice(TILE, 2 * TILE)),
    }
    before = {
        ("down", 3): (1, 2),
        ("gate", 3): (3, 4),
        ("up", 3): (5,),
        ("one", 3): (7,),
    }
    peers = TENSOR_PEERS + tuple(("dp", bit) for bit in dp_order)
    gains = []
    turned = {}

    def turned_back(values, block):
        cosine, sine = block_angles(base_ref, step_ref, block)
        return turn(values, cosine, -sine).astype(jnp.bfloat16)

    def keep(rows, values, grouped, plain):
        dgate_buf[rows, pl.ds(grouped, HD)] = values
        hid_buf[rows, pl.ds(plain, HD)] = values

    def do_start(name):
        if name == "dm":
            loads[0].wait()
            loads[8].wait()
        else:
            dm.close()
            loads[9].start()
            loads[6].start()
            loads[6].wait()
        reduces[name].start_all()

    def do_tile(name, which):
        for i in before.get((name, which), ()):
            loads[i].wait()
        left, right, columns = sources[name]
        grad_tile(left, right, columns, reduces[name], which)
        if (name, which) == ("down", 0):
            loads[5].start()
            loads[7].start()

    def do_arrive(name, step, j, c):
        reduce = reduces[name]
        if name in targets:
            if step == last:
                finish_grad(reduce, targets[name])
            else:
                reduce.arrive(step, j, c)
        elif step == 0:
            reduce.arrive(step, j, c)
        else:
            reduce.arrive(step, j, c, {"dm": finish_dm, "feed": finish_out, "da": finish_da}[name])
            if name == "dm":
                gather.start(c)
            if name == "feed" and c == SPLIT - 1:
                for mask in (1, 2):
                    pl.semaphore_signal(
                        credit,
                        inc=1,
                        device_id={"tensor": flip(index, mask)},
                        device_id_type=MESH,
                    )
                feed.close()
                out_copy.start()
            if name == "da" and c == SPLIT - 1:
                token_copy.start()

    def do_back():
        columns = pl.ds(0, query_columns)

        def some(i, carry):
            rows = span(i * BLOCK, BLOCK)
            m_buf[rows, columns] = nn(ga_buf[rows], mixing_ref[...]).astype(jnp.bfloat16)
            return carry

        lax.fori_loop(0, slots // BLOCK, some, 0)

    def do_attention(h, block):
        group, each = h // queries_each, h % queries_each
        if h not in turned:
            turned[h] = kv_ref[:, head(group)].T
        start = block * BLOCK
        first = each == 0 and start + BLOCK == slots
        values = attention_back(
            q_ref,
            kv_ref,
            m_buf,
            begin_ref,
            lse_ref,
            turned[h],
            (key_sum, value_sum),
            h,
            group,
            start,
            first,
        )
        rows = pl.ds(start, BLOCK)
        keep(rows, turned_back(values, block), group * TILE + each * HD, h * HD)

    def do_keys(group):
        grouped = group * TILE + queries_each * HD
        plain = query_columns + group * HD

        def some(i, carry):
            rows = span(i * BLOCK, BLOCK)
            keep(rows, turned_back(key_sum[rows] * scaling, i), grouped, plain)
            keep(rows, value_sum[rows].astype(jnp.bfloat16), grouped + HD, plain + key_columns)
            return carry

        lax.fori_loop(0, slots // BLOCK, some, 0)

    def do_product(place):
        if place == 3:
            loads[9].wait()
            out_copy.wait()
            pl.semaphore_wait(credit, 2)
        block = span(flip(index, place) * BLOCK, BLOCK)

        def some(i, carry):
            cols = pl.ds(pl.multiple_of(i * 512, 512), 512)
            total = nt(hid_buf[block, pl.ds(0, query_columns)], query_ref[cols])
            total += nn(hid_buf[block, pl.ds(query_columns, key_columns)], key_ref[:, cols])
            total += nn(
                hid_buf[block, pl.ds(query_columns + key_columns, key_columns)], value_ref[:, cols]
            )
            rs_part[block, cols] = total.astype(jnp.bfloat16)
            return carry

        lax.fori_loop(0, rs_part.shape[1] // 512, some, 0)
        if place in (3, 1):
            for c in range(SPLIT):
                da.start(0, (3, 1).index(place), c)

    def do_send_gains(i):
        axis, bit = peers[i]
        copy = pltpu.make_async_remote_copy(
            src_ref=gains_ref,
            dst_ref=gains_land.at[i],
            send_sem=gains_send.at[i],
            recv_sem=gains_recv.at[i],
            device_id={axis: flip(lax.axis_index(axis), 1 << bit)},
            device_id_type=MESH,
        )
        copy.start()
        gains.append(copy)

    def do_finish(c):
        gather.near(c)
        gather.finish(c)

    def do_add_gains(i):
        gains[i].wait()
        gains_ref[...] += gains_land[i]

    actions = {
        "start": do_start,
        "tile": do_tile,
        "arrive": do_arrive,
        "forward": gather.forward,
        "finish": do_finish,
        "back": do_back,
        "attention": do_attention,
        "keys": do_keys,
        "product": do_product,
        "send": do_send_gains,
        "add": do_add_gains,
    }
    for action, *rest in plan_of(count, orders, reduces):
        actions[action](*rest)
    settle()
    token_copy.wait()
    for item in (da, gather, down, gate, up, mix, one, two):
        item.close()


def back_call(
    dm_part,
    feed_part,
    second_in,
    outer_low,
    hidden,
    gate_low,
    upward_low,
    first_in,
    tokens,
    used,
    middle,
    first_gain,
    second_gain,
    mixing_weight,
    query_weight,
    key_weight,
    value_weight,
    attended,
    queries,
    pairs,
    begin,
    log_totals,
    tables,
):
    slots, width = dm_part.shape
    rows = slots // 4
    columns = hidden.shape[1]
    heads = attended.shape[1]
    count = lax.axis_size("dp")
    dp_order = bits_of(count)
    z_order = (dp_order[1], dp_order[0]) + dp_order[2:]
    block = width // count
    share = Reduce.slots(4, SPLIT)
    total = Reduce.slots(count)

    def kernel(*refs):
        back_kernel(dp_order, z_order, *refs)

    def grad(size):
        return jax.ShapeDtypeStruct((block, size), jnp.float32)

    def low(*shape):
        return pltpu.VMEM(shape, jnp.bfloat16)

    sizes = (columns, columns, columns, heads, TILE, TILE)
    hops = 2 + len(dp_order)
    return pl.pallas_call(
        kernel,
        out_shape=(
            jax.ShapeDtypeStruct((rows, width), jnp.bfloat16),
            jax.ShapeDtypeStruct((rows, width), jnp.bfloat16),
            jax.ShapeDtypeStruct((2, width), jnp.float32),
            *(grad(size) for size in sizes),
        ),
        in_specs=[pl.BlockSpec(memory_space=pl.ANY)] * 9
        + [pl.BlockSpec(memory_space=pltpu.SMEM)]
        + vmem_specs(14),
        out_specs=tuple(
            pl.BlockSpec(memory_space=pltpu.VMEM if i == 2 else pl.ANY) for i in range(9)
        ),
        scratch_shapes=[
            low(slots, width),
            low(slots, width),
            low(slots, columns),
            low(slots, columns),
            low(slots, width),
            low(share, rows // SPLIT, width),
            low(slots, width),
            pltpu.VMEM((rows, width), jnp.float32),
            pltpu.VMEM((slots, HD), jnp.float32),
            pltpu.VMEM((slots, HD), jnp.float32),
            pltpu.VMEM((hops, 2, width), jnp.float32),
            low(rows, width),
            low(rows, width),
            *(low(width, size) for size in sizes),
            *(low(total, block, size) for size in sizes),
            pltpu.VMEM((block, columns), jnp.float32),
            pltpu.SemaphoreType.DMA,
            pltpu.SemaphoreType.DMA((2,)),
            pltpu.SemaphoreType.DMA((10,)),
            pltpu.SemaphoreType.REGULAR,
            *dma_sems(share),
            *dma_sems(share),
            *dma_sems(share),
            *dma_sems(3 * SPLIT),
            *(sem for size in sizes for sem in dma_sems(total)),
            *dma_sems(hops),
        ],
        compiler_params=pltpu.CompilerParams(
            collective_id=1, has_side_effects=True, vmem_limit_bytes=67043328
        ),
        name="back",
    )(
        dm_part,
        feed_part,
        second_in,
        outer_low,
        hidden,
        gate_low,
        upward_low,
        first_in,
        tokens,
        used,
        middle,
        first_gain.reshape(1, -1),
        second_gain.reshape(1, -1),
        mixing_weight,
        query_weight,
        key_weight,
        value_weight,
        attended,
        queries,
        pairs,
        begin,
        log_totals,
        *tables,
    )


def on_device(
    tokens,
    lengths,
    owners,
    first_gain,
    query_weight,
    key_weight,
    value_weight,
    mixing_weight,
    second_gain,
    gate_weight,
    up_weight,
    down_weight,
    cotangent,
):
    tables = rope_tables(tokens.shape[0])
    key_turned, value_turned = key_weight.T, value_weight.T
    first_in, outer_low, queries, pairs, attended, log_totals, begin, used = first_call(
        tokens,
        lengths,
        owners,
        first_gain,
        query_weight,
        key_turned,
        value_turned,
        cotangent,
        tables,
    )
    middle, second_in, hidden, gate_low, upward_low, feed_part, second_part = middle_call(
        attended,
        mixing_weight,
        second_gain,
        tokens,
        outer_low,
        gate_weight,
        up_weight,
        down_weight,
    )
    layer_output, token_grad, gains, *grads = back_call(
        second_part,
        feed_part,
        second_in,
        outer_low,
        hidden,
        gate_low,
        upward_low,
        first_in,
        tokens,
        used,
        middle,
        first_gain,
        second_gain,
        mixing_weight,
        query_weight,
        key_turned,
        value_turned,
        attended,
        queries,
        pairs,
        begin,
        log_totals,
        tables,
    )
    (
        layer_output,
        token_grad,
        down_grad,
        gate_grad,
        up_grad,
        mixing_grad,
        query_grad,
        key_grad,
        value_grad,
    ) = last_call([layer_output, token_grad, *grads], query_weight.shape[1], key_weight.shape[1])
    return (
        layer_output,
        token_grad,
        gains[0],
        query_grad,
        key_grad,
        value_grad,
        mixing_grad,
        gains[1],
        gate_grad,
        up_grad,
        down_grad,
    )


def solution(mesh):
    in_specs = (
        P("dp", None),
        P(),
        P(),
        P(),
        P(None, "tensor"),
        P(None, "tensor"),
        P(None, "tensor"),
        P(None, "tensor"),
        P(),
        P(None, "tensor"),
        P(None, "tensor"),
        P(None, "tensor"),
        P("dp", None),
    )
    out_specs = (
        P(("dp", "tensor"), None),
        P(("dp", "tensor"), None),
        P(),
        P("dp", "tensor"),
        P("dp", "tensor"),
        P("dp", "tensor"),
        P("dp", "tensor"),
        P(),
        P("dp", "tensor"),
        P("dp", "tensor"),
        P("dp", "tensor"),
    )
    return jax.shard_map(
        on_device, mesh=mesh, in_specs=in_specs, out_specs=out_specs, check_vma=False
    )
```

```python
import jax
import jax.numpy as jnp
import numpy as np
from jax import lax
from jax.experimental import pallas as pl
from jax.experimental.pallas import tpu as pltpu
from jax.sharding import PartitionSpec as P

HD = 96

MESH = pl.DeviceIdType.MESH

epsilon = 1e-05
rope_base = 10000.0


def bits_of(count):
    return tuple(range(count.bit_length() - 1))


def nn(left, right):
    return jnp.dot(left, right, preferred_element_type=jnp.float32)


def nt(left, right):
    return lax.dot_general(left, right, (((1,), (1,)), ((), ())), preferred_element_type=jnp.float32)


def tn(left, right):
    return lax.dot_general(left, right, (((0,), (0,)), ((), ())), preferred_element_type=jnp.float32)


def flip(index, mask):
    result = index
    bit = 0
    while mask >> bit:
        if (mask >> bit) & 1:
            result = result + (1 << bit) * (1 - 2 * lax.rem(lax.div(index, 1 << bit), 2))
        bit += 1
    return result


def span(start, size, step=16):
    return pl.ds(pl.multiple_of(start, step), size)


def greet(peers):
    barrier = pltpu.get_barrier_semaphore()
    for axis, bit in peers:
        index = lax.axis_index(axis)
        pl.semaphore_signal(
            barrier, inc=1, device_id={axis: flip(index, 1 << bit)}, device_id_type=MESH
        )
    pl.semaphore_wait(barrier, len(peers))


def chunk_rows(rows):
    for size in (16,):
        if rows % size == 0:
            return size
    return rows


class Reduce:
    def __init__(self, part, landing, send_sems, recv_sems, axis, order, split=1):
        self.part, self.landing = part, landing
        self.send_sems, self.recv_sems = send_sems, recv_sems
        self.axis, self.order, self.split = axis, order, split
        self.index = lax.axis_index(axis)
        self.rows = part.shape[0] >> len(order)
        self.piece = self.rows // split
        self.copies = {}
        self.lists = []
        base = 0
        for step in range(len(order)):
            kept = [0]
            for bit in reversed(order[step + 1 :]):
                kept = [place | (1 << bit) for place in kept] + kept
            self.lists.append((kept, base))
            base += len(kept) * split

    @staticmethod
    def slots(count, split=1):
        return (count - 1) * split

    def units(self, step):
        kept, _ = self.lists[step]
        return [(j, c) for j in range(len(kept)) for c in range(self.split)]

    def start(self, step, j, c=0):
        kept, base = self.lists[step]
        mask = 1 << self.order[step]
        slot = base + j * self.split + c
        source = flip(self.index, kept[j] | mask) * self.rows + c * self.piece
        copy = pltpu.make_async_remote_copy(
            src_ref=self.part.at[span(source, self.piece)],
            dst_ref=self.landing.at[slot],
            send_sem=self.send_sems.at[slot],
            recv_sem=self.recv_sems.at[slot],
            device_id={self.axis: flip(self.index, mask)},
            device_id_type=MESH,
        )
        copy.start()
        self.copies[slot] = copy

    def arrive(self, step, j, c=0, store=None):
        kept, base = self.lists[step]
        slot = base + j * self.split + c
        self.copies[slot].wait_recv()
        start = flip(self.index, kept[j]) * self.rows + c * self.piece
        size = chunk_rows(self.piece)

        def add(i, carry):
            rows = span(start + i * size, size)
            other = self.landing[slot, span(i * size, size)]
            total = self.part[rows].astype(jnp.float32) + other.astype(jnp.float32)
            if store is None:
                self.part[rows] = total.astype(self.part.dtype)
            else:
                store(c * self.piece + i * size, size, total)
            return carry

        lax.fori_loop(0, self.piece // size, add, 0)
        if step + 1 < len(self.order):
            later, _ = self.lists[step + 1]
            mask = 1 << self.order[step + 1]
            if kept[j] & mask:
                self.start(step + 1, later.index(kept[j] ^ mask), c)

    def start_all(self):
        for j, c in self.units(0):
            self.start(0, j, c)

    def arrive_all(self, step, store=None):
        for j, c in self.units(step):
            self.arrive(step, j, c, store)

    def close(self):
        for copy in self.copies.values():
            copy.wait_send()


class Gather:
    def __init__(self, whole, send_sems, recv_sems, split=1):
        self.whole, self.split = whole, split
        self.send_sems, self.recv_sems = send_sems, recv_sems
        self.index = lax.axis_index("tensor")
        self.rows = whole.shape[0] // 4
        self.piece = self.rows // split
        self.copies = {}

    def send(self, kind, c):
        mask = (2, 1, 1)[kind]
        block = flip(self.index, 2) if kind == 2 else self.index
        rows = span(block * self.rows + c * self.piece, self.piece)
        slot = kind * self.split + c
        copy = pltpu.make_async_remote_copy(
            src_ref=self.whole.at[rows],
            dst_ref=self.whole.at[rows],
            send_sem=self.send_sems.at[slot],
            recv_sem=self.recv_sems.at[slot],
            device_id={"tensor": flip(self.index, mask)},
            device_id_type=MESH,
        )
        copy.start()
        self.copies[kind, c] = copy

    def start(self, c):
        self.send(0, c)
        self.send(1, c)

    def forward(self, c):
        self.copies[0, c].wait_recv()
        self.send(2, c)

    def near(self, c):
        self.copies[1, c].wait_recv()

    def finish(self, c):
        self.copies[2, c].wait_recv()

    def close(self):
        for copy in self.copies.values():
            copy.wait_send()


TENSOR_PEERS = (("tensor", 0), ("tensor", 1))
SPLIT = 4


def middle_kernel(
    o_ref,
    w_ref,
    gain_ref,
    tokens_hbm,
    gm_hbm,
    gate_hbm,
    up_hbm,
    down_hbm,
    h_ref,
    m_hbm,
    hid_hbm,
    dgate_hbm,
    dup_hbm,
    feed_hbm,
    dm_hbm,
    part,
    landing,
    m_buf,
    x_buf,
    gm_buf,
    gate_w,
    up_w,
    down_w,
    hid_buf,
    dgate_buf,
    dup_buf,
    rs_send,
    rs_recv,
    ag_send,
    ag_recv,
    load_sems,
    leave_sems,
    feed_buf,
):
    index = lax.axis_index("tensor")
    rows = o_ref.shape[0] // 4
    loads = [
        pltpu.make_async_copy(source, target, load_sems.at[i])
        for i, (source, target) in enumerate(
            (
                (tokens_hbm.at[span(index * rows, rows)], x_buf),
                (gate_hbm, gate_w),
                (up_hbm, up_w),
                (gm_hbm, gm_buf),
                (down_hbm, down_w),
            )
        )
    ]
    for load in loads:
        load.start()
    greet(TENSOR_PEERS)
    reduce = Reduce(part, landing, rs_send, rs_recv, "tensor", (0, 1), SPLIT)
    gather = Gather(m_buf, ag_send, ag_recv, SPLIT)
    leaving = []

    def leave(buffer, target, half):
        there = span(half * 2 * rows, 2 * rows)
        copy = pltpu.make_async_copy(
            buffer.at[there], target.at[there], leave_sems.at[len(leaving)]
        )
        copy.start()
        leaving.append(copy)

    def product(place):
        block = span(flip(index, place) * rows, rows)
        columns = 512

        def tile(i, carry):
            cols = pl.ds(pl.multiple_of(i * columns, columns), columns)
            part[block, cols] = nt(o_ref[block], w_ref[cols]).astype(jnp.bfloat16)
            return carry

        lax.fori_loop(0, part.shape[1] // columns, tile, 0)

    def normed(start, size, total):
        own = span(start, size)
        hidden = x_buf[own].astype(jnp.float32) + total
        h_ref[own] = hidden
        inverse = lax.rsqrt(jnp.mean(hidden * hidden, axis=-1, keepdims=True) + epsilon)
        m_buf[span(index * rows + start, size)] = (hidden * inverse * gain_ref[...]).astype(
            jnp.bfloat16
        )

    def hidden_part(half, first, last):
        there = span(half * 2 * rows, 2 * rows)
        columns = 256

        def tile(i, carry):
            cols = pl.ds(pl.multiple_of(i * columns, columns), columns)
            gate = nn(m_buf[there], gate_w[:, cols])
            upward = nn(m_buf[there], up_w[:, cols])
            grad = nn(gm_buf[there], down_w[:, cols])
            sigmoid = 1.0 / (1.0 + jnp.exp(-gate))
            activated = gate * sigmoid
            hid_buf[there, cols] = (activated * upward).astype(jnp.bfloat16)
            dgate_buf[there, cols] = (
                grad * upward * sigmoid * (1.0 + gate * (1.0 - sigmoid))
            ).astype(jnp.bfloat16)
            dup_buf[there, cols] = (grad * activated).astype(jnp.bfloat16)
            return carry

        lax.fori_loop(first, last, tile, 0)

    def feed_part(half):
        there = span(half * 2 * rows, 2 * rows)

        def tile(i, carry):
            cols = pl.ds(pl.multiple_of(i * 512, 512), 512)
            feed_buf[there, cols] = nt(hid_buf[there], down_w[cols]).astype(jnp.bfloat16)
            return carry

        lax.fori_loop(0, feed_buf.shape[1] // 512, tile, 0)

    def dm_part(half):
        there = span(half * 2 * rows, 2 * rows)

        def tile(i, carry):
            cols = pl.ds(pl.multiple_of(i * 512, 512), 512)
            total = nt(dgate_buf[there], gate_w[cols]) + nt(dup_buf[there], up_w[cols])
            part[there, cols] = total.astype(jnp.bfloat16)
            return carry

        lax.fori_loop(0, part.shape[1] // 512, tile, 0)

    product(3)
    for c in range(SPLIT):
        reduce.start(0, 0, c)
    product(2)
    for c in range(SPLIT):
        reduce.arrive(0, 0, c)
    product(1)
    for c in range(SPLIT):
        reduce.start(0, 1, c)
    product(0)
    for c in range(SPLIT):
        reduce.arrive(0, 1, c)
    loads[0].wait()
    for c in range(SPLIT):
        reduce.arrive(1, 0, c, normed)
        gather.start(c)
    near = lax.div(index, 2)
    far = 1 - near
    for load in loads[1:]:
        load.wait()
    for c in range(SPLIT):
        gather.near(c)
    reduce.close()
    tiles = hid_buf.shape[1] // 256
    hidden_part(near, 0, tiles // 2)
    gather.forward(0)
    hidden_part(near, tiles // 2, tiles)
    gather.forward(1)
    leave(hid_buf, hid_hbm, near)
    leave(dgate_buf, dgate_hbm, near)
    leave(dup_buf, dup_hbm, near)
    leave(m_buf, m_hbm, near)
    feed_part(near)
    leave(feed_buf, feed_hbm, near)
    gather.forward(2)
    dm_part(near)
    leave(part, dm_hbm, near)
    for c in range(3, SPLIT):
        gather.forward(c)
    for c in range(SPLIT):
        gather.finish(c)
    leave(m_buf, m_hbm, far)
    hidden_part(far, 0, tiles)
    leave(hid_buf, hid_hbm, far)
    leave(dgate_buf, dgate_hbm, far)
    leave(dup_buf, dup_hbm, far)
    feed_part(far)
    leave(feed_buf, feed_hbm, far)
    dm_part(far)
    leave(part, dm_hbm, far)
    for copy in leaving:
        copy.wait()
    gather.close()


def vmem_specs(count):
    return [pl.BlockSpec(memory_space=pltpu.VMEM)] * count


def dma_sems(count):
    return [pltpu.SemaphoreType.DMA((count,)), pltpu.SemaphoreType.DMA((count,))]


def middle_call(
    attended, mixing_weight, second_gain, tokens, outer_low, gate_weight, up_weight, down_weight
):
    slots, width = tokens.shape
    rows = slots // 4
    columns = gate_weight.shape[1]
    count = Reduce.slots(4, SPLIT)

    def low(*shape):
        return pltpu.VMEM(shape, jnp.bfloat16)

    def result(size):
        return jax.ShapeDtypeStruct((slots, size), jnp.bfloat16)

    return pl.pallas_call(
        middle_kernel,
        out_shape=(
            jax.ShapeDtypeStruct((rows, width), jnp.float32),
            result(width),
            result(columns),
            result(columns),
            result(columns),
            result(width),
            result(width),
        ),
        in_specs=vmem_specs(3) + [pl.BlockSpec(memory_space=pl.ANY)] * 5,
        out_specs=tuple(vmem_specs(1) + [pl.BlockSpec(memory_space=pl.ANY)] * 6),
        scratch_shapes=[
            low(slots, width),
            low(count, rows // SPLIT, width),
            low(slots, width),
            low(rows, width),
            low(slots, width),
            low(width, columns),
            low(width, columns),
            low(width, columns),
            low(slots, columns),
            low(slots, columns),
            low(slots, columns),
            *dma_sems(count),
            *dma_sems(3 * SPLIT),
            pltpu.SemaphoreType.DMA((5,)),
            pltpu.SemaphoreType.DMA((12,)),
            low(slots, width),
        ],
        compiler_params=pltpu.CompilerParams(
            collective_id=0, has_side_effects=True, vmem_limit_bytes=67043328
        ),
        name="middle",
    )(
        attended,
        mixing_weight,
        second_gain.reshape(1, -1),
        tokens,
        outer_low,
        gate_weight,
        up_weight,
        down_weight,
    )


BLOCK = 256
TILE = 384


def head(index):
    return pl.ds(index * HD, HD)


def allowed_keys(begin_row, query_start, key_count, query_count):
    keys = lax.broadcasted_iota(jnp.int32, (key_count, query_count), 0)
    queries = query_start + lax.broadcasted_iota(jnp.int32, (key_count, query_count), 1)
    return (keys >= begin_row) & (keys <= queries)


def rope_tables(slots):
    half = HD // 2
    frequency = rope_base ** (-2.0 * np.arange(half) / HD)

    def table(places):
        angles = places[:, None] * frequency[None, :]
        return np.concatenate([np.cos(angles), np.sin(angles)], axis=1).astype(np.float32)

    return (
        jnp.asarray(table(np.arange(BLOCK))),
        jnp.asarray(table(np.arange(max(8, slots // BLOCK)) * BLOCK)),
    )


def block_angles(base_ref, step_ref, block):
    half = HD // 2
    low_cos, low_sin = base_ref[:, pl.ds(0, half)], base_ref[:, pl.ds(half, half)]
    high = step_ref[pl.ds(block, 1)]
    high_cos, high_sin = high[:, :half], high[:, half:]
    return (low_cos * high_cos - low_sin * high_sin, low_sin * high_cos + low_cos * high_sin)


def turn(values, cosine, sine):
    half = HD // 2
    first, second = values[:, :half], values[:, half:]
    return jnp.concatenate([first * cosine - second * sine, second * cosine + first * sine], axis=1)


def first_kernel(
    blocks,
    lengths_ref,
    owners_ref,
    x_ref,
    cot_ref,
    gain_ref,
    wq_ref,
    wk_ref,
    wv_ref,
    base_ref,
    step_ref,
    a_ref,
    gm_ref,
    q_ref,
    kv_ref,
    o_ref,
    lse_ref,
    begin_ref,
    used_ref,
    kept,
    turned,
    o_heads,
):
    block = pl.program_id(0)
    index = lax.axis_index("dp")
    slots = block * BLOCK + lax.broadcasted_iota(jnp.int32, (1, BLOCK), 1)

    def sequence(s, carry):
        total, begin = carry
        length = jnp.where(owners_ref[s] == index, lengths_ref[s], 0)
        begin = jnp.where((slots >= total) & (slots < total + length), total, begin)
        return total + length, begin

    used, begin = lax.fori_loop(0, lengths_ref.shape[0], sequence, (jnp.int32(0), slots))
    begin_ref[...] = begin
    used_ref[0] = used
    size = 64

    def rows_in(i, carry):
        rows = span(i * size, size)
        values = x_ref[rows].astype(jnp.float32)
        inverse = lax.rsqrt(jnp.mean(values * values, axis=-1, keepdims=True) + epsilon)
        a_ref[rows] = (values * inverse * gain_ref[...]).astype(jnp.bfloat16)
        places = block * BLOCK + i * size + lax.broadcasted_iota(jnp.int32, (size, 1), 0)
        live = (places < used).astype(jnp.float32)
        gm_ref[rows] = (cot_ref[rows].astype(jnp.float32) * live).astype(jnp.bfloat16)
        return carry

    lax.fori_loop(0, BLOCK // size, rows_in, 0)
    cosine, sine = block_angles(base_ref, step_ref, block)
    normed = a_ref[...]
    queries = nn(normed, wq_ref[...])
    query_heads, key_heads = queries.shape[1] // HD, wk_ref.shape[0] // HD
    for h in range(query_heads):
        piece = queries[:, h * HD : (h + 1) * HD]
        q_ref[h] = turn(piece, cosine, sine).astype(jnp.bfloat16)
    keys = nt(normed, wk_ref[...])
    here = span(block * BLOCK, BLOCK)
    for h in range(key_heads):
        piece = turn(keys[:, h * HD : (h + 1) * HD], cosine, sine).astype(jnp.bfloat16)
        kv_ref[h] = piece
        kept[h, here] = piece
    values = nt(normed, wv_ref[...]).astype(jnp.bfloat16)
    for h in range(key_heads):
        kv_ref[key_heads + h] = values[:, h * HD : (h + 1) * HD]
    scaling = HD ** (-0.5)
    groups = query_heads // key_heads

    def attend(now):
        stop = (now + 1) * BLOCK
        for h in range(key_heads):
            turned[h, :, pl.ds(now * BLOCK, BLOCK)] = kv_ref[key_heads + h].T
        allowed = allowed_keys(begin, now * BLOCK, stop, BLOCK)

        def one_head(h, carry):
            group = lax.div(h, groups)
            scores = nt(kept[group, pl.ds(0, stop)], q_ref[h]) * scaling
            scores = jnp.where(allowed, scores, -jnp.inf)
            highest = jnp.max(scores, axis=0, keepdims=True)
            exponent = jnp.exp(scores - highest)
            total = jnp.sum(exponent, axis=0, keepdims=True)
            weights = (exponent * (1.0 / total)).astype(jnp.bfloat16)
            mixed = nn(turned[group, :, pl.ds(0, stop)], weights)
            o_heads[h] = mixed.T.astype(jnp.bfloat16)
            lse_ref[pl.ds(h, 1)] = highest + jnp.log(total)
            return carry

        lax.fori_loop(0, query_heads, one_head, 0)

    for now in range(blocks):
        pl.when(block == now)(lambda now=now: attend(now))
    for h in range(query_heads):
        o_ref[:, head(h)] = o_heads[h]


def first_call(
    tokens, lengths, owners, first_gain, query_weight, key_weight, value_weight, cotangent, tables
):
    slots, width = tokens.shape
    blocks = slots // BLOCK
    columns, pairs = query_weight.shape[1], 2 * key_weight.shape[0] // HD
    heads = columns // HD

    def kernel(*refs):
        first_kernel(blocks, *refs)

    def rows_of(size):
        return pl.BlockSpec((BLOCK, size), lambda i: (i, 0))

    def whole(array):
        return pl.BlockSpec(array.shape, lambda i: (0, 0), pipeline_mode=pl.Buffered(1))

    gain = first_gain.reshape(1, -1)
    scalars = pl.BlockSpec(memory_space=pltpu.SMEM)
    return pl.pallas_call(
        kernel,
        grid=(blocks,),
        out_shape=(
            jax.ShapeDtypeStruct((slots, width), jnp.bfloat16),
            jax.ShapeDtypeStruct((slots, width), jnp.bfloat16),
            jax.ShapeDtypeStruct((heads, slots, HD), jnp.bfloat16),
            jax.ShapeDtypeStruct((pairs, slots, HD), jnp.bfloat16),
            jax.ShapeDtypeStruct((slots, columns), jnp.bfloat16),
            jax.ShapeDtypeStruct((heads, slots), jnp.float32),
            jax.ShapeDtypeStruct((1, slots), jnp.int32),
            jax.ShapeDtypeStruct((1,), jnp.int32),
        ),
        in_specs=[
            scalars,
            scalars,
            rows_of(width),
            rows_of(width),
            whole(gain),
            whole(query_weight),
            whole(key_weight),
            whole(value_weight),
            whole(tables[0]),
            whole(tables[1]),
        ],
        out_specs=(
            rows_of(width),
            rows_of(width),
            pl.BlockSpec((heads, BLOCK, HD), lambda i: (0, i, 0)),
            pl.BlockSpec((pairs, BLOCK, HD), lambda i: (0, i, 0)),
            rows_of(columns),
            pl.BlockSpec((heads, BLOCK), lambda i: (0, i)),
            pl.BlockSpec((1, BLOCK), lambda i: (0, i)),
            scalars,
        ),
        scratch_shapes=[
            pltpu.VMEM((pairs // 2, slots, HD), jnp.bfloat16),
            pltpu.VMEM((pairs // 2, HD, slots), jnp.bfloat16),
            pltpu.VMEM((heads, BLOCK, HD), jnp.bfloat16),
        ],
        compiler_params=pltpu.CompilerParams(vmem_limit_bytes=67043328),
        name="first",
    )(
        lengths,
        owners,
        tokens,
        cotangent,
        gain,
        query_weight,
        key_weight,
        value_weight,
        *tables,
    )


def last_kernel(group_columns, *refs):
    sources, targets, buffers = refs[:8], refs[8:17], refs[17:28]
    in_sems, out_sems = refs[28:]
    out, token, down, gate, up, mix, one, two = buffers[:8]
    turned = buffers[8:]
    coming = [
        pltpu.make_async_copy(source, buffer, in_sems.at[i])
        for i, (source, buffer) in enumerate(zip(sources, buffers[:8]))
    ]
    for copy in coming:
        copy.start()
    leaving = []

    def leave(buffer):
        i = len(leaving)
        copy = pltpu.make_async_copy(buffer, targets[i], out_sems.at[i])
        copy.start()
        leaving.append(copy)

    for i in (0, 1, 2, 3, 4, 5):
        coming[i].wait()
        leave(buffers[i])
    start = 0
    coming[6].wait()
    coming[7].wait()
    for buffer in turned:
        each = buffer.shape[1] // 2
        buffer[:, pl.ds(0, each)] = one[:, pl.ds(start, each)]
        buffer[:, pl.ds(each, each)] = two[:, pl.ds(start, each)]
        start += each
        leave(buffer)
    for copy in leaving:
        copy.wait()


def last_call(arrays, query_columns, key_columns):
    rows = arrays[6].shape[0]
    shapes = [jax.ShapeDtypeStruct(array.shape, array.dtype) for array in arrays[:6]]
    shapes += [
        jax.ShapeDtypeStruct((rows, size), jnp.float32)
        for size in (query_columns, key_columns, key_columns)
    ]

    def kernel(*refs):
        last_kernel(TILE, *refs)

    buffers = [pltpu.VMEM(array.shape, array.dtype) for array in arrays]
    buffers += [pltpu.VMEM(shape.shape, shape.dtype) for shape in shapes[6:]]
    return pl.pallas_call(
        kernel,
        out_shape=tuple(shapes),
        in_specs=[pl.BlockSpec(memory_space=pl.ANY)] * 8,
        out_specs=tuple([pl.BlockSpec(memory_space=pl.ANY)] * 9),
        scratch_shapes=[
            *buffers,
            pltpu.SemaphoreType.DMA((8,)),
            pltpu.SemaphoreType.DMA((9,)),
        ],
        compiler_params=pltpu.CompilerParams(vmem_limit_bytes=67043328),
        name="last",
    )(*arrays)


def lanes(index):
    return pl.ds(pl.multiple_of(index * 128, 128), HD)


def attention_back(q_ref, kv_ref, grads, begin_ref, lse_ref, turned, sums, heads, group, start, leave):
    scaling = HD ** (-0.5)
    key_sum, value_sum = sums
    key_heads = kv_ref.shape[0] // 2
    stop = start + BLOCK
    rows = pl.ds(start, BLOCK)
    seen = pl.ds(0, stop)
    if stop == q_ref.shape[1]:
        key_sum[...] = jnp.zeros_like(key_sum)
        value_sum[...] = jnp.zeros_like(value_sum)
    allowed = allowed_keys(begin_ref[:, rows], start, stop, BLOCK)

    def one_head(h, carry):
        query = q_ref[h, rows]
        grad = grads[rows, lanes(h)]
        scores = nt(kv_ref[group, seen], query) * scaling
        weights = jnp.where(allowed, jnp.exp(scores - lse_ref[pl.ds(h, 1), rows]), 0.0)
        weights_grad = nt(kv_ref[key_heads + group, seen], grad)
        inner = jnp.sum(weights * weights_grad, axis=0, keepdims=True)
        scores_grad = (weights * (weights_grad - inner)).astype(jnp.bfloat16)
        value_sum[seen] += nn(weights.astype(jnp.bfloat16), grad)
        key_sum[seen] += nn(scores_grad, query)
        leave(h, rows, nn(turned[:, :stop], scores_grad).T * scaling)
        return carry

    lax.fori_loop(heads[0], heads[1], one_head, 0)


P_START = "start"
P_TILE = "tile"
P_ARRIVE = "arrive"
P_FORWARD = "forward"
P_FINISH = "finish"
P_BACK = "back"
P_ATTENTION = "attention"
P_KEYS = "keys"
P_PRODUCT = "product"
P_SEND = "send"
P_ADD = "add"
P_DM = "dm"
P_FEED = "feed"
P_DA = "da"
P_DOWN = "down"
P_GATE = "gate"
P_UP = "up"
P_MIX = "mix"
P_ONE = "one"
P_TWO = "two"

PLAN = (
    (P_TILE, P_GATE, 3),
    (P_TILE, P_DOWN, 3),
    (P_START, P_DM),
    (P_TILE, P_GATE, 1),
    (P_ARRIVE, P_DM, 0, 0, 2),
    (P_ARRIVE, P_DM, 0, 1, 1),
    (P_ARRIVE, P_DM, 0, 1, 0),
    (P_ARRIVE, P_DM, 0, 0, 0),
    (P_TILE, P_DOWN, 1),
    (P_TILE, P_GATE, 2),
    (P_ARRIVE, P_DM, 0, 0, 1),
    (P_TILE, P_DOWN, 2),
    (P_ARRIVE, P_DM, 0, 1, 3),
    (P_ARRIVE, P_DM, 1, 0, 1),
    (P_ARRIVE, P_DM, 0, 1, 2),
    (P_ARRIVE, P_DM, 0, 0, 3),
    (P_ARRIVE, P_GATE, 0, 0, 0),
    (P_TILE, P_GATE, 0),
    (P_ARRIVE, P_GATE, 0, 1, 0),
    (P_FORWARD, 1),
    (P_TILE, P_DOWN, 0),
    (P_ARRIVE, P_DOWN, 0, 2, 0),
    (P_ARRIVE, P_GATE, 0, 2, 0),
    (P_ARRIVE, P_DOWN, 0, 0, 0),
    (P_ARRIVE, P_DM, 1, 0, 2),
    (P_TILE, P_UP, 3),
    (P_ARRIVE, P_DM, 1, 0, 0),
    (P_TILE, P_UP, 1),
    (P_FINISH, 1),
    (P_TILE, P_UP, 2),
    (P_ARRIVE, P_DM, 1, 0, 3),
    (P_FORWARD, 0),
    (P_TILE, P_UP, 0),
    (P_ARRIVE, P_DOWN, 0, 1, 0),
    (P_FORWARD, 2),
    (P_ARRIVE, P_GATE, 0, 3, 0),
    (P_FINISH, 0),
    (P_FORWARD, 3),
    (P_FINISH, 3),
    (P_ARRIVE, P_DOWN, 1, 0, 0),
    (P_FINISH, 2),
    (P_START, P_FEED),
    (P_ARRIVE, P_FEED, 0, 0, 0),
    (P_TILE, P_MIX, 3),
    (P_ARRIVE, P_FEED, 0, 0, 1),
    (P_ARRIVE, P_FEED, 0, 0, 2),
    (P_TILE, P_MIX, 1),
    (P_TILE, P_MIX, 2),
    (P_TILE, P_MIX, 0),
    (P_ARRIVE, P_FEED, 0, 1, 1),
    (P_ARRIVE, P_FEED, 0, 0, 3),
    (P_ARRIVE, P_UP, 0, 0, 0),
    (P_ARRIVE, P_GATE, 1, 0, 0),
    (P_BACK,),
    (P_ARRIVE, P_FEED, 1, 0, 1),
    (P_ATTENTION, 0, 3),
    (P_ARRIVE, P_UP, 0, 1, 0),
    (P_ARRIVE, P_FEED, 0, 1, 0),
    (P_ARRIVE, P_DOWN, 0, 3, 0),
    (P_ATTENTION, 0, 2),
    (P_ATTENTION, 0, 1),
    (P_ATTENTION, 0, 0),
    (P_KEYS, 0),
    (P_ARRIVE, P_FEED, 1, 0, 0),
    (P_TILE, P_ONE, 3),
    (P_TILE, P_ONE, 1),
    (P_ARRIVE, P_GATE, 1, 1, 0),
    (P_TILE, P_ONE, 2),
    (P_TILE, P_ONE, 0),
    (P_ARRIVE, P_FEED, 0, 1, 2),
    (P_ARRIVE, P_FEED, 1, 0, 2),
    (P_ATTENTION, 1, 3),
    (P_ATTENTION, 1, 2),
    (P_ARRIVE, P_FEED, 0, 1, 3),
    (P_ARRIVE, P_UP, 0, 2, 0),
    (P_ARRIVE, P_FEED, 1, 0, 3),
    (P_ATTENTION, 1, 1),
    (P_ATTENTION, 1, 0),
    (P_ARRIVE, P_MIX, 0, 0, 0),
    (P_ARRIVE, P_UP, 1, 0, 0),
    (P_ARRIVE, P_GATE, 2, 0, 0),
    (P_KEYS, 1),
    (P_ARRIVE, P_DOWN, 1, 1, 0),
    (P_ARRIVE, P_DOWN, 2, 0, 0),
    (P_TILE, P_TWO, 3),
    (P_TILE, P_TWO, 1),
    (P_TILE, P_TWO, 2),
    (P_TILE, P_TWO, 0),
    (P_PRODUCT, 3),
    (P_PRODUCT, 1),
    (P_PRODUCT, 2),
    (P_ARRIVE, P_DA, 0, 0, 1),
    (P_PRODUCT, 0),
    (P_ARRIVE, P_DA, 0, 1, 1),
    (P_ARRIVE, P_DA, 0, 0, 0),
    (P_ARRIVE, P_MIX, 0, 1, 0),
    (P_ARRIVE, P_DA, 0, 0, 3),
    (P_ARRIVE, P_UP, 0, 3, 0),
    (P_ARRIVE, P_DA, 0, 1, 0),
    (P_ARRIVE, P_ONE, 0, 0, 0),
    (P_ARRIVE, P_DA, 0, 1, 2),
    (P_ARRIVE, P_MIX, 0, 2, 0),
    (P_ARRIVE, P_DA, 1, 0, 0),
    (P_ARRIVE, P_MIX, 0, 3, 0),
    (P_ARRIVE, P_MIX, 1, 0, 0),
    (P_ARRIVE, P_DA, 0, 0, 2),
    (P_ARRIVE, P_DA, 1, 0, 1),
    (P_ARRIVE, P_ONE, 0, 1, 0),
    (P_ARRIVE, P_ONE, 0, 2, 0),
    (P_ARRIVE, P_TWO, 0, 0, 0),
    (P_ARRIVE, P_MIX, 1, 1, 0),
    (P_ARRIVE, P_TWO, 0, 1, 0),
    (P_ARRIVE, P_DA, 1, 0, 2),
    (P_ARRIVE, P_UP, 1, 1, 0),
    (P_ARRIVE, P_DA, 0, 1, 3),
    (P_ARRIVE, P_DA, 1, 0, 3),
    (P_SEND, 0),
    (P_ARRIVE, P_TWO, 0, 2, 0),
    (P_ADD, 0),
    (P_ARRIVE, P_ONE, 1, 0, 0),
    (P_ARRIVE, P_UP, 2, 0, 0),
    (P_SEND, 1),
    (P_ADD, 1),
    (P_SEND, 2),
    (P_ADD, 2),
    (P_SEND, 3),
    (P_ARRIVE, P_TWO, 1, 0, 0),
    (P_ADD, 3),
    (P_ARRIVE, P_ONE, 0, 3, 0),
    (P_ARRIVE, P_MIX, 2, 0, 0),
    (P_ARRIVE, P_TWO, 0, 3, 0),
    (P_ARRIVE, P_TWO, 1, 1, 0),
    (P_ARRIVE, P_ONE, 1, 1, 0),
    (P_ARRIVE, P_ONE, 2, 0, 0),
    (P_SEND, 4),
    (P_ARRIVE, P_TWO, 2, 0, 0),
    (P_ADD, 4),
)


def plan_of(count, orders, reduces):
    if count == 8:
        return PLAN
    tiles = (3, 1, 2, 0)

    def units(name, step):
        return [(P_ARRIVE, name, step, j, c) for j, c in reduces[name].units(step)]

    plan = [(P_START, P_DM)]
    plan += [(P_TILE, name, which) for name in (P_DOWN, P_GATE, P_UP) for which in tiles]
    plan += units(P_DM, 0) + units(P_DM, 1)
    plan += [(P_FORWARD, c) for c in range(SPLIT)] + [(P_FINISH, c) for c in range(SPLIT)]
    plan += [(P_START, P_FEED)] + [(P_TILE, P_MIX, which) for which in tiles] + [(P_BACK,)]
    for group in range(2):
        plan += [(P_ATTENTION, group, block) for block in (3, 2, 1, 0)]
        plan += [(P_KEYS, group)]
        plan += [(P_TILE, (P_ONE, P_TWO)[group], which) for which in tiles]
    plan += units(P_FEED, 0) + units(P_FEED, 1)
    plan += [(P_PRODUCT, place) for place in (3, 1, 2, 0)] + units(P_DA, 0) + units(P_DA, 1)
    names = (P_DOWN, P_GATE, P_UP, P_MIX, P_ONE, P_TWO)
    for step in range(len(orders[0])):
        for name in names:
            plan += units(name, step)
    for i in range(2 + len(orders[0])):
        plan += [(P_SEND, i), (P_ADD, i)]
    return plan


def back_kernel(
    dp_order,
    z_order,
    dm_hbm,
    feed_hbm,
    m_hbm,
    gm_hbm,
    hid_hbm,
    dgate_hbm,
    dup_hbm,
    a_hbm,
    tokens_hbm,
    used_ref,
    h_ref,
    gain1_ref,
    gain2_ref,
    mixing_ref,
    query_ref,
    key_ref,
    value_ref,
    o_ref,
    q_ref,
    kv_ref,
    begin_ref,
    lse_ref,
    base_ref,
    step_ref,
    out_ref,
    token_ref,
    gains_ref,
    down_ref,
    gate_ref,
    up_ref,
    mix_ref,
    one_ref,
    two_ref,
    *scratch,
):
    (
        wide,
        m_buf,
        hid_buf,
        dgate_buf,
        rs_part,
        rs_land,
        ga_buf,
        dh_buf,
        key_sum,
        value_sum,
        gains_land,
        cot_ref,
        result,
        *scratch,
    ) = scratch
    parts, lands, sems = scratch[:6], scratch[6:12], scratch[12:]
    stage, stage_sem, out_sem, load_sems, credit, *sems = sems
    index = lax.axis_index("tensor")
    dp_index = lax.axis_index("dp")
    count = 1 << len(dp_order)

    own_rows = span(index * h_ref.shape[0], h_ref.shape[0])
    loads = [
        pltpu.make_async_copy(source, target, load_sems.at[i])
        for i, (source, target) in enumerate(
            (
                (dm_hbm, rs_part),
                (gm_hbm, wide),
                (hid_hbm, hid_buf),
                (m_hbm, m_buf),
                (dgate_hbm, dgate_buf),
                (dup_hbm, hid_buf),
                (feed_hbm, rs_part),
                (a_hbm, wide),
                (gm_hbm.at[own_rows], cot_ref),
                (tokens_hbm.at[own_rows], cot_ref),
            )
        )
    ]
    for i in (3, 4, 1, 2, 0, 8):
        loads[i].start()
    greet(TENSOR_PEERS + tuple(("dp", bit) for bit in dp_order))

    def share_reduce(first_sem):
        return Reduce(rs_part, rs_land, sems[first_sem], sems[first_sem + 1], "tensor", (0, 1), SPLIT)

    dm, feed, da = share_reduce(0), share_reduce(2), share_reduce(4)
    gather = Gather(ga_buf, sems[6], sems[7], SPLIT)
    orders = (z_order, dp_order, dp_order, dp_order, dp_order, dp_order)
    down, gate, up, mix, one, two = (
        Reduce(parts[i], lands[i], sems[8 + 2 * i], sems[9 + 2 * i], "dp", orders[i])
        for i in range(6)
    )
    gains_send, gains_recv = sems[20], sems[21]
    gains_ref[...] = jnp.zeros_like(gains_ref)

    def finish_out(start, size, total):
        own = span(start, size)
        places = index * h_ref.shape[0] + start + lax.broadcasted_iota(jnp.int32, (size, 1), 0)
        live = (places < used_ref[0]).astype(jnp.float32)
        result[own] = ((h_ref[own] + total) * live).astype(jnp.bfloat16)

    def finish_dm(start, size, total):
        own = span(start, size)
        hidden = h_ref[own]
        inverse = lax.rsqrt(jnp.mean(hidden * hidden, axis=-1, keepdims=True) + epsilon)
        scaled = total * gain2_ref[...]
        inner = jnp.mean(scaled * hidden, axis=-1, keepdims=True)
        grad = (
            cot_ref[own].astype(jnp.float32)
            + inverse * scaled
            - hidden * (inverse * inverse * inverse) * inner
        )
        dh_buf[own] = grad
        ga_buf[span(index * dh_buf.shape[0] + start, size)] = grad.astype(jnp.bfloat16)
        gains_ref[pl.ds(1, 1)] += jnp.sum(total * hidden * inverse, axis=0, keepdims=True)

    def finish_da(start, size, total):
        own = span(start, size)
        values = cot_ref[own].astype(jnp.float32)
        inverse = lax.rsqrt(jnp.mean(values * values, axis=-1, keepdims=True) + epsilon)
        scaled = total * gain1_ref[...]
        inner = jnp.mean(scaled * values, axis=-1, keepdims=True)
        grad = dh_buf[own] + inverse * scaled - values * (inverse * inverse * inverse) * inner
        result[own] = grad.astype(jnp.bfloat16)
        gains_ref[pl.ds(0, 1)] += jnp.sum(total * values * inverse, axis=0, keepdims=True)

    out_copy = pltpu.make_async_copy(result, out_ref, out_sem.at[0])
    token_copy = pltpu.make_async_copy(result, token_ref, out_sem.at[1])
    flying = []

    def settle():
        for copy in flying:
            copy.wait()
        flying.clear()

    def finish_grad(reduce, target):
        settle()
        columns = pl.ds(0, reduce.part.shape[1])

        def store(start, size, total):
            stage[span(start, size), columns] = total

        reduce.arrive_all(last, store)
        copy = pltpu.make_async_copy(stage.at[:, columns], target, stage_sem)
        copy.start()
        flying.append(copy)

    def grad_tile(left, right, columns, reduce, which):
        blocks = TILE // reduce.rows
        tile = flip(lax.div(dp_index, blocks), which) * TILE
        cols = pl.ds(pl.multiple_of(tile, 128), TILE)
        width = columns.stop - columns.start
        step = min(width, 512)

        def some(i, carry):
            there = pl.ds(pl.multiple_of(i * step, 128), step)
            here = pl.ds(pl.multiple_of(columns.start + i * step, 128), step)
            reduce.part[span(tile, TILE), there] = tn(left[:, cols], right[:, here]).astype(
                jnp.bfloat16
            )
            return carry

        lax.fori_loop(0, width // step, some, 0)
        kept, _ = reduce.lists[0]
        for j, kept_place in enumerate(kept):
            if (kept_place | (1 << reduce.order[0])) // blocks == which:
                reduce.start(0, j)

    slots, hidden_columns = hid_buf.shape
    query_heads = q_ref.shape[0]
    query_columns, key_columns = query_heads * HD, kv_ref.shape[0] * HD // 2
    queries_each = query_columns // key_columns
    scaling = HD ** (-0.5)
    last = len(dp_order) - 1
    reduces = {
        "dm": dm,
        "feed": feed,
        "da": da,
        "down": down,
        "gate": gate,
        "up": up,
        "mix": mix,
        "one": one,
        "two": two,
    }
    targets = {
        "down": down_ref,
        "gate": gate_ref,
        "up": up_ref,
        "mix": mix_ref,
        "one": one_ref,
        "two": two_ref,
    }
    sources = {
        "down": (wide, hid_buf, slice(0, hidden_columns)),
        "gate": (m_buf, dgate_buf, slice(0, hidden_columns)),
        "up": (m_buf, hid_buf, slice(0, hidden_columns)),
        "mix": (ga_buf, o_ref, slice(0, query_columns)),
        "one": (wide, dgate_buf, slice(0, TILE)),
        "two": (wide, dgate_buf, slice(TILE, 2 * TILE)),
    }
    before = {
        ("down", 3): (1, 2),
        ("gate", 3): (3, 4),
        ("up", 3): (5,),
        ("one", 3): (7,),
    }
    peers = TENSOR_PEERS + tuple(("dp", bit) for bit in dp_order)
    gains = []
    turned = {}

    def turned_back(values, block):
        cosine, sine = block_angles(base_ref, step_ref, block)
        return turn(values, cosine, -sine).astype(jnp.bfloat16)

    def keep(rows, values, grouped, plain):
        dgate_buf[rows, pl.ds(grouped, HD)] = values
        hid_buf[rows, pl.ds(plain, HD)] = values

    def do_start(name):
        if name == "dm":
            loads[0].wait()
            loads[8].wait()
        else:
            dm.close()
            loads[9].start()
            loads[6].start()
            loads[6].wait()
        reduces[name].start_all()

    def do_tile(name, which):
        for i in before.get((name, which), ()):
            loads[i].wait()
        left, right, columns = sources[name]
        grad_tile(left, right, columns, reduces[name], which)
        if (name, which) == ("down", 0):
            loads[5].start()
            loads[7].start()

    def do_arrive(name, step, j, c):
        reduce = reduces[name]
        if name in targets:
            if step == last:
                finish_grad(reduce, targets[name])
            else:
                reduce.arrive(step, j, c)
        elif step == 0:
            reduce.arrive(step, j, c)
        else:
            reduce.arrive(step, j, c, {"dm": finish_dm, "feed": finish_out, "da": finish_da}[name])
            if name == "dm":
                gather.start(c)
            if name == "feed" and c == SPLIT - 1:
                for mask in (1, 2):
                    pl.semaphore_signal(
                        credit,
                        inc=1,
                        device_id={"tensor": flip(index, mask)},
                        device_id_type=MESH,
                    )
                feed.close()
                out_copy.start()
            if name == "da" and c == SPLIT - 1:
                token_copy.start()

    def do_back():
        def some(i, carry):
            rows = span(i * BLOCK, BLOCK)
            grads = nn(ga_buf[rows], mixing_ref[...]).astype(jnp.bfloat16)
            for h in range(query_heads):
                m_buf[rows, lanes(h)] = grads[:, h * HD : (h + 1) * HD]
            return carry

        lax.fori_loop(0, slots // BLOCK, some, 0)

    def do_attention(group, block):
        if group not in turned:
            turned[group] = kv_ref[group].T

        def leave(h, rows, values):
            m_buf[rows, lanes(query_heads + h)] = turned_back(values, block)

        attention_back(
            q_ref,
            kv_ref,
            m_buf,
            begin_ref,
            lse_ref,
            turned[group],
            (key_sum, value_sum),
            (group * queries_each, (group + 1) * queries_each),
            group,
            block * BLOCK,
            leave,
        )

    def do_keys(group):
        grouped = group * TILE + queries_each * HD
        plain = query_columns + group * HD

        def some(i, carry):
            rows = span(i * BLOCK, BLOCK)
            for each in range(queries_each):
                h = group * queries_each + each
                keep(rows, m_buf[rows, lanes(query_heads + h)], group * TILE + each * HD, h * HD)
            keep(rows, turned_back(key_sum[rows] * scaling, i), grouped, plain)
            keep(rows, value_sum[rows].astype(jnp.bfloat16), grouped + HD, plain + key_columns)
            return carry

        lax.fori_loop(0, slots // BLOCK, some, 0)

    def do_product(place):
        if place == 3:
            loads[9].wait()
            out_copy.wait()
            pl.semaphore_wait(credit, 2)
        block = span(flip(index, place) * BLOCK, BLOCK)

        def some(i, carry):
            cols = pl.ds(pl.multiple_of(i * 512, 512), 512)
            total = nt(hid_buf[block, pl.ds(0, query_columns)], query_ref[cols])
            total += nn(hid_buf[block, pl.ds(query_columns, key_columns)], key_ref[:, cols])
            total += nn(
                hid_buf[block, pl.ds(query_columns + key_columns, key_columns)], value_ref[:, cols]
            )
            rs_part[block, cols] = total.astype(jnp.bfloat16)
            return carry

        lax.fori_loop(0, rs_part.shape[1] // 512, some, 0)
        if place in (3, 1):
            for c in range(SPLIT):
                da.start(0, (3, 1).index(place), c)

    def do_send_gains(i):
        axis, bit = peers[i]
        copy = pltpu.make_async_remote_copy(
            src_ref=gains_ref,
            dst_ref=gains_land.at[i],
            send_sem=gains_send.at[i],
            recv_sem=gains_recv.at[i],
            device_id={axis: flip(lax.axis_index(axis), 1 << bit)},
            device_id_type=MESH,
        )
        copy.start()
        gains.append(copy)

    def do_finish(c):
        gather.near(c)
        gather.finish(c)

    def do_add_gains(i):
        gains[i].wait()
        gains_ref[...] += gains_land[i]

    actions = {
        "start": do_start,
        "tile": do_tile,
        "arrive": do_arrive,
        "forward": gather.forward,
        "finish": do_finish,
        "back": do_back,
        "attention": do_attention,
        "keys": do_keys,
        "product": do_product,
        "send": do_send_gains,
        "add": do_add_gains,
    }
    for action, *rest in plan_of(count, orders, reduces):
        actions[action](*rest)
    settle()
    token_copy.wait()
    for item in (da, gather, down, gate, up, mix, one, two):
        item.close()


def back_call(
    dm_part,
    feed_part,
    second_in,
    outer_low,
    hidden,
    gate_low,
    upward_low,
    first_in,
    tokens,
    used,
    middle,
    first_gain,
    second_gain,
    mixing_weight,
    query_weight,
    key_weight,
    value_weight,
    attended,
    queries,
    pairs,
    begin,
    log_totals,
    tables,
):
    slots, width = dm_part.shape
    rows = slots // 4
    columns = hidden.shape[1]
    heads = attended.shape[1]
    count = lax.axis_size("dp")
    dp_order = bits_of(count)
    z_order = (dp_order[1], dp_order[0]) + dp_order[2:]
    block = width // count
    share = Reduce.slots(4, SPLIT)
    total = Reduce.slots(count)

    def kernel(*refs):
        back_kernel(dp_order, z_order, *refs)

    def grad(size):
        return jax.ShapeDtypeStruct((block, size), jnp.float32)

    def low(*shape):
        return pltpu.VMEM(shape, jnp.bfloat16)

    sizes = (columns, columns, columns, heads, TILE, TILE)
    hops = 2 + len(dp_order)
    return pl.pallas_call(
        kernel,
        out_shape=(
            jax.ShapeDtypeStruct((rows, width), jnp.bfloat16),
            jax.ShapeDtypeStruct((rows, width), jnp.bfloat16),
            jax.ShapeDtypeStruct((2, width), jnp.float32),
            *(grad(size) for size in sizes),
        ),
        in_specs=[pl.BlockSpec(memory_space=pl.ANY)] * 9
        + [pl.BlockSpec(memory_space=pltpu.SMEM)]
        + vmem_specs(14),
        out_specs=tuple(
            pl.BlockSpec(memory_space=pltpu.VMEM if i == 2 else pl.ANY) for i in range(9)
        ),
        scratch_shapes=[
            low(slots, width),
            low(slots, width),
            low(slots, columns),
            low(slots, columns),
            low(slots, width),
            low(share, rows // SPLIT, width),
            low(slots, width),
            pltpu.VMEM((rows, width), jnp.float32),
            pltpu.VMEM((slots, HD), jnp.float32),
            pltpu.VMEM((slots, HD), jnp.float32),
            pltpu.VMEM((hops, 2, width), jnp.float32),
            low(rows, width),
            low(rows, width),
            *(low(width, size) for size in sizes),
            *(low(total, block, size) for size in sizes),
            pltpu.VMEM((block, columns), jnp.float32),
            pltpu.SemaphoreType.DMA,
            pltpu.SemaphoreType.DMA((2,)),
            pltpu.SemaphoreType.DMA((10,)),
            pltpu.SemaphoreType.REGULAR,
            *dma_sems(share),
            *dma_sems(share),
            *dma_sems(share),
            *dma_sems(3 * SPLIT),
            *(sem for size in sizes for sem in dma_sems(total)),
            *dma_sems(hops),
        ],
        compiler_params=pltpu.CompilerParams(
            collective_id=1, has_side_effects=True, vmem_limit_bytes=67043328
        ),
        name="back",
    )(
        dm_part,
        feed_part,
        second_in,
        outer_low,
        hidden,
        gate_low,
        upward_low,
        first_in,
        tokens,
        used,
        middle,
        first_gain.reshape(1, -1),
        second_gain.reshape(1, -1),
        mixing_weight,
        query_weight,
        key_weight,
        value_weight,
        attended,
        queries,
        pairs,
        begin,
        log_totals,
        *tables,
    )


def on_device(
    tokens,
    lengths,
    owners,
    first_gain,
    query_weight,
    key_weight,
    value_weight,
    mixing_weight,
    second_gain,
    gate_weight,
    up_weight,
    down_weight,
    cotangent,
):
    tables = rope_tables(tokens.shape[0])
    key_turned, value_turned = key_weight.T, value_weight.T
    first_in, outer_low, queries, pairs, attended, log_totals, begin, used = first_call(
        tokens,
        lengths,
        owners,
        first_gain,
        query_weight,
        key_turned,
        value_turned,
        cotangent,
        tables,
    )
    middle, second_in, hidden, gate_low, upward_low, feed_part, second_part = middle_call(
        attended,
        mixing_weight,
        second_gain,
        tokens,
        outer_low,
        gate_weight,
        up_weight,
        down_weight,
    )
    layer_output, token_grad, gains, *grads = back_call(
        second_part,
        feed_part,
        second_in,
        outer_low,
        hidden,
        gate_low,
        upward_low,
        first_in,
        tokens,
        used,
        middle,
        first_gain,
        second_gain,
        mixing_weight,
        query_weight,
        key_turned,
        value_turned,
        attended,
        queries,
        pairs,
        begin,
        log_totals,
        tables,
    )
    (
        layer_output,
        token_grad,
        down_grad,
        gate_grad,
        up_grad,
        mixing_grad,
        query_grad,
        key_grad,
        value_grad,
    ) = last_call([layer_output, token_grad, *grads], query_weight.shape[1], key_weight.shape[1])
    return (
        layer_output,
        token_grad,
        gains[0],
        query_grad,
        key_grad,
        value_grad,
        mixing_grad,
        gains[1],
        gate_grad,
        up_grad,
        down_grad,
    )


def solution(mesh):
    in_specs = (
        P("dp", None),
        P(),
        P(),
        P(),
        P(None, "tensor"),
        P(None, "tensor"),
        P(None, "tensor"),
        P(None, "tensor"),
        P(),
        P(None, "tensor"),
        P(None, "tensor"),
        P(None, "tensor"),
        P("dp", None),
    )
    out_specs = (
        P(("dp", "tensor"), None),
        P(("dp", "tensor"), None),
        P(),
        P("dp", "tensor"),
        P("dp", "tensor"),
        P("dp", "tensor"),
        P("dp", "tensor"),
        P(),
        P("dp", "tensor"),
        P("dp", "tensor"),
        P("dp", "tensor"),
    )
    return jax.shard_map(
        on_device, mesh=mesh, in_specs=in_specs, out_specs=out_specs, check_vma=False
    )
```

```python
import jax
import jax.numpy as jnp
import numpy as np
from jax import lax
from jax.experimental import pallas as pl
from jax.experimental.pallas import tpu as pltpu
from jax.sharding import PartitionSpec as P

HD = 96

MESH = pl.DeviceIdType.MESH

epsilon = 1e-05
rope_base = 10000.0


def bits_of(count):
    return tuple(range(count.bit_length() - 1))


def nn(left, right):
    return jnp.dot(left, right, preferred_element_type=jnp.float32)


def nt(left, right):
    return lax.dot_general(left, right, (((1,), (1,)), ((), ())), preferred_element_type=jnp.float32)


def tn(left, right):
    return lax.dot_general(left, right, (((0,), (0,)), ((), ())), preferred_element_type=jnp.float32)


def flip(index, mask):
    result = index
    bit = 0
    while mask >> bit:
        if (mask >> bit) & 1:
            result = result + (1 << bit) * (1 - 2 * lax.rem(lax.div(index, 1 << bit), 2))
        bit += 1
    return result


def span(start, size, step=16):
    return pl.ds(pl.multiple_of(start, step), size)


def greet(peers):
    barrier = pltpu.get_barrier_semaphore()
    for axis, bit in peers:
        index = lax.axis_index(axis)
        pl.semaphore_signal(
            barrier, inc=1, device_id={axis: flip(index, 1 << bit)}, device_id_type=MESH
        )
    pl.semaphore_wait(barrier, len(peers))


def chunk_rows(rows):
    for size in (16,):
        if rows % size == 0:
            return size
    return rows


class Reduce:
    def __init__(self, part, landing, send_sems, recv_sems, axis, order, split=1):
        self.part, self.landing = part, landing
        self.send_sems, self.recv_sems = send_sems, recv_sems
        self.axis, self.order, self.split = axis, order, split
        self.index = lax.axis_index(axis)
        self.rows = part.shape[0] >> len(order)
        self.piece = self.rows // split
        self.copies = {}
        self.lists = []
        base = 0
        for step in range(len(order)):
            kept = [0]
            for bit in reversed(order[step + 1 :]):
                kept = [place | (1 << bit) for place in kept] + kept
            self.lists.append((kept, base))
            base += len(kept) * split

    @staticmethod
    def slots(count, split=1):
        return (count - 1) * split

    def units(self, step):
        kept, _ = self.lists[step]
        return [(j, c) for j in range(len(kept)) for c in range(self.split)]

    def start(self, step, j, c=0):
        kept, base = self.lists[step]
        mask = 1 << self.order[step]
        slot = base + j * self.split + c
        source = flip(self.index, kept[j] | mask) * self.rows + c * self.piece
        copy = pltpu.make_async_remote_copy(
            src_ref=self.part.at[span(source, self.piece)],
            dst_ref=self.landing.at[slot],
            send_sem=self.send_sems.at[slot],
            recv_sem=self.recv_sems.at[slot],
            device_id={self.axis: flip(self.index, mask)},
            device_id_type=MESH,
        )
        copy.start()
        self.copies[slot] = copy

    def arrive(self, step, j, c=0, store=None):
        kept, base = self.lists[step]
        slot = base + j * self.split + c
        self.copies[slot].wait_recv()
        start = flip(self.index, kept[j]) * self.rows + c * self.piece
        size = chunk_rows(self.piece)

        def add(i, carry):
            rows = span(start + i * size, size)
            other = self.landing[slot, span(i * size, size)]
            total = self.part[rows].astype(jnp.float32) + other.astype(jnp.float32)
            if store is None:
                self.part[rows] = total.astype(self.part.dtype)
            else:
                store(c * self.piece + i * size, size, total)
            return carry

        lax.fori_loop(0, self.piece // size, add, 0)
        if step + 1 < len(self.order):
            later, _ = self.lists[step + 1]
            mask = 1 << self.order[step + 1]
            if kept[j] & mask:
                self.start(step + 1, later.index(kept[j] ^ mask), c)

    def start_all(self):
        for j, c in self.units(0):
            self.start(0, j, c)

    def arrive_all(self, step, store=None):
        for j, c in self.units(step):
            self.arrive(step, j, c, store)

    def close(self):
        for copy in self.copies.values():
            copy.wait_send()


class Gather:
    def __init__(self, whole, send_sems, recv_sems, split=1):
        self.whole, self.split = whole, split
        self.send_sems, self.recv_sems = send_sems, recv_sems
        self.index = lax.axis_index("tensor")
        self.rows = whole.shape[0] // 4
        self.piece = self.rows // split
        self.copies = {}

    def send(self, kind, c):
        mask = (2, 1, 1)[kind]
        block = flip(self.index, 2) if kind == 2 else self.index
        rows = span(block * self.rows + c * self.piece, self.piece)
        slot = kind * self.split + c
        copy = pltpu.make_async_remote_copy(
            src_ref=self.whole.at[rows],
            dst_ref=self.whole.at[rows],
            send_sem=self.send_sems.at[slot],
            recv_sem=self.recv_sems.at[slot],
            device_id={"tensor": flip(self.index, mask)},
            device_id_type=MESH,
        )
        copy.start()
        self.copies[kind, c] = copy

    def start(self, c):
        self.send(0, c)
        self.send(1, c)

    def forward(self, c):
        self.copies[0, c].wait_recv()
        self.send(2, c)

    def near(self, c):
        self.copies[1, c].wait_recv()

    def finish(self, c):
        self.copies[2, c].wait_recv()

    def close(self):
        for copy in self.copies.values():
            copy.wait_send()


TENSOR_PEERS = (("tensor", 0), ("tensor", 1))
SPLIT = 4


def middle_kernel(
    o_ref,
    w_ref,
    gain_ref,
    tokens_hbm,
    gm_hbm,
    gate_hbm,
    up_hbm,
    down_hbm,
    h_ref,
    m_hbm,
    hid_hbm,
    dgate_hbm,
    dup_hbm,
    feed_hbm,
    dm_hbm,
    part,
    landing,
    m_buf,
    x_buf,
    gm_buf,
    gate_w,
    up_w,
    down_w,
    hid_buf,
    dgate_buf,
    dup_buf,
    rs_send,
    rs_recv,
    ag_send,
    ag_recv,
    load_sems,
    leave_sems,
    feed_buf,
    grad_buf,
):
    index = lax.axis_index("tensor")
    rows = o_ref.shape[0] // 4
    loads = [
        pltpu.make_async_copy(source, target, load_sems.at[i])
        for i, (source, target) in enumerate(
            (
                (tokens_hbm.at[span(index * rows, rows)], x_buf),
                (gate_hbm, gate_w),
                (up_hbm, up_w),
                (gm_hbm, gm_buf),
                (down_hbm, down_w),
            )
        )
    ]
    for load in loads:
        load.start()
    greet(TENSOR_PEERS)
    reduce = Reduce(part, landing, rs_send, rs_recv, "tensor", (0, 1), SPLIT)
    gather = Gather(m_buf, ag_send, ag_recv, SPLIT)
    leaving = []

    def leave(buffer, target, half):
        there = span(half * 2 * rows, 2 * rows)
        copy = pltpu.make_async_copy(
            buffer.at[there], target.at[there], leave_sems.at[len(leaving)]
        )
        copy.start()
        leaving.append(copy)

    def product(place):
        block = span(flip(index, place) * rows, rows)
        columns = 512

        def tile(i, carry):
            cols = pl.ds(pl.multiple_of(i * columns, columns), columns)
            part[block, cols] = nt(o_ref[block], w_ref[cols]).astype(jnp.bfloat16)
            return carry

        lax.fori_loop(0, part.shape[1] // columns, tile, 0)

    def normed(start, size, total):
        own = span(start, size)
        hidden = x_buf[own].astype(jnp.float32) + total
        h_ref[own] = hidden
        inverse = lax.rsqrt(jnp.mean(hidden * hidden, axis=-1, keepdims=True) + epsilon)
        m_buf[span(index * rows + start, size)] = (hidden * inverse * gain_ref[...]).astype(
            jnp.bfloat16
        )

    def hidden_part(half, first, last):
        there = span(half * 2 * rows, 2 * rows)
        columns = 256

        def tile(i, carry):
            cols = pl.ds(pl.multiple_of(i * columns, columns), columns)
            gate = nn(m_buf[there], gate_w[:, cols])
            upward = nn(m_buf[there], up_w[:, cols])
            grad = grad_buf[there, cols]
            sigmoid = 1.0 / (1.0 + jnp.exp(-gate))
            activated = gate * sigmoid
            hid_buf[there, cols] = (activated * upward).astype(jnp.bfloat16)
            dgate_buf[there, cols] = (
                grad * upward * sigmoid * (1.0 + gate * (1.0 - sigmoid))
            ).astype(jnp.bfloat16)
            dup_buf[there, cols] = (grad * activated).astype(jnp.bfloat16)
            return carry

        lax.fori_loop(first, last, tile, 0)

    def feed_part(half):
        there = span(half * 2 * rows, 2 * rows)

        def tile(i, carry):
            cols = pl.ds(pl.multiple_of(i * 512, 512), 512)
            feed_buf[there, cols] = nt(hid_buf[there], down_w[cols]).astype(jnp.bfloat16)
            return carry

        lax.fori_loop(0, feed_buf.shape[1] // 512, tile, 0)

    def dm_part(half):
        there = span(half * 2 * rows, 2 * rows)

        def tile(i, carry):
            cols = pl.ds(pl.multiple_of(i * 512, 512), 512)
            total = nt(dgate_buf[there], gate_w[cols]) + nt(dup_buf[there], up_w[cols])
            part[there, cols] = total.astype(jnp.bfloat16)
            return carry

        lax.fori_loop(0, part.shape[1] // 512, tile, 0)

    product(3)
    for c in range(SPLIT):
        reduce.start(0, 0, c)
    product(2)
    for c in range(SPLIT):
        reduce.arrive(0, 0, c)
    product(1)
    for c in range(SPLIT):
        reduce.start(0, 1, c)
    product(0)
    for c in range(SPLIT):
        reduce.arrive(0, 1, c)
    for i in (0, 3, 4):
        loads[i].wait()
    piece = grad_buf.shape[1] // SPLIT

    def hidden_grad(c):
        cols = pl.ds(c * piece, piece)

        def some(i, carry):
            there = span(i * 2 * rows, 2 * rows)
            grad_buf[there, cols] = nn(gm_buf[there], down_w[:, cols])
            return carry

        lax.fori_loop(0, 2, some, 0)

    for c in range(SPLIT):
        hidden_grad(c)
        reduce.arrive(1, 0, c, normed)
        gather.start(c)
    near = lax.div(index, 2)
    far = 1 - near
    for load in loads[1:3]:
        load.wait()
    for c in range(SPLIT):
        gather.near(c)
    reduce.close()
    tiles = hid_buf.shape[1] // 256
    hidden_part(near, 0, tiles // 2)
    gather.forward(0)
    hidden_part(near, tiles // 2, tiles)
    gather.forward(1)
    leave(hid_buf, hid_hbm, near)
    leave(dgate_buf, dgate_hbm, near)
    leave(dup_buf, dup_hbm, near)
    leave(m_buf, m_hbm, near)
    feed_part(near)
    leave(feed_buf, feed_hbm, near)
    gather.forward(2)
    dm_part(near)
    leave(part, dm_hbm, near)
    for c in range(3, SPLIT):
        gather.forward(c)
    for c in range(SPLIT):
        gather.finish(c)
    leave(m_buf, m_hbm, far)
    hidden_part(far, 0, tiles)
    leave(hid_buf, hid_hbm, far)
    leave(dgate_buf, dgate_hbm, far)
    leave(dup_buf, dup_hbm, far)
    feed_part(far)
    leave(feed_buf, feed_hbm, far)
    dm_part(far)
    leave(part, dm_hbm, far)
    for copy in leaving:
        copy.wait()
    gather.close()


def vmem_specs(count):
    return [pl.BlockSpec(memory_space=pltpu.VMEM)] * count


def dma_sems(count):
    return [pltpu.SemaphoreType.DMA((count,)), pltpu.SemaphoreType.DMA((count,))]


def middle_call(
    attended, mixing_weight, second_gain, tokens, outer_low, gate_weight, up_weight, down_weight
):
    slots, width = tokens.shape
    rows = slots // 4
    columns = gate_weight.shape[1]
    count = Reduce.slots(4, SPLIT)

    def low(*shape):
        return pltpu.VMEM(shape, jnp.bfloat16)

    def result(size):
        return jax.ShapeDtypeStruct((slots, size), jnp.bfloat16)

    return pl.pallas_call(
        middle_kernel,
        out_shape=(
            jax.ShapeDtypeStruct((rows, width), jnp.float32),
            result(width),
            result(columns),
            result(columns),
            result(columns),
            result(width),
            result(width),
        ),
        in_specs=vmem_specs(3) + [pl.BlockSpec(memory_space=pl.ANY)] * 5,
        out_specs=tuple(vmem_specs(1) + [pl.BlockSpec(memory_space=pl.ANY)] * 6),
        scratch_shapes=[
            low(slots, width),
            low(count, rows // SPLIT, width),
            low(slots, width),
            low(rows, width),
            low(slots, width),
            low(width, columns),
            low(width, columns),
            low(width, columns),
            low(slots, columns),
            low(slots, columns),
            low(slots, columns),
            *dma_sems(count),
            *dma_sems(3 * SPLIT),
            pltpu.SemaphoreType.DMA((5,)),
            pltpu.SemaphoreType.DMA((12,)),
            low(slots, width),
            pltpu.VMEM((slots, columns), jnp.float32),
        ],
        compiler_params=pltpu.CompilerParams(
            collective_id=0, has_side_effects=True, vmem_limit_bytes=67043328
        ),
        name="middle",
    )(
        attended,
        mixing_weight,
        second_gain,
        tokens,
        outer_low,
        gate_weight,
        up_weight,
        down_weight,
    )


BLOCK = 256
TILE = 384
LOG2_E = float(np.log2(np.e))


def head(index):
    return pl.ds(index * HD, HD)


def allowed_keys(begin_row, query_start, key_count, query_count):
    keys = lax.broadcasted_iota(jnp.int32, (key_count, query_count), 0)
    queries = query_start + lax.broadcasted_iota(jnp.int32, (key_count, query_count), 1)
    return (keys >= begin_row) & (keys <= queries)


def rope_tables(slots):
    half = HD // 2
    frequency = rope_base ** (-2.0 * np.arange(half) / HD)

    def table(places):
        angles = places[:, None] * frequency[None, :]
        return np.concatenate([np.cos(angles), np.sin(angles)], axis=1).astype(np.float32)

    return (
        jnp.asarray(table(np.arange(BLOCK))),
        jnp.asarray(table(np.arange(max(8, slots // BLOCK)) * BLOCK)),
    )


def block_angles(base_ref, step_ref, block):
    half = HD // 2
    low_cos, low_sin = base_ref[:, pl.ds(0, half)], base_ref[:, pl.ds(half, half)]
    high = step_ref[pl.ds(block, 1)]
    high_cos, high_sin = high[:, :half], high[:, half:]
    return (low_cos * high_cos - low_sin * high_sin, low_sin * high_cos + low_cos * high_sin)


def turn(values, cosine, sine):
    half = HD // 2
    first, second = values[:, :half], values[:, half:]
    return jnp.concatenate([first * cosine - second * sine, second * cosine + first * sine], axis=1)


def first_kernel(
    blocks,
    lengths_ref,
    owners_ref,
    x_ref,
    cot_ref,
    gain_ref,
    next_gain_ref,
    wq_ref,
    wk_ref,
    wv_ref,
    base_ref,
    step_ref,
    a_ref,
    gm_ref,
    q_ref,
    kv_ref,
    o_ref,
    lse_ref,
    begin_ref,
    used_ref,
    gain_row,
    next_row,
    kept,
    turned,
    o_heads,
):
    block = pl.program_id(0)
    index = lax.axis_index("dp")
    slots = block * BLOCK + lax.broadcasted_iota(jnp.int32, (1, BLOCK), 1)

    def sequence(s, carry):
        total, begin = carry
        length = jnp.where(owners_ref[s] == index, lengths_ref[s], 0)
        begin = jnp.where((slots >= total) & (slots < total + length), total, begin)
        return total + length, begin

    used, begin = lax.fori_loop(0, lengths_ref.shape[0], sequence, (jnp.int32(0), slots))
    gain_row[...] = gain_ref[...].reshape(1, -1)
    next_row[...] = next_gain_ref[...].reshape(1, -1)
    begin_ref[...] = begin
    used_ref[0] = used
    size = 64

    def rows_in(i, carry):
        rows = span(i * size, size)
        values = x_ref[rows].astype(jnp.float32)
        inverse = lax.rsqrt(jnp.mean(values * values, axis=-1, keepdims=True) + epsilon)
        a_ref[rows] = (values * inverse * gain_row[...]).astype(jnp.bfloat16)
        places = block * BLOCK + i * size + lax.broadcasted_iota(jnp.int32, (size, 1), 0)
        live = (places < used).astype(jnp.float32)
        gm_ref[rows] = (cot_ref[rows].astype(jnp.float32) * live).astype(jnp.bfloat16)
        return carry

    lax.fori_loop(0, BLOCK // size, rows_in, 0)
    cosine, sine = block_angles(base_ref, step_ref, block)
    normed = a_ref[...]
    queries = nn(normed, wq_ref[...])
    query_heads, key_heads = queries.shape[1] // HD, wk_ref.shape[0] // HD
    for h in range(query_heads):
        piece = queries[:, h * HD : (h + 1) * HD]
        q_ref[h] = turn(piece, cosine, sine).astype(jnp.bfloat16)
    keys = nt(normed, wk_ref[...])
    here = span(block * BLOCK, BLOCK)
    for h in range(key_heads):
        piece = turn(keys[:, h * HD : (h + 1) * HD], cosine, sine).astype(jnp.bfloat16)
        kv_ref[h] = piece
        kept[h, here] = piece
    values = nt(normed, wv_ref[...]).astype(jnp.bfloat16)
    for h in range(key_heads):
        kv_ref[key_heads + h] = values[:, h * HD : (h + 1) * HD]
    scaling = HD ** (-0.5)
    groups = query_heads // key_heads

    def attend(now):
        stop = (now + 1) * BLOCK
        for h in range(key_heads):
            turned[h, :, pl.ds(now * BLOCK, BLOCK)] = kv_ref[key_heads + h].T
        allowed = allowed_keys(begin, now * BLOCK, stop, BLOCK)

        def one_head(h, carry):
            group = lax.div(h, groups)
            scores = nt(kept[group, pl.ds(0, stop)], q_ref[h])
            scores = jnp.where(allowed, scores, -jnp.inf)
            highest = jnp.max(scores, axis=0, keepdims=True)
            exponent = jnp.exp2((scores - highest) * (scaling * LOG2_E))
            total = jnp.sum(exponent, axis=0, keepdims=True)
            weights = exponent.astype(jnp.bfloat16)
            mixed = nn(turned[group, :, pl.ds(0, stop)], weights) * (1.0 / total)
            highest = highest * scaling
            o_heads[h] = mixed.T.astype(jnp.bfloat16)
            lse_ref[pl.ds(h, 1)] = highest + jnp.log(total)
            return carry

        lax.fori_loop(0, query_heads, one_head, 0)

    for now in range(blocks):
        pl.when(block == now)(lambda now=now: attend(now))
    for h in range(query_heads):
        o_ref[:, head(h)] = o_heads[h]


def first_call(
    tokens,
    lengths,
    owners,
    first_gain,
    second_gain,
    query_weight,
    key_weight,
    value_weight,
    cotangent,
    tables,
):
    slots, width = tokens.shape
    blocks = slots // BLOCK
    columns, pairs = query_weight.shape[1], 2 * key_weight.shape[0] // HD
    heads = columns // HD

    def kernel(*refs):
        first_kernel(blocks, *refs)

    def rows_of(size):
        return pl.BlockSpec((BLOCK, size), lambda i: (i, 0))

    def whole(array):
        return pl.BlockSpec(array.shape, lambda i: (0, 0), pipeline_mode=pl.Buffered(1))

    whole_gain = pl.BlockSpec((width,), lambda i: (0,), pipeline_mode=pl.Buffered(1))
    row = jax.ShapeDtypeStruct((1, width), jnp.float32)
    scalars = pl.BlockSpec(memory_space=pltpu.SMEM)
    return pl.pallas_call(
        kernel,
        grid=(blocks,),
        out_shape=(
            jax.ShapeDtypeStruct((slots, width), jnp.bfloat16),
            jax.ShapeDtypeStruct((slots, width), jnp.bfloat16),
            jax.ShapeDtypeStruct((heads, slots, HD), jnp.bfloat16),
            jax.ShapeDtypeStruct((pairs, slots, HD), jnp.bfloat16),
            jax.ShapeDtypeStruct((slots, columns), jnp.bfloat16),
            jax.ShapeDtypeStruct((heads, slots), jnp.float32),
            jax.ShapeDtypeStruct((1, slots), jnp.int32),
            jax.ShapeDtypeStruct((1,), jnp.int32),
            row,
            row,
        ),
        in_specs=[
            scalars,
            scalars,
            rows_of(width),
            rows_of(width),
            whole_gain,
            whole_gain,
            whole(query_weight),
            whole(key_weight),
            whole(value_weight),
            whole(tables[0]),
            whole(tables[1]),
        ],
        out_specs=(
            rows_of(width),
            rows_of(width),
            pl.BlockSpec((heads, BLOCK, HD), lambda i: (0, i, 0)),
            pl.BlockSpec((pairs, BLOCK, HD), lambda i: (0, i, 0)),
            rows_of(columns),
            pl.BlockSpec((heads, BLOCK), lambda i: (0, i)),
            pl.BlockSpec((1, BLOCK), lambda i: (0, i)),
            scalars,
            pl.BlockSpec((1, width), lambda i: (0, 0)),
            pl.BlockSpec((1, width), lambda i: (0, 0)),
        ),
        scratch_shapes=[
            pltpu.VMEM((pairs // 2, slots, HD), jnp.bfloat16),
            pltpu.VMEM((pairs // 2, HD, slots), jnp.bfloat16),
            pltpu.VMEM((heads, BLOCK, HD), jnp.bfloat16),
        ],
        compiler_params=pltpu.CompilerParams(vmem_limit_bytes=67043328),
        name="first",
    )(
        lengths,
        owners,
        tokens,
        cotangent,
        first_gain,
        second_gain,
        query_weight,
        key_weight,
        value_weight,
        *tables,
    )


def last_kernel(group_columns, *refs):
    sources, gains, targets, buffers = refs[:8], refs[8], refs[9:18], refs[20:31]
    in_sems, out_sems = refs[31:]
    for i, target in enumerate(refs[18:20]):
        target[...] = gains[i]
    out, token, down, gate, up, mix, one, two = buffers[:8]
    turned = buffers[8:]
    coming = [
        pltpu.make_async_copy(source, buffer, in_sems.at[i])
        for i, (source, buffer) in enumerate(zip(sources, buffers[:8]))
    ]
    for copy in coming:
        copy.start()
    leaving = []

    def leave(buffer):
        i = len(leaving)
        copy = pltpu.make_async_copy(buffer, targets[i], out_sems.at[i])
        copy.start()
        leaving.append(copy)

    for i in (0, 1, 2, 3, 4, 5):
        coming[i].wait()
        leave(buffers[i])
    start = 0
    coming[6].wait()
    coming[7].wait()
    for buffer in turned:
        each = buffer.shape[1] // 2
        buffer[:, pl.ds(0, each)] = one[:, pl.ds(start, each)]
        buffer[:, pl.ds(each, each)] = two[:, pl.ds(start, each)]
        start += each
        leave(buffer)
    for copy in leaving:
        copy.wait()


def last_call(arrays, gains, query_columns, key_columns):
    rows = arrays[6].shape[0]
    shapes = [jax.ShapeDtypeStruct(array.shape, array.dtype) for array in arrays[:6]]
    shapes += [
        jax.ShapeDtypeStruct((rows, size), jnp.float32)
        for size in (query_columns, key_columns, key_columns)
    ]

    def kernel(*refs):
        last_kernel(TILE, *refs)

    buffers = [pltpu.VMEM(array.shape, array.dtype) for array in arrays]
    buffers += [pltpu.VMEM(shape.shape, shape.dtype) for shape in shapes[6:]]
    return pl.pallas_call(
        kernel,
        out_shape=(*shapes, *([jax.ShapeDtypeStruct(gains.shape[1:], gains.dtype)] * 2)),
        in_specs=[pl.BlockSpec(memory_space=pl.ANY)] * 8 + vmem_specs(1),
        out_specs=(*([pl.BlockSpec(memory_space=pl.ANY)] * 9), *vmem_specs(2)),
        scratch_shapes=[
            *buffers,
            pltpu.SemaphoreType.DMA((8,)),
            pltpu.SemaphoreType.DMA((9,)),
        ],
        compiler_params=pltpu.CompilerParams(vmem_limit_bytes=67043328),
        name="last",
    )(*arrays, gains)


def lanes(index):
    return pl.ds(pl.multiple_of(index * 128, 128), HD)


def attention_back(q_ref, kv_ref, grads, begin_ref, lse_ref, turned, sums, heads, group, start, leave):
    scaling = HD ** (-0.5)
    key_sum, value_sum = sums
    key_heads = kv_ref.shape[0] // 2
    stop = start + BLOCK
    rows = pl.ds(start, BLOCK)
    seen = pl.ds(0, stop)
    if stop == q_ref.shape[1]:
        key_sum[...] = jnp.zeros_like(key_sum)
        value_sum[...] = jnp.zeros_like(value_sum)
    allowed = allowed_keys(begin_ref[:, rows], start, stop, BLOCK)

    def one_head(h, carry):
        query = q_ref[h, rows]
        grad = grads[rows, lanes(h)]
        scores = nt(kv_ref[group, seen], query) * scaling
        weights = jnp.where(allowed, jnp.exp(scores - lse_ref[pl.ds(h, 1), rows]), 0.0)
        weights_grad = nt(kv_ref[key_heads + group, seen], grad)
        inner = jnp.sum(weights * weights_grad, axis=0, keepdims=True)
        scores_grad = (weights * (weights_grad - inner)).astype(jnp.bfloat16)
        value_sum[seen] += nn(weights.astype(jnp.bfloat16), grad)
        key_sum[seen] += nn(scores_grad, query)
        leave(h, rows, nn(turned[:, :stop], scores_grad).T * scaling)
        return carry

    lax.fori_loop(heads[0], heads[1], one_head, 0)


P_START = "start"
P_TILE = "tile"
P_ARRIVE = "arrive"
P_FORWARD = "forward"
P_FINISH = "finish"
P_BACK = "back"
P_ATTENTION = "attention"
P_KEYS = "keys"
P_PRODUCT = "product"
P_SEND = "send"
P_ADD = "add"
P_DM = "dm"
P_FEED = "feed"
P_DA = "da"
P_DOWN = "down"
P_GATE = "gate"
P_UP = "up"
P_MIX = "mix"
P_ONE = "one"
P_TWO = "two"

PLAN = (
    (P_TILE, P_GATE, 3),
    (P_TILE, P_DOWN, 3),
    (P_START, P_DM),
    (P_TILE, P_GATE, 1),
    (P_ARRIVE, P_DM, 0, 0, 2),
    (P_ARRIVE, P_DM, 0, 1, 1),
    (P_ARRIVE, P_DM, 0, 1, 0),
    (P_ARRIVE, P_DM, 0, 0, 0),
    (P_TILE, P_DOWN, 1),
    (P_TILE, P_GATE, 2),
    (P_ARRIVE, P_DM, 0, 0, 1),
    (P_TILE, P_DOWN, 2),
    (P_ARRIVE, P_DM, 0, 1, 3),
    (P_ARRIVE, P_DM, 1, 0, 1),
    (P_ARRIVE, P_DM, 0, 1, 2),
    (P_ARRIVE, P_DM, 0, 0, 3),
    (P_ARRIVE, P_GATE, 0, 0, 0),
    (P_TILE, P_GATE, 0),
    (P_ARRIVE, P_GATE, 0, 1, 0),
    (P_FORWARD, 1),
    (P_TILE, P_DOWN, 0),
    (P_ARRIVE, P_DOWN, 0, 2, 0),
    (P_ARRIVE, P_GATE, 0, 2, 0),
    (P_ARRIVE, P_DOWN, 0, 0, 0),
    (P_ARRIVE, P_DM, 1, 0, 2),
    (P_TILE, P_UP, 3),
    (P_ARRIVE, P_DM, 1, 0, 0),
    (P_TILE, P_UP, 1),
    (P_FINISH, 1),
    (P_TILE, P_UP, 2),
    (P_ARRIVE, P_DM, 1, 0, 3),
    (P_FORWARD, 0),
    (P_TILE, P_UP, 0),
    (P_ARRIVE, P_DOWN, 0, 1, 0),
    (P_FORWARD, 2),
    (P_ARRIVE, P_GATE, 0, 3, 0),
    (P_FINISH, 0),
    (P_FORWARD, 3),
    (P_FINISH, 3),
    (P_ARRIVE, P_DOWN, 1, 0, 0),
    (P_FINISH, 2),
    (P_START, P_FEED),
    (P_ARRIVE, P_FEED, 0, 0, 0),
    (P_TILE, P_MIX, 3),
    (P_ARRIVE, P_FEED, 0, 0, 1),
    (P_ARRIVE, P_FEED, 0, 0, 2),
    (P_TILE, P_MIX, 1),
    (P_TILE, P_MIX, 2),
    (P_TILE, P_MIX, 0),
    (P_ARRIVE, P_FEED, 0, 1, 1),
    (P_ARRIVE, P_FEED, 0, 0, 3),
    (P_ARRIVE, P_UP, 0, 0, 0),
    (P_ARRIVE, P_GATE, 1, 0, 0),
    (P_BACK,),
    (P_ARRIVE, P_FEED, 1, 0, 1),
    (P_ATTENTION, 0, 3),
    (P_ARRIVE, P_UP, 0, 1, 0),
    (P_ARRIVE, P_FEED, 0, 1, 0),
    (P_ARRIVE, P_DOWN, 0, 3, 0),
    (P_ATTENTION, 0, 2),
    (P_ATTENTION, 0, 1),
    (P_ATTENTION, 0, 0),
    (P_KEYS, 0),
    (P_ARRIVE, P_FEED, 1, 0, 0),
    (P_TILE, P_ONE, 3),
    (P_TILE, P_ONE, 1),
    (P_ARRIVE, P_GATE, 1, 1, 0),
    (P_TILE, P_ONE, 2),
    (P_TILE, P_ONE, 0),
    (P_ARRIVE, P_FEED, 0, 1, 2),
    (P_ARRIVE, P_FEED, 1, 0, 2),
    (P_ATTENTION, 1, 3),
    (P_ATTENTION, 1, 2),
    (P_ARRIVE, P_FEED, 0, 1, 3),
    (P_ARRIVE, P_UP, 0, 2, 0),
    (P_ARRIVE, P_FEED, 1, 0, 3),
    (P_ATTENTION, 1, 1),
    (P_ATTENTION, 1, 0),
    (P_ARRIVE, P_MIX, 0, 0, 0),
    (P_ARRIVE, P_UP, 1, 0, 0),
    (P_ARRIVE, P_GATE, 2, 0, 0),
    (P_KEYS, 1),
    (P_ARRIVE, P_DOWN, 1, 1, 0),
    (P_ARRIVE, P_DOWN, 2, 0, 0),
    (P_TILE, P_TWO, 3),
    (P_TILE, P_TWO, 1),
    (P_TILE, P_TWO, 2),
    (P_TILE, P_TWO, 0),
    (P_PRODUCT, 3),
    (P_PRODUCT, 1),
    (P_PRODUCT, 2),
    (P_ARRIVE, P_DA, 0, 0, 1),
    (P_PRODUCT, 0),
    (P_ARRIVE, P_DA, 0, 1, 1),
    (P_ARRIVE, P_DA, 0, 0, 0),
    (P_ARRIVE, P_MIX, 0, 1, 0),
    (P_ARRIVE, P_DA, 0, 0, 3),
    (P_ARRIVE, P_UP, 0, 3, 0),
    (P_ARRIVE, P_DA, 0, 1, 0),
    (P_ARRIVE, P_ONE, 0, 0, 0),
    (P_ARRIVE, P_DA, 0, 1, 2),
    (P_ARRIVE, P_MIX, 0, 2, 0),
    (P_ARRIVE, P_DA, 1, 0, 0),
    (P_ARRIVE, P_MIX, 0, 3, 0),
    (P_ARRIVE, P_MIX, 1, 0, 0),
    (P_ARRIVE, P_DA, 0, 0, 2),
    (P_ARRIVE, P_DA, 1, 0, 1),
    (P_ARRIVE, P_ONE, 0, 1, 0),
    (P_ARRIVE, P_ONE, 0, 2, 0),
    (P_ARRIVE, P_TWO, 0, 0, 0),
    (P_ARRIVE, P_MIX, 1, 1, 0),
    (P_ARRIVE, P_TWO, 0, 1, 0),
    (P_ARRIVE, P_DA, 1, 0, 2),
    (P_ARRIVE, P_UP, 1, 1, 0),
    (P_ARRIVE, P_DA, 0, 1, 3),
    (P_ARRIVE, P_DA, 1, 0, 3),
    (P_SEND, 0),
    (P_ARRIVE, P_TWO, 0, 2, 0),
    (P_ADD, 0),
    (P_ARRIVE, P_ONE, 1, 0, 0),
    (P_ARRIVE, P_UP, 2, 0, 0),
    (P_SEND, 1),
    (P_ADD, 1),
    (P_SEND, 2),
    (P_ADD, 2),
    (P_SEND, 3),
    (P_ARRIVE, P_TWO, 1, 0, 0),
    (P_ADD, 3),
    (P_ARRIVE, P_ONE, 0, 3, 0),
    (P_ARRIVE, P_MIX, 2, 0, 0),
    (P_ARRIVE, P_TWO, 0, 3, 0),
    (P_ARRIVE, P_TWO, 1, 1, 0),
    (P_ARRIVE, P_ONE, 1, 1, 0),
    (P_ARRIVE, P_ONE, 2, 0, 0),
    (P_SEND, 4),
    (P_ARRIVE, P_TWO, 2, 0, 0),
    (P_ADD, 4),
)


def plan_of(count, orders, reduces):
    if count == 8:
        return PLAN
    tiles = (3, 1, 2, 0)

    def units(name, step):
        return [(P_ARRIVE, name, step, j, c) for j, c in reduces[name].units(step)]

    plan = [(P_START, P_DM)]
    plan += [(P_TILE, name, which) for name in (P_DOWN, P_GATE, P_UP) for which in tiles]
    plan += units(P_DM, 0) + units(P_DM, 1)
    plan += [(P_FORWARD, c) for c in range(SPLIT)] + [(P_FINISH, c) for c in range(SPLIT)]
    plan += [(P_START, P_FEED)] + [(P_TILE, P_MIX, which) for which in tiles] + [(P_BACK,)]
    for group in range(2):
        plan += [(P_ATTENTION, group, block) for block in (3, 2, 1, 0)]
        plan += [(P_KEYS, group)]
        plan += [(P_TILE, (P_ONE, P_TWO)[group], which) for which in tiles]
    plan += units(P_FEED, 0) + units(P_FEED, 1)
    plan += [(P_PRODUCT, place) for place in (3, 1, 2, 0)] + units(P_DA, 0) + units(P_DA, 1)
    names = (P_DOWN, P_GATE, P_UP, P_MIX, P_ONE, P_TWO)
    for step in range(len(orders[0])):
        for name in names:
            plan += units(name, step)
    for i in range(2 + len(orders[0])):
        plan += [(P_SEND, i), (P_ADD, i)]
    return plan


def back_kernel(
    dp_order,
    z_order,
    dm_hbm,
    feed_hbm,
    m_hbm,
    gm_hbm,
    hid_hbm,
    dgate_hbm,
    dup_hbm,
    a_hbm,
    tokens_hbm,
    used_ref,
    h_ref,
    gain1_ref,
    gain2_ref,
    mixing_ref,
    query_ref,
    key_ref,
    value_ref,
    o_ref,
    q_ref,
    kv_ref,
    begin_ref,
    lse_ref,
    base_ref,
    step_ref,
    out_ref,
    token_ref,
    gains_ref,
    down_ref,
    gate_ref,
    up_ref,
    mix_ref,
    one_ref,
    two_ref,
    *scratch,
):
    (
        wide,
        m_buf,
        hid_buf,
        dgate_buf,
        rs_part,
        rs_land,
        ga_buf,
        dh_buf,
        key_sum,
        value_sum,
        gains_land,
        cot_ref,
        result,
        *scratch,
    ) = scratch
    parts, lands, sems = scratch[:6], scratch[6:12], scratch[12:]
    stage, stage_sem, out_sem, load_sems, credit, *sems = sems
    index = lax.axis_index("tensor")
    dp_index = lax.axis_index("dp")
    count = 1 << len(dp_order)

    own_rows = span(index * h_ref.shape[0], h_ref.shape[0])
    loads = [
        pltpu.make_async_copy(source, target, load_sems.at[i])
        for i, (source, target) in enumerate(
            (
                (dm_hbm, rs_part),
                (gm_hbm, wide),
                (hid_hbm, hid_buf),
                (m_hbm, m_buf),
                (dgate_hbm, dgate_buf),
                (dup_hbm, hid_buf),
                (feed_hbm, rs_part),
                (a_hbm, wide),
                (gm_hbm.at[own_rows], cot_ref),
                (tokens_hbm.at[own_rows], cot_ref),
            )
        )
    ]
    for i in (3, 4, 1, 2, 0, 8):
        loads[i].start()
    greet(TENSOR_PEERS + tuple(("dp", bit) for bit in dp_order))

    def share_reduce(first_sem):
        return Reduce(rs_part, rs_land, sems[first_sem], sems[first_sem + 1], "tensor", (0, 1), SPLIT)

    dm, feed, da = share_reduce(0), share_reduce(2), share_reduce(4)
    gather = Gather(ga_buf, sems[6], sems[7], SPLIT)
    orders = (z_order, dp_order, dp_order, dp_order, dp_order, dp_order)
    down, gate, up, mix, one, two = (
        Reduce(parts[i], lands[i], sems[8 + 2 * i], sems[9 + 2 * i], "dp", orders[i])
        for i in range(6)
    )
    gains_send, gains_recv = sems[20], sems[21]
    gains_ref[...] = jnp.zeros_like(gains_ref)

    def finish_out(start, size, total):
        own = span(start, size)
        places = index * h_ref.shape[0] + start + lax.broadcasted_iota(jnp.int32, (size, 1), 0)
        live = (places < used_ref[0]).astype(jnp.float32)
        result[own] = ((h_ref[own] + total) * live).astype(jnp.bfloat16)

    def finish_dm(start, size, total):
        own = span(start, size)
        hidden = h_ref[own]
        inverse = lax.rsqrt(jnp.mean(hidden * hidden, axis=-1, keepdims=True) + epsilon)
        scaled = total * gain2_ref[...]
        inner = jnp.mean(scaled * hidden, axis=-1, keepdims=True)
        grad = (
            cot_ref[own].astype(jnp.float32)
            + inverse * scaled
            - hidden * (inverse * inverse * inverse) * inner
        )
        dh_buf[own] = grad
        ga_buf[span(index * dh_buf.shape[0] + start, size)] = grad.astype(jnp.bfloat16)
        gains_ref[pl.ds(1, 1)] += jnp.sum(total * hidden * inverse, axis=0, keepdims=True)

    def finish_da(start, size, total):
        own = span(start, size)
        values = cot_ref[own].astype(jnp.float32)
        inverse = lax.rsqrt(jnp.mean(values * values, axis=-1, keepdims=True) + epsilon)
        scaled = total * gain1_ref[...]
        inner = jnp.mean(scaled * values, axis=-1, keepdims=True)
        grad = dh_buf[own] + inverse * scaled - values * (inverse * inverse * inverse) * inner
        result[own] = grad.astype(jnp.bfloat16)
        gains_ref[pl.ds(0, 1)] += jnp.sum(total * values * inverse, axis=0, keepdims=True)

    out_copy = pltpu.make_async_copy(result, out_ref, out_sem.at[0])
    token_copy = pltpu.make_async_copy(result, token_ref, out_sem.at[1])
    flying = []

    def settle():
        for copy in flying:
            copy.wait()
        flying.clear()

    def finish_grad(reduce, target):
        settle()
        columns = pl.ds(0, reduce.part.shape[1])

        def store(start, size, total):
            stage[span(start, size), columns] = total

        reduce.arrive_all(last, store)
        copy = pltpu.make_async_copy(stage.at[:, columns], target, stage_sem)
        copy.start()
        flying.append(copy)

    def grad_tile(left, right, columns, reduce, which):
        blocks = TILE // reduce.rows
        tile = flip(lax.div(dp_index, blocks), which) * TILE
        cols = pl.ds(pl.multiple_of(tile, 128), TILE)
        width = columns.stop - columns.start
        step = min(width, 512)

        def some(i, carry):
            there = pl.ds(pl.multiple_of(i * step, 128), step)
            here = pl.ds(pl.multiple_of(columns.start + i * step, 128), step)
            reduce.part[span(tile, TILE), there] = tn(left[:, cols], right[:, here]).astype(
                jnp.bfloat16
            )
            return carry

        lax.fori_loop(0, width // step, some, 0)
        kept, _ = reduce.lists[0]
        for j, kept_place in enumerate(kept):
            if (kept_place | (1 << reduce.order[0])) // blocks == which:
                reduce.start(0, j)

    slots, hidden_columns = hid_buf.shape
    query_heads = q_ref.shape[0]
    query_columns, key_columns = query_heads * HD, kv_ref.shape[0] * HD // 2
    queries_each = query_columns // key_columns
    scaling = HD ** (-0.5)
    last = len(dp_order) - 1
    reduces = {
        "dm": dm,
        "feed": feed,
        "da": da,
        "down": down,
        "gate": gate,
        "up": up,
        "mix": mix,
        "one": one,
        "two": two,
    }
    targets = {
        "down": down_ref,
        "gate": gate_ref,
        "up": up_ref,
        "mix": mix_ref,
        "one": one_ref,
        "two": two_ref,
    }
    sources = {
        "down": (wide, hid_buf, slice(0, hidden_columns)),
        "gate": (m_buf, dgate_buf, slice(0, hidden_columns)),
        "up": (m_buf, hid_buf, slice(0, hidden_columns)),
        "mix": (ga_buf, o_ref, slice(0, query_columns)),
        "one": (wide, dgate_buf, slice(0, TILE)),
        "two": (wide, dgate_buf, slice(TILE, 2 * TILE)),
    }
    before = {
        ("down", 3): (1, 2),
        ("gate", 3): (3, 4),
        ("up", 3): (5,),
        ("one", 3): (7,),
    }
    peers = TENSOR_PEERS + tuple(("dp", bit) for bit in dp_order)
    gains = []
    turned = {}

    def turned_back(values, block):
        cosine, sine = block_angles(base_ref, step_ref, block)
        return turn(values, cosine, -sine).astype(jnp.bfloat16)

    def keep(rows, values, grouped, plain):
        dgate_buf[rows, pl.ds(grouped, HD)] = values
        hid_buf[rows, pl.ds(plain, HD)] = values

    def do_start(name):
        if name == "dm":
            loads[0].wait()
            loads[8].wait()
        else:
            dm.close()
            loads[9].start()
            loads[6].start()
            loads[6].wait()
        reduces[name].start_all()

    def do_tile(name, which):
        for i in before.get((name, which), ()):
            loads[i].wait()
        left, right, columns = sources[name]
        grad_tile(left, right, columns, reduces[name], which)
        if (name, which) == ("down", 0):
            loads[5].start()
            loads[7].start()

    def do_arrive(name, step, j, c):
        reduce = reduces[name]
        if name in targets:
            if step == last:
                finish_grad(reduce, targets[name])
            else:
                reduce.arrive(step, j, c)
        elif step == 0:
            reduce.arrive(step, j, c)
        else:
            reduce.arrive(step, j, c, {"dm": finish_dm, "feed": finish_out, "da": finish_da}[name])
            if name == "dm":
                gather.start(c)
            if name == "feed" and c == SPLIT - 1:
                for mask in (1, 2):
                    pl.semaphore_signal(
                        credit,
                        inc=1,
                        device_id={"tensor": flip(index, mask)},
                        device_id_type=MESH,
                    )
                feed.close()
                out_copy.start()
            if name == "da" and c == SPLIT - 1:
                token_copy.start()

    def do_back():
        def some(i, carry):
            rows = span(i * BLOCK, BLOCK)
            grads = nn(ga_buf[rows], mixing_ref[...]).astype(jnp.bfloat16)
            for h in range(query_heads):
                m_buf[rows, lanes(h)] = grads[:, h * HD : (h + 1) * HD]
            return carry

        lax.fori_loop(0, slots // BLOCK, some, 0)

    def do_attention(group, block):
        if group not in turned:
            turned[group] = kv_ref[group].T

        def leave(h, rows, values):
            m_buf[rows, lanes(query_heads + h)] = turned_back(values, block)

        attention_back(
            q_ref,
            kv_ref,
            m_buf,
            begin_ref,
            lse_ref,
            turned[group],
            (key_sum, value_sum),
            (group * queries_each, (group + 1) * queries_each),
            group,
            block * BLOCK,
            leave,
        )

    def do_keys(group):
        grouped = group * TILE + queries_each * HD
        plain = query_columns + group * HD

        def some(i, carry):
            rows = span(i * BLOCK, BLOCK)
            for each in range(queries_each):
                h = group * queries_each + each
                keep(rows, m_buf[rows, lanes(query_heads + h)], group * TILE + each * HD, h * HD)
            keep(rows, turned_back(key_sum[rows] * scaling, i), grouped, plain)
            keep(rows, value_sum[rows].astype(jnp.bfloat16), grouped + HD, plain + key_columns)
            return carry

        lax.fori_loop(0, slots // BLOCK, some, 0)

    def do_product(place):
        if place == 3:
            loads[9].wait()
            out_copy.wait()
            pl.semaphore_wait(credit, 2)
        block = span(flip(index, place) * BLOCK, BLOCK)

        def some(i, carry):
            cols = pl.ds(pl.multiple_of(i * 512, 512), 512)
            total = nt(hid_buf[block, pl.ds(0, query_columns)], query_ref[cols])
            total += nn(hid_buf[block, pl.ds(query_columns, key_columns)], key_ref[:, cols])
            total += nn(
                hid_buf[block, pl.ds(query_columns + key_columns, key_columns)], value_ref[:, cols]
            )
            rs_part[block, cols] = total.astype(jnp.bfloat16)
            return carry

        lax.fori_loop(0, rs_part.shape[1] // 512, some, 0)
        if place in (3, 1):
            for c in range(SPLIT):
                da.start(0, (3, 1).index(place), c)

    def do_send_gains(i):
        axis, bit = peers[i]
        copy = pltpu.make_async_remote_copy(
            src_ref=gains_ref,
            dst_ref=gains_land.at[i],
            send_sem=gains_send.at[i],
            recv_sem=gains_recv.at[i],
            device_id={axis: flip(lax.axis_index(axis), 1 << bit)},
            device_id_type=MESH,
        )
        copy.start()
        gains.append(copy)

    def do_finish(c):
        gather.near(c)
        gather.finish(c)

    def do_add_gains(i):
        gains[i].wait()
        gains_ref[...] += gains_land[i]

    actions = {
        "start": do_start,
        "tile": do_tile,
        "arrive": do_arrive,
        "forward": gather.forward,
        "finish": do_finish,
        "back": do_back,
        "attention": do_attention,
        "keys": do_keys,
        "product": do_product,
        "send": do_send_gains,
        "add": do_add_gains,
    }
    for action, *rest in plan_of(count, orders, reduces):
        actions[action](*rest)
    settle()
    token_copy.wait()
    for item in (da, gather, down, gate, up, mix, one, two):
        item.close()


def back_call(
    dm_part,
    feed_part,
    second_in,
    outer_low,
    hidden,
    gate_low,
    upward_low,
    first_in,
    tokens,
    used,
    middle,
    first_gain,
    second_gain,
    mixing_weight,
    query_weight,
    key_weight,
    value_weight,
    attended,
    queries,
    pairs,
    begin,
    log_totals,
    tables,
):
    slots, width = dm_part.shape
    rows = slots // 4
    columns = hidden.shape[1]
    heads = attended.shape[1]
    count = lax.axis_size("dp")
    dp_order = bits_of(count)
    z_order = (dp_order[1], dp_order[0]) + dp_order[2:]
    block = width // count
    share = Reduce.slots(4, SPLIT)
    total = Reduce.slots(count)

    def kernel(*refs):
        back_kernel(dp_order, z_order, *refs)

    def grad(size):
        return jax.ShapeDtypeStruct((block, size), jnp.float32)

    def low(*shape):
        return pltpu.VMEM(shape, jnp.bfloat16)

    sizes = (columns, columns, columns, heads, TILE, TILE)
    hops = 2 + len(dp_order)
    return pl.pallas_call(
        kernel,
        out_shape=(
            jax.ShapeDtypeStruct((rows, width), jnp.bfloat16),
            jax.ShapeDtypeStruct((rows, width), jnp.bfloat16),
            jax.ShapeDtypeStruct((2, width), jnp.float32),
            *(grad(size) for size in sizes),
        ),
        in_specs=[pl.BlockSpec(memory_space=pl.ANY)] * 9
        + [pl.BlockSpec(memory_space=pltpu.SMEM)]
        + vmem_specs(14),
        out_specs=tuple(
            pl.BlockSpec(memory_space=pltpu.VMEM if i == 2 else pl.ANY) for i in range(9)
        ),
        scratch_shapes=[
            low(slots, width),
            low(slots, width),
            low(slots, columns),
            low(slots, columns),
            low(slots, width),
            low(share, rows // SPLIT, width),
            low(slots, width),
            pltpu.VMEM((rows, width), jnp.float32),
            pltpu.VMEM((slots, HD), jnp.float32),
            pltpu.VMEM((slots, HD), jnp.float32),
            pltpu.VMEM((hops, 2, width), jnp.float32),
            low(rows, width),
            low(rows, width),
            *(low(width, size) for size in sizes),
            *(low(total, block, size) for size in sizes),
            pltpu.VMEM((block, columns), jnp.float32),
            pltpu.SemaphoreType.DMA,
            pltpu.SemaphoreType.DMA((2,)),
            pltpu.SemaphoreType.DMA((10,)),
            pltpu.SemaphoreType.REGULAR,
            *dma_sems(share),
            *dma_sems(share),
            *dma_sems(share),
            *dma_sems(3 * SPLIT),
            *(sem for size in sizes for sem in dma_sems(total)),
            *dma_sems(hops),
        ],
        compiler_params=pltpu.CompilerParams(
            collective_id=1, has_side_effects=True, vmem_limit_bytes=67043328
        ),
        name="back",
    )(
        dm_part,
        feed_part,
        second_in,
        outer_low,
        hidden,
        gate_low,
        upward_low,
        first_in,
        tokens,
        used,
        middle,
        first_gain,
        second_gain,
        mixing_weight,
        query_weight,
        key_weight,
        value_weight,
        attended,
        queries,
        pairs,
        begin,
        log_totals,
        *tables,
    )


def on_device(
    tokens,
    lengths,
    owners,
    first_gain,
    query_weight,
    key_weight,
    value_weight,
    mixing_weight,
    second_gain,
    gate_weight,
    up_weight,
    down_weight,
    cotangent,
):
    tables = rope_tables(tokens.shape[0])
    key_turned, value_turned = key_weight.T, value_weight.T
    (
        first_in,
        outer_low,
        queries,
        pairs,
        attended,
        log_totals,
        begin,
        used,
        first_row,
        second_row,
    ) = first_call(
        tokens,
        lengths,
        owners,
        first_gain,
        second_gain,
        query_weight,
        key_turned,
        value_turned,
        cotangent,
        tables,
    )
    middle, second_in, hidden, gate_low, upward_low, feed_part, second_part = middle_call(
        attended,
        mixing_weight,
        second_row,
        tokens,
        outer_low,
        gate_weight,
        up_weight,
        down_weight,
    )
    layer_output, token_grad, gains, *grads = back_call(
        second_part,
        feed_part,
        second_in,
        outer_low,
        hidden,
        gate_low,
        upward_low,
        first_in,
        tokens,
        used,
        middle,
        first_row,
        second_row,
        mixing_weight,
        query_weight,
        key_turned,
        value_turned,
        attended,
        queries,
        pairs,
        begin,
        log_totals,
        tables,
    )
    (
        layer_output,
        token_grad,
        down_grad,
        gate_grad,
        up_grad,
        mixing_grad,
        query_grad,
        key_grad,
        value_grad,
        first_grad,
        second_grad,
    ) = last_call(
        [layer_output, token_grad, *grads], gains, query_weight.shape[1], key_weight.shape[1]
    )
    return (
        layer_output,
        token_grad,
        first_grad,
        query_grad,
        key_grad,
        value_grad,
        mixing_grad,
        second_grad,
        gate_grad,
        up_grad,
        down_grad,
    )


def solution(mesh):
    in_specs = (
        P("dp", None),
        P(),
        P(),
        P(),
        P(None, "tensor"),
        P(None, "tensor"),
        P(None, "tensor"),
        P(None, "tensor"),
        P(),
        P(None, "tensor"),
        P(None, "tensor"),
        P(None, "tensor"),
        P("dp", None),
    )
    out_specs = (
        P(("dp", "tensor"), None),
        P(("dp", "tensor"), None),
        P(),
        P("dp", "tensor"),
        P("dp", "tensor"),
        P("dp", "tensor"),
        P("dp", "tensor"),
        P(),
        P("dp", "tensor"),
        P("dp", "tensor"),
        P("dp", "tensor"),
    )
    return jax.shard_map(
        on_device, mesh=mesh, in_specs=in_specs, out_specs=out_specs, check_vma=False
    )
```

```python
import jax
import jax.numpy as jnp
import numpy as np
from jax import lax
from jax.experimental import pallas as pl
from jax.experimental.pallas import tpu as pltpu
from jax.sharding import PartitionSpec as P

HD = 96

MESH = pl.DeviceIdType.MESH

epsilon = 1e-05
rope_base = 10000.0


def bits_of(count):
    return tuple(range(count.bit_length() - 1))


def nn(left, right):
    return jnp.dot(left, right, preferred_element_type=jnp.float32)


def nt(left, right):
    return lax.dot_general(left, right, (((1,), (1,)), ((), ())), preferred_element_type=jnp.float32)


def tn(left, right):
    return lax.dot_general(left, right, (((0,), (0,)), ((), ())), preferred_element_type=jnp.float32)


def flip(index, mask):
    result = index
    bit = 0
    while mask >> bit:
        if (mask >> bit) & 1:
            result = result + (1 << bit) * (1 - 2 * lax.rem(lax.div(index, 1 << bit), 2))
        bit += 1
    return result


def span(start, size, step=16):
    return pl.ds(pl.multiple_of(start, step), size)


def greet(peers):
    barrier = pltpu.get_barrier_semaphore()
    for axis, bit in peers:
        index = lax.axis_index(axis)
        pl.semaphore_signal(
            barrier, inc=1, device_id={axis: flip(index, 1 << bit)}, device_id_type=MESH
        )
    pl.semaphore_wait(barrier, len(peers))


def chunk_rows(rows):
    for size in (16,):
        if rows % size == 0:
            return size
    return rows


class Reduce:
    def __init__(self, part, landing, send_sems, recv_sems, axis, order, split=1):
        self.part, self.landing = part, landing
        self.send_sems, self.recv_sems = send_sems, recv_sems
        self.axis, self.order, self.split = axis, order, split
        self.index = lax.axis_index(axis)
        self.rows = part.shape[0] >> len(order)
        self.piece = self.rows // split
        self.copies = {}
        self.lists = []
        base = 0
        for step in range(len(order)):
            kept = [0]
            for bit in reversed(order[step + 1 :]):
                kept = [place | (1 << bit) for place in kept] + kept
            self.lists.append((kept, base))
            base += len(kept) * split

    @staticmethod
    def slots(count, split=1):
        return (count - 1) * split

    def units(self, step):
        kept, _ = self.lists[step]
        return [(j, c) for j in range(len(kept)) for c in range(self.split)]

    def start(self, step, j, c=0):
        kept, base = self.lists[step]
        mask = 1 << self.order[step]
        slot = base + j * self.split + c
        source = flip(self.index, kept[j] | mask) * self.rows + c * self.piece
        copy = pltpu.make_async_remote_copy(
            src_ref=self.part.at[span(source, self.piece)],
            dst_ref=self.landing.at[slot],
            send_sem=self.send_sems.at[slot],
            recv_sem=self.recv_sems.at[slot],
            device_id={self.axis: flip(self.index, mask)},
            device_id_type=MESH,
        )
        copy.start()
        self.copies[slot] = copy

    def arrive(self, step, j, c=0, store=None):
        kept, base = self.lists[step]
        slot = base + j * self.split + c
        self.copies[slot].wait_recv()
        start = flip(self.index, kept[j]) * self.rows + c * self.piece
        size = chunk_rows(self.piece)

        def add(i, carry):
            rows = span(start + i * size, size)
            other = self.landing[slot, span(i * size, size)]
            total = self.part[rows].astype(jnp.float32) + other.astype(jnp.float32)
            if store is None:
                self.part[rows] = total.astype(self.part.dtype)
            else:
                store(c * self.piece + i * size, size, total)
            return carry

        lax.fori_loop(0, self.piece // size, add, 0)
        if step + 1 < len(self.order):
            later, _ = self.lists[step + 1]
            mask = 1 << self.order[step + 1]
            if kept[j] & mask:
                self.start(step + 1, later.index(kept[j] ^ mask), c)

    def start_all(self):
        for j, c in self.units(0):
            self.start(0, j, c)

    def arrive_all(self, step, store=None):
        for j, c in self.units(step):
            self.arrive(step, j, c, store)

    def close(self):
        for copy in self.copies.values():
            copy.wait_send()


class Gather:
    def __init__(self, whole, send_sems, recv_sems, split=1):
        self.whole, self.split = whole, split
        self.send_sems, self.recv_sems = send_sems, recv_sems
        self.index = lax.axis_index("tensor")
        self.rows = whole.shape[0] // 4
        self.piece = self.rows // split
        self.copies = {}

    def send(self, kind, c):
        mask = (2, 1, 1)[kind]
        block = flip(self.index, 2) if kind == 2 else self.index
        rows = span(block * self.rows + c * self.piece, self.piece)
        slot = kind * self.split + c
        copy = pltpu.make_async_remote_copy(
            src_ref=self.whole.at[rows],
            dst_ref=self.whole.at[rows],
            send_sem=self.send_sems.at[slot],
            recv_sem=self.recv_sems.at[slot],
            device_id={"tensor": flip(self.index, mask)},
            device_id_type=MESH,
        )
        copy.start()
        self.copies[kind, c] = copy

    def start(self, c):
        self.send(0, c)
        self.send(1, c)

    def forward(self, c):
        self.copies[0, c].wait_recv()
        self.send(2, c)

    def near(self, c):
        self.copies[1, c].wait_recv()

    def finish(self, c):
        self.copies[2, c].wait_recv()

    def close(self):
        for copy in self.copies.values():
            copy.wait_send()


TENSOR_PEERS = (("tensor", 0), ("tensor", 1))
SPLIT = 4


def middle_kernel(
    o_ref,
    w_ref,
    gain_ref,
    tokens_hbm,
    gm_hbm,
    gate_hbm,
    up_hbm,
    down_hbm,
    h_ref,
    m_hbm,
    hid_hbm,
    dgate_hbm,
    dup_hbm,
    feed_hbm,
    dm_hbm,
    part,
    landing,
    m_buf,
    x_buf,
    gm_buf,
    gate_w,
    up_w,
    down_w,
    hid_buf,
    dgate_buf,
    dup_buf,
    rs_send,
    rs_recv,
    ag_send,
    ag_recv,
    load_sems,
    leave_sems,
    feed_buf,
    grad_buf,
):
    index = lax.axis_index("tensor")
    rows = o_ref.shape[0] // 4
    loads = [
        pltpu.make_async_copy(source, target, load_sems.at[i])
        for i, (source, target) in enumerate(
            (
                (tokens_hbm.at[span(index * rows, rows)], x_buf),
                (gate_hbm, gate_w),
                (up_hbm, up_w),
                (gm_hbm, gm_buf),
                (down_hbm, down_w),
            )
        )
    ]
    for load in loads:
        load.start()
    greet(TENSOR_PEERS)
    reduce = Reduce(part, landing, rs_send, rs_recv, "tensor", (0, 1), SPLIT)
    gather = Gather(m_buf, ag_send, ag_recv, SPLIT)
    leaving = []

    def leave(buffer, target, half):
        there = span(half * 2 * rows, 2 * rows)
        copy = pltpu.make_async_copy(
            buffer.at[there], target.at[there], leave_sems.at[len(leaving)]
        )
        copy.start()
        leaving.append(copy)

    def product(place):
        block = span(flip(index, place) * rows, rows)
        columns = 512

        def tile(i, carry):
            cols = pl.ds(pl.multiple_of(i * columns, columns), columns)
            part[block, cols] = nt(o_ref[block], w_ref[cols]).astype(jnp.bfloat16)
            return carry

        lax.fori_loop(0, part.shape[1] // columns, tile, 0)

    def normed(start, size, total):
        own = span(start, size)
        hidden = x_buf[own].astype(jnp.float32) + total
        h_ref[own] = hidden
        inverse = lax.rsqrt(jnp.mean(hidden * hidden, axis=-1, keepdims=True) + epsilon)
        m_buf[span(index * rows + start, size)] = (hidden * inverse * gain_ref[...]).astype(
            jnp.bfloat16
        )

    def hidden_part(half, first, last):
        there = span(half * 2 * rows, 2 * rows)
        columns = 256

        def tile(i, carry):
            cols = pl.ds(pl.multiple_of(i * columns, columns), columns)
            gate = nn(m_buf[there], gate_w[:, cols])
            upward = nn(m_buf[there], up_w[:, cols])
            grad = grad_buf[there, cols]
            sigmoid = 1.0 / (1.0 + jnp.exp(-gate))
            activated = gate * sigmoid
            hid_buf[there, cols] = (activated * upward).astype(jnp.bfloat16)
            dgate_buf[there, cols] = (
                grad * upward * sigmoid * (1.0 + gate * (1.0 - sigmoid))
            ).astype(jnp.bfloat16)
            dup_buf[there, cols] = (grad * activated).astype(jnp.bfloat16)
            return carry

        lax.fori_loop(first, last, tile, 0)

    def feed_part(half):
        there = span(half * 2 * rows, 2 * rows)

        def tile(i, carry):
            cols = pl.ds(pl.multiple_of(i * 512, 512), 512)
            feed_buf[there, cols] = nt(hid_buf[there], down_w[cols]).astype(jnp.bfloat16)
            return carry

        lax.fori_loop(0, feed_buf.shape[1] // 512, tile, 0)

    def dm_part(half):
        there = span(half * 2 * rows, 2 * rows)

        def tile(i, carry):
            cols = pl.ds(pl.multiple_of(i * 512, 512), 512)
            total = nt(dgate_buf[there], gate_w[cols]) + nt(dup_buf[there], up_w[cols])
            part[there, cols] = total.astype(jnp.bfloat16)
            return carry

        lax.fori_loop(0, part.shape[1] // 512, tile, 0)

    product(3)
    for c in range(SPLIT):
        reduce.start(0, 0, c)
    product(2)
    for c in range(SPLIT):
        reduce.arrive(0, 0, c)
    product(1)
    for c in range(SPLIT):
        reduce.start(0, 1, c)
    product(0)
    for c in range(SPLIT):
        reduce.arrive(0, 1, c)
    for i in (0, 3, 4):
        loads[i].wait()
    piece = grad_buf.shape[1] // SPLIT

    def hidden_grad(c):
        cols = pl.ds(c * piece, piece)

        def some(i, carry):
            there = span(i * 2 * rows, 2 * rows)
            grad_buf[there, cols] = nn(gm_buf[there], down_w[:, cols])
            return carry

        lax.fori_loop(0, 2, some, 0)

    for c in range(SPLIT):
        hidden_grad(c)
        reduce.arrive(1, 0, c, normed)
        gather.start(c)
    near = lax.div(index, 2)
    far = 1 - near
    for load in loads[1:3]:
        load.wait()
    for c in range(SPLIT):
        gather.near(c)
    reduce.close()
    tiles = hid_buf.shape[1] // 256
    hidden_part(near, 0, tiles // 2)
    gather.forward(0)
    hidden_part(near, tiles // 2, tiles)
    gather.forward(1)
    leave(hid_buf, hid_hbm, near)
    leave(dgate_buf, dgate_hbm, near)
    leave(dup_buf, dup_hbm, near)
    leave(m_buf, m_hbm, near)
    feed_part(near)
    leave(feed_buf, feed_hbm, near)
    gather.forward(2)
    dm_part(near)
    leave(part, dm_hbm, near)
    for c in range(3, SPLIT):
        gather.forward(c)
    for c in range(SPLIT):
        gather.finish(c)
    leave(m_buf, m_hbm, far)
    hidden_part(far, 0, tiles)
    leave(hid_buf, hid_hbm, far)
    leave(dgate_buf, dgate_hbm, far)
    leave(dup_buf, dup_hbm, far)
    feed_part(far)
    leave(feed_buf, feed_hbm, far)
    dm_part(far)
    leave(part, dm_hbm, far)
    for copy in leaving:
        copy.wait()
    gather.close()


def vmem_specs(count):
    return [pl.BlockSpec(memory_space=pltpu.VMEM)] * count


def dma_sems(count):
    return [pltpu.SemaphoreType.DMA((count,)), pltpu.SemaphoreType.DMA((count,))]


def middle_call(
    attended, mixing_weight, second_gain, tokens, outer_low, gate_weight, up_weight, down_weight
):
    slots, width = tokens.shape
    rows = slots // 4
    columns = gate_weight.shape[1]
    count = Reduce.slots(4, SPLIT)

    def low(*shape):
        return pltpu.VMEM(shape, jnp.bfloat16)

    def result(size):
        return jax.ShapeDtypeStruct((slots, size), jnp.bfloat16)

    return pl.pallas_call(
        middle_kernel,
        out_shape=(
            jax.ShapeDtypeStruct((rows, width), jnp.float32),
            result(width),
            result(columns),
            result(columns),
            result(columns),
            result(width),
            result(width),
        ),
        in_specs=vmem_specs(3) + [pl.BlockSpec(memory_space=pl.ANY)] * 5,
        out_specs=tuple(vmem_specs(1) + [pl.BlockSpec(memory_space=pl.ANY)] * 6),
        scratch_shapes=[
            low(slots, width),
            low(count, rows // SPLIT, width),
            low(slots, width),
            low(rows, width),
            low(slots, width),
            low(width, columns),
            low(width, columns),
            low(width, columns),
            low(slots, columns),
            low(slots, columns),
            low(slots, columns),
            *dma_sems(count),
            *dma_sems(3 * SPLIT),
            pltpu.SemaphoreType.DMA((5,)),
            pltpu.SemaphoreType.DMA((12,)),
            low(slots, width),
            pltpu.VMEM((slots, columns), jnp.float32),
        ],
        compiler_params=pltpu.CompilerParams(
            collective_id=0, has_side_effects=True, vmem_limit_bytes=67043328
        ),
        name="middle",
    )(
        attended,
        mixing_weight,
        second_gain,
        tokens,
        outer_low,
        gate_weight,
        up_weight,
        down_weight,
    )


BLOCK = 256
TILE = 384
LOG2_E = float(np.log2(np.e))


def head(index):
    return pl.ds(index * HD, HD)


def allowed_keys(begin_row, query_start, key_count, query_count):
    keys = lax.broadcasted_iota(jnp.int32, (key_count, query_count), 0)
    queries = query_start + lax.broadcasted_iota(jnp.int32, (key_count, query_count), 1)
    return (keys >= begin_row) & (keys <= queries)


def rope_tables(slots):
    half = HD // 2
    frequency = rope_base ** (-2.0 * np.arange(half) / HD)

    def table(places):
        angles = places[:, None] * frequency[None, :]
        return np.concatenate([np.cos(angles), np.sin(angles)], axis=1).astype(np.float32)

    return (
        jnp.asarray(table(np.arange(BLOCK))),
        jnp.asarray(table(np.arange(max(8, slots // BLOCK)) * BLOCK)),
    )


def block_angles(base_ref, step_ref, block):
    half = HD // 2
    low_cos, low_sin = base_ref[:, pl.ds(0, half)], base_ref[:, pl.ds(half, half)]
    high = step_ref[pl.ds(block, 1)]
    high_cos, high_sin = high[:, :half], high[:, half:]
    return (low_cos * high_cos - low_sin * high_sin, low_sin * high_cos + low_cos * high_sin)


def turn(values, cosine, sine):
    half = HD // 2
    first, second = values[:, :half], values[:, half:]
    return jnp.concatenate([first * cosine - second * sine, second * cosine + first * sine], axis=1)


def first_kernel(
    blocks,
    lengths_ref,
    owners_ref,
    x_ref,
    cot_ref,
    gain_ref,
    next_gain_ref,
    wq_ref,
    wk_ref,
    wv_ref,
    base_ref,
    step_ref,
    a_ref,
    gm_ref,
    q_ref,
    kv_ref,
    o_ref,
    lse_ref,
    begin_ref,
    used_ref,
    gain_row,
    next_row,
    kept,
    turned,
    o_heads,
):
    block = pl.program_id(0)
    index = lax.axis_index("dp")
    slots = block * BLOCK + lax.broadcasted_iota(jnp.int32, (1, BLOCK), 1)

    def sequence(s, carry):
        total, begin = carry
        length = jnp.where(owners_ref[s] == index, lengths_ref[s], 0)
        begin = jnp.where((slots >= total) & (slots < total + length), total, begin)
        return total + length, begin

    used, begin = lax.fori_loop(0, lengths_ref.shape[0], sequence, (jnp.int32(0), slots))
    gain_row[...] = gain_ref[...].reshape(1, -1)
    next_row[...] = next_gain_ref[...].reshape(1, -1)
    begin_ref[...] = begin
    used_ref[0] = used
    size = 64

    def rows_in(i, carry):
        rows = span(i * size, size)
        values = x_ref[rows].astype(jnp.float32)
        inverse = lax.rsqrt(jnp.mean(values * values, axis=-1, keepdims=True) + epsilon)
        a_ref[rows] = (values * inverse * gain_row[...]).astype(jnp.bfloat16)
        places = block * BLOCK + i * size + lax.broadcasted_iota(jnp.int32, (size, 1), 0)
        live = (places < used).astype(jnp.float32)
        gm_ref[rows] = (cot_ref[rows].astype(jnp.float32) * live).astype(jnp.bfloat16)
        return carry

    lax.fori_loop(0, BLOCK // size, rows_in, 0)
    cosine, sine = block_angles(base_ref, step_ref, block)
    normed = a_ref[...]
    queries = nn(normed, wq_ref[...])
    query_heads, key_heads = queries.shape[1] // HD, wk_ref.shape[0] // HD
    for h in range(query_heads):
        piece = queries[:, h * HD : (h + 1) * HD]
        q_ref[h] = turn(piece, cosine, sine).astype(jnp.bfloat16)
    keys = nt(normed, wk_ref[...])
    here = span(block * BLOCK, BLOCK)
    for h in range(key_heads):
        piece = turn(keys[:, h * HD : (h + 1) * HD], cosine, sine).astype(jnp.bfloat16)
        kv_ref[h] = piece
        kept[h, here] = piece
    values = nt(normed, wv_ref[...]).astype(jnp.bfloat16)
    for h in range(key_heads):
        kv_ref[key_heads + h] = values[:, h * HD : (h + 1) * HD]
    scaling = HD ** (-0.5)
    groups = query_heads // key_heads

    def attend(now):
        stop = (now + 1) * BLOCK
        for h in range(key_heads):
            turned[h, :, pl.ds(now * BLOCK, BLOCK)] = kv_ref[key_heads + h].T
        allowed = allowed_keys(begin, now * BLOCK, stop, BLOCK)

        def one_head(h, carry):
            group = lax.div(h, groups)
            scores = nt(kept[group, pl.ds(0, stop)], q_ref[h])
            scores = jnp.where(allowed, scores, -jnp.inf)
            highest = jnp.max(scores, axis=0, keepdims=True)
            exponent = jnp.exp2((scores - highest) * (scaling * LOG2_E))
            total = jnp.sum(exponent, axis=0, keepdims=True)
            weights = exponent.astype(jnp.bfloat16)
            mixed = nn(turned[group, :, pl.ds(0, stop)], weights) * (1.0 / total)
            highest = highest * scaling
            o_heads[h] = mixed.T.astype(jnp.bfloat16)
            lse_ref[pl.ds(h, 1)] = highest + jnp.log(total)
            return carry

        lax.fori_loop(0, query_heads, one_head, 0)

    for now in range(blocks):
        pl.when(block == now)(lambda now=now: attend(now))
    for h in range(query_heads):
        o_ref[:, head(h)] = o_heads[h]


def first_call(
    tokens,
    lengths,
    owners,
    first_gain,
    second_gain,
    query_weight,
    key_weight,
    value_weight,
    cotangent,
    tables,
):
    slots, width = tokens.shape
    blocks = slots // BLOCK
    columns, pairs = query_weight.shape[1], 2 * key_weight.shape[0] // HD
    heads = columns // HD

    def kernel(*refs):
        first_kernel(blocks, *refs)

    def rows_of(size):
        return pl.BlockSpec((BLOCK, size), lambda i: (i, 0))

    def whole(array):
        return pl.BlockSpec(array.shape, lambda i: (0, 0), pipeline_mode=pl.Buffered(1))

    whole_gain = pl.BlockSpec((width,), lambda i: (0,), pipeline_mode=pl.Buffered(1))
    row = jax.ShapeDtypeStruct((1, width), jnp.float32)
    scalars = pl.BlockSpec(memory_space=pltpu.SMEM)
    return pl.pallas_call(
        kernel,
        grid=(blocks,),
        out_shape=(
            jax.ShapeDtypeStruct((slots, width), jnp.bfloat16),
            jax.ShapeDtypeStruct((slots, width), jnp.bfloat16),
            jax.ShapeDtypeStruct((heads, slots, HD), jnp.bfloat16),
            jax.ShapeDtypeStruct((pairs, slots, HD), jnp.bfloat16),
            jax.ShapeDtypeStruct((slots, columns), jnp.bfloat16),
            jax.ShapeDtypeStruct((heads, slots), jnp.float32),
            jax.ShapeDtypeStruct((1, slots), jnp.int32),
            jax.ShapeDtypeStruct((1,), jnp.int32),
            row,
            row,
        ),
        in_specs=[
            scalars,
            scalars,
            rows_of(width),
            rows_of(width),
            whole_gain,
            whole_gain,
            whole(query_weight),
            whole(key_weight),
            whole(value_weight),
            whole(tables[0]),
            whole(tables[1]),
        ],
        out_specs=(
            rows_of(width),
            rows_of(width),
            pl.BlockSpec((heads, BLOCK, HD), lambda i: (0, i, 0)),
            pl.BlockSpec((pairs, BLOCK, HD), lambda i: (0, i, 0)),
            rows_of(columns),
            pl.BlockSpec((heads, BLOCK), lambda i: (0, i)),
            pl.BlockSpec((1, BLOCK), lambda i: (0, i)),
            scalars,
            pl.BlockSpec((1, width), lambda i: (0, 0)),
            pl.BlockSpec((1, width), lambda i: (0, 0)),
        ),
        scratch_shapes=[
            pltpu.VMEM((pairs // 2, slots, HD), jnp.bfloat16),
            pltpu.VMEM((pairs // 2, HD, slots), jnp.bfloat16),
            pltpu.VMEM((heads, BLOCK, HD), jnp.bfloat16),
        ],
        compiler_params=pltpu.CompilerParams(vmem_limit_bytes=67043328),
        name="first",
    )(
        lengths,
        owners,
        tokens,
        cotangent,
        first_gain,
        second_gain,
        query_weight,
        key_weight,
        value_weight,
        *tables,
    )


def last_kernel(group_columns, *refs):
    sources, gains, targets, buffers = refs[:8], refs[8], refs[9:18], refs[20:31]
    in_sems, out_sems = refs[31:]
    for i, target in enumerate(refs[18:20]):
        target[...] = gains[i]
    out, token, down, gate, up, mix, one, two = buffers[:8]
    turned = buffers[8:]
    coming = [
        pltpu.make_async_copy(source, buffer, in_sems.at[i])
        for i, (source, buffer) in enumerate(zip(sources, buffers[:8]))
    ]
    for copy in coming:
        copy.start()
    leaving = []

    def leave(buffer):
        i = len(leaving)
        copy = pltpu.make_async_copy(buffer, targets[i], out_sems.at[i])
        copy.start()
        leaving.append(copy)

    for i in (0, 1, 2, 3, 4, 5):
        coming[i].wait()
        leave(buffers[i])
    start = 0
    coming[6].wait()
    coming[7].wait()
    for buffer in turned:
        each = buffer.shape[1] // 2
        buffer[:, pl.ds(0, each)] = one[:, pl.ds(start, each)]
        buffer[:, pl.ds(each, each)] = two[:, pl.ds(start, each)]
        start += each
        leave(buffer)
    for copy in leaving:
        copy.wait()


def last_call(arrays, gains, query_columns, key_columns):
    rows = arrays[6].shape[0]
    shapes = [jax.ShapeDtypeStruct(array.shape, array.dtype) for array in arrays[:6]]
    shapes += [
        jax.ShapeDtypeStruct((rows, size), jnp.float32)
        for size in (query_columns, key_columns, key_columns)
    ]

    def kernel(*refs):
        last_kernel(TILE, *refs)

    buffers = [pltpu.VMEM(array.shape, array.dtype) for array in arrays]
    buffers += [pltpu.VMEM(shape.shape, shape.dtype) for shape in shapes[6:]]
    return pl.pallas_call(
        kernel,
        out_shape=(*shapes, *([jax.ShapeDtypeStruct(gains.shape[1:], gains.dtype)] * 2)),
        in_specs=[pl.BlockSpec(memory_space=pl.ANY)] * 8 + vmem_specs(1),
        out_specs=(*([pl.BlockSpec(memory_space=pl.ANY)] * 9), *vmem_specs(2)),
        scratch_shapes=[
            *buffers,
            pltpu.SemaphoreType.DMA((8,)),
            pltpu.SemaphoreType.DMA((9,)),
        ],
        compiler_params=pltpu.CompilerParams(vmem_limit_bytes=67043328),
        name="last",
    )(*arrays, gains)


def lanes(index):
    return pl.ds(pl.multiple_of(index * 128, 128), HD)


def attention_back(q_ref, kv_ref, grads, begin_ref, lse_ref, turned, sums, heads, group, start, leave):
    scaling = HD ** (-0.5)
    key_sum, value_sum = sums
    key_heads = kv_ref.shape[0] // 2
    stop = start + BLOCK
    rows = pl.ds(start, BLOCK)
    seen = pl.ds(0, stop)
    if stop == q_ref.shape[1]:
        key_sum[...] = jnp.zeros_like(key_sum)
        value_sum[...] = jnp.zeros_like(value_sum)
    allowed = allowed_keys(begin_ref[:, rows], start, stop, BLOCK)

    def one_head(h, carry):
        query = q_ref[h, rows]
        grad = grads[rows, lanes(h)]
        scores = nt(kv_ref[group, seen], query) * scaling
        weights = jnp.where(allowed, jnp.exp(scores - lse_ref[pl.ds(h, 1), rows]), 0.0)
        weights_grad = nt(kv_ref[key_heads + group, seen], grad)
        inner = jnp.sum(weights * weights_grad, axis=0, keepdims=True)
        scores_grad = (weights * (weights_grad - inner)).astype(jnp.bfloat16)
        value_sum[seen] += nn(weights.astype(jnp.bfloat16), grad)
        key_sum[seen] += nn(scores_grad, query)
        leave(h, rows, nn(turned[:, :stop], scores_grad).T * scaling)
        return carry

    lax.fori_loop(heads[0], heads[1], one_head, 0)


P_START = "start"
P_TILE = "tile"
P_ARRIVE = "arrive"
P_FORWARD = "forward"
P_FINISH = "finish"
P_BACK = "back"
P_ATTENTION = "attention"
P_KEYS = "keys"
P_PRODUCT = "product"
P_SEND = "send"
P_ADD = "add"
P_DM = "dm"
P_FEED = "feed"
P_DA = "da"
P_DOWN = "down"
P_GATE = "gate"
P_UP = "up"
P_MIX = "mix"
P_ONE = "one"
P_TWO = "two"

PLAN = (
    (P_TILE, P_GATE, 3),
    (P_TILE, P_DOWN, 3),
    (P_START, P_DM),
    (P_ARRIVE, P_DM, 0, 0, 1),
    (P_TILE, P_GATE, 1),
    (P_TILE, P_DOWN, 1),
    (P_TILE, P_GATE, 2),
    (P_ARRIVE, P_DM, 0, 0, 2),
    (P_ARRIVE, P_GATE, 0, 0, 0),
    (P_ARRIVE, P_DM, 0, 0, 0),
    (P_ARRIVE, P_DM, 0, 1, 1),
    (P_ARRIVE, P_DM, 0, 1, 3),
    (P_ARRIVE, P_DM, 0, 0, 3),
    (P_ARRIVE, P_GATE, 0, 1, 0),
    (P_TILE, P_DOWN, 2),
    (P_ARRIVE, P_DOWN, 0, 0, 0),
    (P_ARRIVE, P_DM, 0, 1, 0),
    (P_TILE, P_GATE, 0),
    (P_ARRIVE, P_DM, 0, 1, 2),
    (P_TILE, P_DOWN, 0),
    (P_TILE, P_UP, 3),
    (P_ARRIVE, P_DM, 1, 0, 1),
    (P_ARRIVE, P_DM, 1, 0, 0),
    (P_ARRIVE, P_GATE, 0, 2, 0),
    (P_FORWARD, 1),
    (P_ARRIVE, P_DM, 1, 0, 2),
    (P_FINISH, 1),
    (P_ARRIVE, P_DOWN, 0, 2, 0),
    (P_FORWARD, 0),
    (P_ARRIVE, P_DM, 1, 0, 3),
    (P_TILE, P_UP, 1),
    (P_TILE, P_UP, 2),
    (P_TILE, P_UP, 0),
    (P_ARRIVE, P_GATE, 0, 3, 0),
    (P_FINISH, 0),
    (P_ARRIVE, P_DOWN, 1, 0, 0),
    (P_FORWARD, 2),
    (P_FINISH, 2),
    (P_FORWARD, 3),
    (P_FINISH, 3),
    (P_START, P_FEED),
    (P_TILE, P_MIX, 3),
    (P_ARRIVE, P_FEED, 0, 0, 0),
    (P_TILE, P_MIX, 1),
    (P_TILE, P_MIX, 2),
    (P_TILE, P_MIX, 0),
    (P_BACK,),
    (P_ARRIVE, P_FEED, 0, 0, 1),
    (P_ATTENTION, 0, 3),
    (P_ARRIVE, P_FEED, 0, 1, 2),
    (P_ARRIVE, P_UP, 0, 0, 0),
    (P_ARRIVE, P_FEED, 0, 1, 1),
    (P_ARRIVE, P_FEED, 0, 0, 3),
    (P_ARRIVE, P_GATE, 1, 1, 0),
    (P_ARRIVE, P_GATE, 1, 0, 0),
    (P_ARRIVE, P_UP, 0, 1, 0),
    (P_ARRIVE, P_FEED, 0, 1, 0),
    (P_ARRIVE, P_FEED, 0, 1, 3),
    (P_ATTENTION, 0, 2),
    (P_ATTENTION, 0, 1),
    (P_ARRIVE, P_FEED, 1, 0, 1),
    (P_ATTENTION, 0, 0),
    (P_ARRIVE, P_FEED, 0, 0, 2),
    (P_ARRIVE, P_DOWN, 0, 1, 0),
    (P_ARRIVE, P_DOWN, 0, 3, 0),
    (P_ARRIVE, P_UP, 0, 2, 0),
    (P_ARRIVE, P_FEED, 1, 0, 0),
    (P_KEYS, 0),
    (P_TILE, P_ONE, 3),
    (P_TILE, P_ONE, 1),
    (P_TILE, P_ONE, 2),
    (P_TILE, P_ONE, 0),
    (P_ATTENTION, 1, 3),
    (P_ATTENTION, 1, 2),
    (P_ARRIVE, P_MIX, 0, 0, 0),
    (P_ATTENTION, 1, 1),
    (P_ATTENTION, 1, 0),
    (P_ARRIVE, P_UP, 1, 0, 0),
    (P_ARRIVE, P_FEED, 1, 0, 2),
    (P_ARRIVE, P_GATE, 2, 0, 0),
    (P_ARRIVE, P_MIX, 0, 2, 0),
    (P_ARRIVE, P_UP, 0, 3, 0),
    (P_ARRIVE, P_FEED, 1, 0, 3),
    (P_KEYS, 1),
    (P_TILE, P_TWO, 3),
    (P_TILE, P_TWO, 1),
    (P_TILE, P_TWO, 2),
    (P_TILE, P_TWO, 0),
    (P_PRODUCT, 3),
    (P_PRODUCT, 1),
    (P_PRODUCT, 2),
    (P_ARRIVE, P_DA, 0, 0, 1),
    (P_ARRIVE, P_DA, 0, 0, 2),
    (P_ARRIVE, P_MIX, 0, 1, 0),
    (P_PRODUCT, 0),
    (P_ARRIVE, P_DOWN, 1, 1, 0),
    (P_ARRIVE, P_DA, 0, 0, 3),
    (P_ARRIVE, P_ONE, 0, 0, 0),
    (P_ARRIVE, P_DA, 0, 0, 0),
    (P_ARRIVE, P_ONE, 0, 1, 0),
    (P_ARRIVE, P_UP, 1, 1, 0),
    (P_ARRIVE, P_DA, 0, 1, 0),
    (P_ARRIVE, P_MIX, 1, 0, 0),
    (P_ARRIVE, P_ONE, 0, 3, 0),
    (P_ARRIVE, P_DA, 0, 1, 2),
    (P_ARRIVE, P_TWO, 0, 0, 0),
    (P_ARRIVE, P_ONE, 0, 2, 0),
    (P_ARRIVE, P_DA, 0, 1, 3),
    (P_ARRIVE, P_DA, 1, 0, 3),
    (P_ARRIVE, P_DA, 0, 1, 1),
    (P_ARRIVE, P_DA, 1, 0, 1),
    (P_ARRIVE, P_TWO, 0, 1, 0),
    (P_ARRIVE, P_MIX, 0, 3, 0),
    (P_ARRIVE, P_DA, 1, 0, 0),
    (P_ARRIVE, P_DA, 1, 0, 2),
    (P_SEND, 0),
    (P_ADD, 0),
    (P_ARRIVE, P_ONE, 1, 0, 0),
    (P_ARRIVE, P_DOWN, 2, 0, 0),
    (P_ARRIVE, P_TWO, 0, 2, 0),
    (P_SEND, 1),
    (P_ADD, 1),
    (P_SEND, 2),
    (P_ADD, 2),
    (P_SEND, 3),
    (P_ARRIVE, P_TWO, 1, 0, 0),
    (P_ARRIVE, P_MIX, 1, 1, 0),
    (P_ADD, 3),
    (P_ARRIVE, P_UP, 2, 0, 0),
    (P_ARRIVE, P_ONE, 1, 1, 0),
    (P_ARRIVE, P_ONE, 2, 0, 0),
    (P_ARRIVE, P_MIX, 2, 0, 0),
    (P_ARRIVE, P_TWO, 0, 3, 0),
    (P_ARRIVE, P_TWO, 1, 1, 0),
    (P_SEND, 4),
    (P_ARRIVE, P_TWO, 2, 0, 0),
    (P_ADD, 4),
)


def plan_of(count, orders, reduces):
    if count == 8:
        return PLAN
    tiles = (3, 1, 2, 0)

    def units(name, step):
        return [(P_ARRIVE, name, step, j, c) for j, c in reduces[name].units(step)]

    plan = [(P_START, P_DM)]
    plan += [(P_TILE, name, which) for name in (P_DOWN, P_GATE, P_UP) for which in tiles]
    plan += units(P_DM, 0) + units(P_DM, 1)
    plan += [(P_FORWARD, c) for c in range(SPLIT)] + [(P_FINISH, c) for c in range(SPLIT)]
    plan += [(P_START, P_FEED)] + [(P_TILE, P_MIX, which) for which in tiles] + [(P_BACK,)]
    for group in range(2):
        plan += [(P_ATTENTION, group, block) for block in (3, 2, 1, 0)]
        plan += [(P_KEYS, group)]
        plan += [(P_TILE, (P_ONE, P_TWO)[group], which) for which in tiles]
    plan += units(P_FEED, 0) + units(P_FEED, 1)
    plan += [(P_PRODUCT, place) for place in (3, 1, 2, 0)] + units(P_DA, 0) + units(P_DA, 1)
    names = (P_DOWN, P_GATE, P_UP, P_MIX, P_ONE, P_TWO)
    for step in range(len(orders[0])):
        for name in names:
            plan += units(name, step)
    for i in range(2 + len(orders[0])):
        plan += [(P_SEND, i), (P_ADD, i)]
    return plan


def back_kernel(
    dp_order,
    z_order,
    dm_hbm,
    feed_hbm,
    m_hbm,
    gm_hbm,
    hid_hbm,
    dgate_hbm,
    dup_hbm,
    a_hbm,
    tokens_hbm,
    used_ref,
    h_ref,
    gain1_ref,
    gain2_ref,
    mixing_ref,
    query_ref,
    key_ref,
    value_ref,
    o_ref,
    q_ref,
    kv_ref,
    begin_ref,
    lse_ref,
    base_ref,
    step_ref,
    out_ref,
    token_ref,
    gains_ref,
    down_ref,
    gate_ref,
    up_ref,
    mix_ref,
    one_ref,
    two_ref,
    *scratch,
):
    (
        wide,
        m_buf,
        hid_buf,
        dgate_buf,
        rs_part,
        rs_land,
        ga_buf,
        dh_buf,
        key_sum,
        value_sum,
        gains_land,
        cot_ref,
        result,
        *scratch,
    ) = scratch
    parts, lands, sems = scratch[:6], scratch[6:12], scratch[12:]
    stage, stage_sem, out_sem, load_sems, credit, *sems = sems
    index = lax.axis_index("tensor")
    dp_index = lax.axis_index("dp")
    count = 1 << len(dp_order)

    own_rows = span(index * h_ref.shape[0], h_ref.shape[0])
    loads = [
        pltpu.make_async_copy(source, target, load_sems.at[i])
        for i, (source, target) in enumerate(
            (
                (dm_hbm, rs_part),
                (gm_hbm, wide),
                (hid_hbm, hid_buf),
                (m_hbm, m_buf),
                (dgate_hbm, dgate_buf),
                (dup_hbm, hid_buf),
                (feed_hbm, rs_part),
                (a_hbm, wide),
                (gm_hbm.at[own_rows], cot_ref),
                (tokens_hbm.at[own_rows], cot_ref),
            )
        )
    ]
    for i in (3, 4, 1, 2, 0, 8):
        loads[i].start()
    greet(TENSOR_PEERS + tuple(("dp", bit) for bit in dp_order))

    def share_reduce(first_sem):
        return Reduce(rs_part, rs_land, sems[first_sem], sems[first_sem + 1], "tensor", (0, 1), SPLIT)

    dm, feed, da = share_reduce(0), share_reduce(2), share_reduce(4)
    gather = Gather(ga_buf, sems[6], sems[7], SPLIT)
    orders = (z_order, dp_order, dp_order, dp_order, dp_order, dp_order)
    down, gate, up, mix, one, two = (
        Reduce(parts[i], lands[i], sems[8 + 2 * i], sems[9 + 2 * i], "dp", orders[i])
        for i in range(6)
    )
    gains_send, gains_recv = sems[20], sems[21]
    gains_ref[...] = jnp.zeros_like(gains_ref)

    def finish_out(start, size, total):
        own = span(start, size)
        places = index * h_ref.shape[0] + start + lax.broadcasted_iota(jnp.int32, (size, 1), 0)
        live = (places < used_ref[0]).astype(jnp.float32)
        result[own] = ((h_ref[own] + total) * live).astype(jnp.bfloat16)

    def finish_dm(start, size, total):
        own = span(start, size)
        hidden = h_ref[own]
        inverse = lax.rsqrt(jnp.mean(hidden * hidden, axis=-1, keepdims=True) + epsilon)
        scaled = total * gain2_ref[...]
        inner = jnp.mean(scaled * hidden, axis=-1, keepdims=True)
        grad = (
            cot_ref[own].astype(jnp.float32)
            + inverse * scaled
            - hidden * (inverse * inverse * inverse) * inner
        )
        dh_buf[own] = grad
        ga_buf[span(index * dh_buf.shape[0] + start, size)] = grad.astype(jnp.bfloat16)
        gains_ref[pl.ds(1, 1)] += jnp.sum(total * hidden * inverse, axis=0, keepdims=True)

    def finish_da(start, size, total):
        own = span(start, size)
        values = cot_ref[own].astype(jnp.float32)
        inverse = lax.rsqrt(jnp.mean(values * values, axis=-1, keepdims=True) + epsilon)
        scaled = total * gain1_ref[...]
        inner = jnp.mean(scaled * values, axis=-1, keepdims=True)
        grad = dh_buf[own] + inverse * scaled - values * (inverse * inverse * inverse) * inner
        result[own] = grad.astype(jnp.bfloat16)
        gains_ref[pl.ds(0, 1)] += jnp.sum(total * values * inverse, axis=0, keepdims=True)

    out_copy = pltpu.make_async_copy(result, out_ref, out_sem.at[0])
    token_copy = pltpu.make_async_copy(result, token_ref, out_sem.at[1])
    flying = []

    def settle():
        for copy in flying:
            copy.wait()
        flying.clear()

    def finish_grad(reduce, target):
        settle()
        columns = pl.ds(0, reduce.part.shape[1])

        def store(start, size, total):
            stage[span(start, size), columns] = total

        reduce.arrive_all(last, store)
        copy = pltpu.make_async_copy(stage.at[:, columns], target, stage_sem)
        copy.start()
        flying.append(copy)

    def grad_tile(left, right, columns, reduce, which):
        blocks = TILE // reduce.rows
        tile = flip(lax.div(dp_index, blocks), which) * TILE
        cols = pl.ds(pl.multiple_of(tile, 128), TILE)
        width = columns.stop - columns.start
        step = min(width, 512)

        def some(i, carry):
            there = pl.ds(pl.multiple_of(i * step, 128), step)
            here = pl.ds(pl.multiple_of(columns.start + i * step, 128), step)
            reduce.part[span(tile, TILE), there] = tn(left[:, cols], right[:, here]).astype(
                jnp.bfloat16
            )
            return carry

        lax.fori_loop(0, width // step, some, 0)
        kept, _ = reduce.lists[0]
        for j, kept_place in enumerate(kept):
            if (kept_place | (1 << reduce.order[0])) // blocks == which:
                reduce.start(0, j)

    slots, hidden_columns = hid_buf.shape
    query_heads = q_ref.shape[0]
    query_columns, key_columns = query_heads * HD, kv_ref.shape[0] * HD // 2
    queries_each = query_columns // key_columns
    scaling = HD ** (-0.5)
    last = len(dp_order) - 1
    reduces = {
        "dm": dm,
        "feed": feed,
        "da": da,
        "down": down,
        "gate": gate,
        "up": up,
        "mix": mix,
        "one": one,
        "two": two,
    }
    targets = {
        "down": down_ref,
        "gate": gate_ref,
        "up": up_ref,
        "mix": mix_ref,
        "one": one_ref,
        "two": two_ref,
    }
    sources = {
        "down": (wide, hid_buf, slice(0, hidden_columns)),
        "gate": (m_buf, dgate_buf, slice(0, hidden_columns)),
        "up": (m_buf, hid_buf, slice(0, hidden_columns)),
        "mix": (ga_buf, o_ref, slice(0, query_columns)),
        "one": (wide, dgate_buf, slice(0, TILE)),
        "two": (wide, dgate_buf, slice(TILE, 2 * TILE)),
    }
    before = {
        ("down", 3): (1, 2),
        ("gate", 3): (3, 4),
        ("up", 3): (5,),
        ("one", 3): (7,),
    }
    peers = TENSOR_PEERS + tuple(("dp", bit) for bit in dp_order)
    gains = []
    ended = []
    turned = {}

    def turned_back(values, block):
        cosine, sine = block_angles(base_ref, step_ref, block)
        return turn(values, cosine, -sine).astype(jnp.bfloat16)

    def keep(rows, values, grouped, plain):
        dgate_buf[rows, pl.ds(grouped, HD)] = values
        hid_buf[rows, pl.ds(plain, HD)] = values

    def do_start(name):
        if name == "dm":
            loads[0].wait()
            loads[8].wait()
        else:
            dm.close()
            loads[9].start()
            loads[6].start()
            loads[6].wait()
        reduces[name].start_all()

    def do_tile(name, which):
        for i in before.get((name, which), ()):
            loads[i].wait()
        left, right, columns = sources[name]
        grad_tile(left, right, columns, reduces[name], which)
        if (name, which) == ("down", 0):
            loads[5].start()
            loads[7].start()

    def do_arrive(name, step, j, c):
        reduce = reduces[name]
        if name in targets:
            if step == last:
                finish_grad(reduce, targets[name])
            else:
                reduce.arrive(step, j, c)
        elif step == 0:
            reduce.arrive(step, j, c)
        else:
            reduce.arrive(step, j, c, {"dm": finish_dm, "feed": finish_out, "da": finish_da}[name])
            if name == "dm":
                gather.start(c)
            ended.append(name)
            if name == "feed" and ended.count(name) == SPLIT:
                for mask in (1, 2):
                    pl.semaphore_signal(
                        credit,
                        inc=1,
                        device_id={"tensor": flip(index, mask)},
                        device_id_type=MESH,
                    )
                feed.close()
                out_copy.start()
            if name == "da" and ended.count(name) == SPLIT:
                token_copy.start()

    def do_back():
        def some(i, carry):
            rows = span(i * BLOCK, BLOCK)
            grads = nn(ga_buf[rows], mixing_ref[...]).astype(jnp.bfloat16)
            for h in range(query_heads):
                m_buf[rows, lanes(h)] = grads[:, h * HD : (h + 1) * HD]
            return carry

        lax.fori_loop(0, slots // BLOCK, some, 0)

    def do_attention(group, block):
        if group not in turned:
            turned[group] = kv_ref[group].T

        def leave(h, rows, values):
            m_buf[rows, lanes(query_heads + h)] = turned_back(values, block)

        attention_back(
            q_ref,
            kv_ref,
            m_buf,
            begin_ref,
            lse_ref,
            turned[group],
            (key_sum, value_sum),
            (group * queries_each, (group + 1) * queries_each),
            group,
            block * BLOCK,
            leave,
        )

    def do_keys(group):
        grouped = group * TILE + queries_each * HD
        plain = query_columns + group * HD

        def some(i, carry):
            rows = span(i * BLOCK, BLOCK)
            for each in range(queries_each):
                h = group * queries_each + each
                keep(rows, m_buf[rows, lanes(query_heads + h)], group * TILE + each * HD, h * HD)
            keep(rows, turned_back(key_sum[rows] * scaling, i), grouped, plain)
            keep(rows, value_sum[rows].astype(jnp.bfloat16), grouped + HD, plain + key_columns)
            return carry

        lax.fori_loop(0, slots // BLOCK, some, 0)

    def do_product(place):
        if place == 3:
            loads[9].wait()
            out_copy.wait()
            pl.semaphore_wait(credit, 2)
        block = span(flip(index, place) * BLOCK, BLOCK)

        def some(i, carry):
            cols = pl.ds(pl.multiple_of(i * 512, 512), 512)
            total = nt(hid_buf[block, pl.ds(0, query_columns)], query_ref[cols])
            total += nn(hid_buf[block, pl.ds(query_columns, key_columns)], key_ref[:, cols])
            total += nn(
                hid_buf[block, pl.ds(query_columns + key_columns, key_columns)], value_ref[:, cols]
            )
            rs_part[block, cols] = total.astype(jnp.bfloat16)
            return carry

        lax.fori_loop(0, rs_part.shape[1] // 512, some, 0)
        if place in (3, 1):
            for c in range(SPLIT):
                da.start(0, (3, 1).index(place), c)

    def do_send_gains(i):
        axis, bit = peers[i]
        copy = pltpu.make_async_remote_copy(
            src_ref=gains_ref,
            dst_ref=gains_land.at[i],
            send_sem=gains_send.at[i],
            recv_sem=gains_recv.at[i],
            device_id={axis: flip(lax.axis_index(axis), 1 << bit)},
            device_id_type=MESH,
        )
        copy.start()
        gains.append(copy)

    def do_finish(c):
        gather.near(c)
        gather.finish(c)

    def do_add_gains(i):
        gains[i].wait()
        gains_ref[...] += gains_land[i]

    actions = {
        "start": do_start,
        "tile": do_tile,
        "arrive": do_arrive,
        "forward": gather.forward,
        "finish": do_finish,
        "back": do_back,
        "attention": do_attention,
        "keys": do_keys,
        "product": do_product,
        "send": do_send_gains,
        "add": do_add_gains,
    }
    for action, *rest in plan_of(count, orders, reduces):
        actions[action](*rest)
    settle()
    token_copy.wait()
    for item in (da, gather, down, gate, up, mix, one, two):
        item.close()


def back_call(
    dm_part,
    feed_part,
    second_in,
    outer_low,
    hidden,
    gate_low,
    upward_low,
    first_in,
    tokens,
    used,
    middle,
    first_gain,
    second_gain,
    mixing_weight,
    query_weight,
    key_weight,
    value_weight,
    attended,
    queries,
    pairs,
    begin,
    log_totals,
    tables,
):
    slots, width = dm_part.shape
    rows = slots // 4
    columns = hidden.shape[1]
    heads = attended.shape[1]
    count = lax.axis_size("dp")
    dp_order = bits_of(count)
    z_order = (dp_order[1], dp_order[0]) + dp_order[2:]
    block = width // count
    share = Reduce.slots(4, SPLIT)
    total = Reduce.slots(count)

    def kernel(*refs):
        back_kernel(dp_order, z_order, *refs)

    def grad(size):
        return jax.ShapeDtypeStruct((block, size), jnp.float32)

    def low(*shape):
        return pltpu.VMEM(shape, jnp.bfloat16)

    sizes = (columns, columns, columns, heads, TILE, TILE)
    hops = 2 + len(dp_order)
    return pl.pallas_call(
        kernel,
        out_shape=(
            jax.ShapeDtypeStruct((rows, width), jnp.bfloat16),
            jax.ShapeDtypeStruct((rows, width), jnp.bfloat16),
            jax.ShapeDtypeStruct((2, width), jnp.float32),
            *(grad(size) for size in sizes),
        ),
        in_specs=[pl.BlockSpec(memory_space=pl.ANY)] * 9
        + [pl.BlockSpec(memory_space=pltpu.SMEM)]
        + vmem_specs(14),
        out_specs=tuple(
            pl.BlockSpec(memory_space=pltpu.VMEM if i == 2 else pl.ANY) for i in range(9)
        ),
        scratch_shapes=[
            low(slots, width),
            low(slots, width),
            low(slots, columns),
            low(slots, columns),
            low(slots, width),
            low(share, rows // SPLIT, width),
            low(slots, width),
            pltpu.VMEM((rows, width), jnp.float32),
            pltpu.VMEM((slots, HD), jnp.float32),
            pltpu.VMEM((slots, HD), jnp.float32),
            pltpu.VMEM((hops, 2, width), jnp.float32),
            low(rows, width),
            low(rows, width),
            *(low(width, size) for size in sizes),
            *(low(total, block, size) for size in sizes),
            pltpu.VMEM((block, columns), jnp.float32),
            pltpu.SemaphoreType.DMA,
            pltpu.SemaphoreType.DMA((2,)),
            pltpu.SemaphoreType.DMA((10,)),
            pltpu.SemaphoreType.REGULAR,
            *dma_sems(share),
            *dma_sems(share),
            *dma_sems(share),
            *dma_sems(3 * SPLIT),
            *(sem for size in sizes for sem in dma_sems(total)),
            *dma_sems(hops),
        ],
        compiler_params=pltpu.CompilerParams(
            collective_id=1, has_side_effects=True, vmem_limit_bytes=67043328
        ),
        name="back",
    )(
        dm_part,
        feed_part,
        second_in,
        outer_low,
        hidden,
        gate_low,
        upward_low,
        first_in,
        tokens,
        used,
        middle,
        first_gain,
        second_gain,
        mixing_weight,
        query_weight,
        key_weight,
        value_weight,
        attended,
        queries,
        pairs,
        begin,
        log_totals,
        *tables,
    )


def on_device(
    tokens,
    lengths,
    owners,
    first_gain,
    query_weight,
    key_weight,
    value_weight,
    mixing_weight,
    second_gain,
    gate_weight,
    up_weight,
    down_weight,
    cotangent,
):
    tables = rope_tables(tokens.shape[0])
    key_turned, value_turned = key_weight.T, value_weight.T
    (
        first_in,
        outer_low,
        queries,
        pairs,
        attended,
        log_totals,
        begin,
        used,
        first_row,
        second_row,
    ) = first_call(
        tokens,
        lengths,
        owners,
        first_gain,
        second_gain,
        query_weight,
        key_turned,
        value_turned,
        cotangent,
        tables,
    )
    middle, second_in, hidden, gate_low, upward_low, feed_part, second_part = middle_call(
        attended,
        mixing_weight,
        second_row,
        tokens,
        outer_low,
        gate_weight,
        up_weight,
        down_weight,
    )
    layer_output, token_grad, gains, *grads = back_call(
        second_part,
        feed_part,
        second_in,
        outer_low,
        hidden,
        gate_low,
        upward_low,
        first_in,
        tokens,
        used,
        middle,
        first_row,
        second_row,
        mixing_weight,
        query_weight,
        key_turned,
        value_turned,
        attended,
        queries,
        pairs,
        begin,
        log_totals,
        tables,
    )
    (
        layer_output,
        token_grad,
        down_grad,
        gate_grad,
        up_grad,
        mixing_grad,
        query_grad,
        key_grad,
        value_grad,
        first_grad,
        second_grad,
    ) = last_call(
        [layer_output, token_grad, *grads], gains, query_weight.shape[1], key_weight.shape[1]
    )
    return (
        layer_output,
        token_grad,
        first_grad,
        query_grad,
        key_grad,
        value_grad,
        mixing_grad,
        second_grad,
        gate_grad,
        up_grad,
        down_grad,
    )


def solution(mesh):
    in_specs = (
        P("dp", None),
        P(),
        P(),
        P(),
        P(None, "tensor"),
        P(None, "tensor"),
        P(None, "tensor"),
        P(None, "tensor"),
        P(),
        P(None, "tensor"),
        P(None, "tensor"),
        P(None, "tensor"),
        P("dp", None),
    )
    out_specs = (
        P(("dp", "tensor"), None),
        P(("dp", "tensor"), None),
        P(),
        P("dp", "tensor"),
        P("dp", "tensor"),
        P("dp", "tensor"),
        P("dp", "tensor"),
        P(),
        P("dp", "tensor"),
        P("dp", "tensor"),
        P("dp", "tensor"),
    )
    return jax.shard_map(
        on_device, mesh=mesh, in_specs=in_specs, out_specs=out_specs, check_vma=False
    )
```
